32 devices in a mesh: dp: 4 (over y, x), expert: 8 (over z, core).
Axes of the slice: x: 2, y: 2, z: 4, core: 2. Of those that a mesh axis runs over, the one named last changes fastest.
Arguments:
- tokens: bfloat16 [10240, 2048], P(('dp', 'expert')), may hold values from -6 to 6
- out_grad: bfloat16 [10240, 2048], P(('dp', 'expert')), may hold values from -6 to 6
- expert_ids: int32 [10240, 2], P(('dp', 'expert')), may hold values from 0 to 7, all different within a row; in each aligned block of 320 rows (0 to 319, 320 to 639, ...) at most 120 rows name the same one
- route_weight: bfloat16 [10240, 2], P(('dp', 'expert')), may hold values from 0.099609375 to 1
- w_gate: bfloat16 [8, 2048, 768], P('expert', 'dp'), may hold values from -0.125 to 0.125
- w_up: bfloat16 [8, 2048, 768], P('expert', 'dp'), may hold values from -0.125 to 0.125
- w_down: bfloat16 [8, 768, 2048], P('expert', None, 'dp'), may hold values from -0.21875 to 0.21875
Outputs:
- token_grad: bfloat16 [10240, 2048], P(('dp', 'expert'))
- route_grad: bfloat16 [10240, 2], P(('dp', 'expert'))
- gate_grad: bfloat16 [8, 2048, 768], P('expert', 'dp')
- up_grad: bfloat16 [8, 2048, 768], P('expert', 'dp')
- down_grad: bfloat16 [8, 768, 2048], P('expert', None, 'dp')
The draws below stay inside these ranges and needn't reach their ends.
Inputs may be any that keep to these rules, and one draw needn't show every extreme that they name: `expert_ids`: each row names 2 different experts. In the rows of one device no expert is named more than 120 times, a bound that some block reaches in some device.
All inputs are finite; a program needn't handle non-finite values.
Results may differ from the reference program's by a relative error of at most 0.014.
Values may be sent and summed in bfloat16 or wider, within the bound.
A program may use at most 128 MiB of HBM per device.

```python
import math
import jax
import jax.numpy as jnp
import numpy as np
from jax import lax

D = 2048
FF = 768
TOP_WIN = 2
TOK_DEV = 320
EXPERTS_WIN = 8
CAP = 120
TOKENS = 10240
N_DP = 4
N_EXPERT = 8


def with_spikes(result, key, source, target, blocks, factor):
    owner, partner = [(jnp.arange(result.shape[axis_at]) // (result.shape[axis_at] // blocks)).reshape([-1 if axis == axis_at else 1 for axis in range(result.ndim)]) for axis_at in (source, target)]
    chosen = jax.random.permutation(key, blocks)[partner]
    strong = (owner == chosen) | (owner == (partner + blocks // 2) % blocks)
    return jnp.where(strong, factor * result, result)


def steps_of(rng, shape, pieces, smallest, largest):
    loudness = 1.0
    for dim, shards_of in pieces:
        heights = jax.random.uniform(jax.random.fold_in(jax.random.fold_in(rng, 6), dim), (shards_of,), jnp.float32, smallest / len(pieces), largest / len(pieces))
        loudness = loudness * jnp.repeat(jnp.exp(heights), shape[dim] // shards_of).reshape((-1,) + (1,) * (len(shape) - 1 - dim))
    return loudness


def routed_block(rng, own, number, rows, number_of, top, limit, slope):
    order = jax.random.permutation(rng, number_of)
    heavy_load, common = portions_of(number_of, rows * top, limit, slope, True), portions_of(number_of, rows * top, limit, slope, False)
    places = jnp.arange(number_of)

    def named(tallies, offset_by):
        used = int((tallies > 0).sum())
        fixed = max(1, used // 4)
        shifted = fixed + (places - fixed + offset_by * (used - fixed)) % max(1, number_of - fixed)
        return jnp.zeros((number_of,), jnp.int32).at[order[jnp.where(places < fixed, places, shifted)]].set(jnp.asarray(tallies, jnp.int32))

    tallies = jnp.where(number % 4 == 0, named(heavy_load, number // 4), named(common, number - number // 4 - 1))
    mixed = jax.random.permutation(jax.random.fold_in(own, 3), number_of)
    donor, taker = mixed[0:number_of // 2 * 2:2], mixed[1:number_of // 2 * 2:2]
    slack = jnp.minimum(tallies[donor] - 1, limit - tallies[taker]) // 2
    slack = jnp.where((donor == order[0]) | (taker == order[0]) | (tallies[taker] == 0), 0, jnp.maximum(slack, 0))
    shifted = jax.random.randint(jax.random.fold_in(own, 4), (number_of // 2,), 0, 1 << 20) % (slack + 1)
    tallies = tallies.at[donor].add(-shifted).at[taker].add(shifted)
    members = jnp.searchsorted(jnp.cumsum(tallies), jnp.arange(rows * top), side="right").astype(jnp.int32)
    listing = members.reshape(top, rows).T
    listing = listing[jax.random.permutation(jax.random.fold_in(own, 1), rows)]
    offset_by = jax.random.randint(jax.random.fold_in(own, 2), (rows, 1), 0, top)
    return jnp.take_along_axis(listing, (jnp.arange(top)[None, :] + offset_by) % top, axis=1)


def portions_of(count, total, most, lean, full):
    loads = [(1 << 20) // math.isqrt(standing ** lean) + 1 for standing in range(1, count + 1)]
    largest = most if full else min(most, max(-(-total // count), total * loads[0] // sum(loads)))
    least = 1 if total - largest >= count - 1 else 0
    given, rest = [largest] + [least] * (count - 1), total - largest - least * (count - 1)
    while rest > 0:
        movable = [i for i in range(1, count) if given[i] < largest] or [i for i in range(1, count) if given[i] < most]
        pool, left = sum([loads[i] for i in movable]), rest
        for i in movable:
            more = min(most - given[i], max(1, left * loads[i] // pool), rest)
            given[i] = given[i] + more
            rest = rest - more
    return np.array(given)


def noise(stream_key, extent, scale, most, pieces=(), held_as=jnp.bfloat16):
    result = scale * jax.random.normal(stream_key, extent, jnp.float32)
    if pieces:
        result = result * steps_of(stream_key, extent, pieces, -0.22, 0.18)
    return jnp.clip(result, -most, most).astype(held_as)


def gaussian_with(stream_key, extent, deviation, bound, split, heavy, kind=jnp.bfloat16):
    result = deviation * jax.random.normal(stream_key, extent, jnp.float32)
    if split:
        result = result * steps_of(stream_key, extent, split, -0.22, 0.18)
    return jnp.clip(with_spikes(result, jax.random.fold_in(stream_key, 3), *heavy), -bound, bound).astype(kind)


def setup_inputs(seed: int = 0) -> dict:
    keys = jax.random.split(jax.random.key(seed), 8)
    tokens = gaussian_with(keys[0], (TOKENS, D), 1.0, 6.0, ((0, 32),), (0, 1, 32, 2.75))
    out_grad = gaussian_with(keys[1], (TOKENS, D), 1.0, 6.0, ((0, 32),), (0, 1, 32, 2.75))
    expert_ids_keys = jax.random.split(jax.random.fold_in(keys[2], 1), TOKENS // TOK_DEV)
    expert_ids_turns = jax.random.permutation(jax.random.fold_in(keys[2], 3), TOKENS // TOK_DEV)
    expert_ids = jax.vmap(lambda own, number: routed_block(jax.random.fold_in(keys[2], 2), own, number, TOK_DEV, EXPERTS_WIN, TOP_WIN, CAP, 2))(expert_ids_keys, expert_ids_turns).reshape((TOKENS, TOP_WIN))
    route_weight = jnp.clip(jnp.exp(math.log(1.0) - 2.306499 * jax.random.uniform(keys[3], (TOKENS, TOP_WIN), jnp.float32) ** steps_of(keys[3], (TOKENS, TOP_WIN), ((0, 32),), -0.2, 0.2)), 0.099609375, 1.0).astype(jnp.bfloat16)
    w_gate = noise(keys[4], (EXPERTS_WIN, D, FF), D ** -0.5, 0.125, ((0, 8), (1, 4)))
    w_up = noise(keys[5], (EXPERTS_WIN, D, FF), D ** -0.5, 0.125, ((0, 8), (1, 4)))
    w_down = noise(keys[6], (EXPERTS_WIN, FF, D), FF ** -0.5, 0.21875, ((0, 8), (2, 4)))
    return {"tokens": tokens, "out_grad": out_grad, "expert_ids": expert_ids, "route_weight": route_weight, "w_gate": w_gate, "w_up": w_up, "w_down": w_down}


def reference(tokens, out_grad, expert_ids, route_weight, w_gate, w_up, w_down):
    group_routes = TOK_DEV * N_EXPERT * TOP_WIN
    row_limit = N_EXPERT * CAP
    all_routes = group_routes * N_DP
    all_tokens = TOK_DEV * N_EXPERT * N_DP
    flat_ids = expert_ids.reshape(N_DP, group_routes)
    flat_weights = route_weight.reshape(all_routes)

    def one_group(expert_index, group_index):
        picked = jnp.nonzero(flat_ids[group_index] == expert_index, size=row_limit, fill_value=-1)[0]
        valid = picked >= 0
        route_index = (group_index * group_routes + jnp.maximum(picked, 0)).astype(jnp.int32)
        token_index = (route_index // TOP_WIN).astype(jnp.int32)
        rows_in = jnp.where(valid[:, None], tokens[token_index], jnp.zeros((), tokens.dtype))
        rows_grad = jnp.where(valid[:, None], out_grad[token_index], jnp.zeros((), out_grad.dtype))
        weights = jnp.where(valid, flat_weights[route_index], jnp.zeros((), route_weight.dtype))
        gate_w = w_gate[expert_index]
        up_w = w_up[expert_index]
        down_w = w_down[expert_index]
        gate_value = jnp.dot(rows_in, gate_w, preferred_element_type=jnp.float32)
        up_value = jnp.dot(rows_in, up_w, preferred_element_type=jnp.float32)
        sigmoid_gate = jax.nn.sigmoid(gate_value)
        activated = gate_value * sigmoid_gate
        hidden = (activated * up_value).astype(jnp.bfloat16)
        expert_out = jnp.dot(hidden, down_w, preferred_element_type=jnp.float32)
        route_dot = jnp.sum(expert_out * rows_grad.astype(jnp.float32), axis=1).astype(jnp.bfloat16)
        scaled = (weights.astype(jnp.float32)[:, None] * rows_grad.astype(jnp.float32)).astype(jnp.bfloat16)
        hidden_grad = jnp.dot(scaled, down_w.T, preferred_element_type=jnp.float32)
        gate_delta = (hidden_grad * up_value * sigmoid_gate * (1.0 + gate_value * (1.0 - sigmoid_gate))).astype(jnp.bfloat16)
        up_delta = (hidden_grad * activated).astype(jnp.bfloat16)
        input_grad = (jnp.dot(gate_delta, gate_w.T, preferred_element_type=jnp.float32)
                      + jnp.dot(up_delta, up_w.T, preferred_element_type=jnp.float32)).astype(jnp.bfloat16)
        gate_part = jnp.dot(rows_in.T, gate_delta, preferred_element_type=jnp.float32).astype(jnp.bfloat16)
        up_part = jnp.dot(rows_in.T, up_delta, preferred_element_type=jnp.float32).astype(jnp.bfloat16)
        down_part = jnp.dot(hidden.T, scaled, preferred_element_type=jnp.float32).astype(jnp.bfloat16)
        target = jnp.where(valid, route_index, all_routes).astype(jnp.int32)
        return target, input_grad, route_dot, gate_part, up_part, down_part

    def one_expert(totals, expert_index):
        route_rows, route_dots = totals

        def group_step(group_index):
            return one_group(expert_index, group_index)

        target, input_grad, route_dot, gate_part, up_part, down_part = lax.map(group_step, jnp.arange(N_DP, dtype=jnp.int32))
        flat_target = target.reshape(-1)
        route_rows = route_rows.at[flat_target].set(input_grad.reshape(-1, D), mode="drop")
        route_dots = route_dots.at[flat_target].set(route_dot.reshape(-1), mode="drop")
        gate_sum = jnp.sum(gate_part.astype(jnp.float32), axis=0).astype(jnp.bfloat16)
        up_sum = jnp.sum(up_part.astype(jnp.float32), axis=0).astype(jnp.bfloat16)
        down_sum = jnp.sum(down_part.astype(jnp.float32), axis=0).astype(jnp.bfloat16)
        return (route_rows, route_dots), (gate_sum, up_sum, down_sum)

    start_rows = (jnp.zeros((all_routes, D), jnp.bfloat16), jnp.zeros((all_routes,), jnp.bfloat16))
    finals, grads = lax.scan(one_expert, start_rows, jnp.arange(EXPERTS_WIN, dtype=jnp.int32))
    route_rows, route_dots = finals
    gate_grad, up_grad, down_grad = grads
    token_grad = jnp.sum(route_rows.astype(jnp.float32).reshape(all_tokens, TOP_WIN, D), axis=1).astype(jnp.bfloat16)
    route_grad = route_dots.reshape(all_tokens, TOP_WIN)
    return (token_grad, route_grad, gate_grad, up_grad, down_grad)
```

```python
import functools
import jax
import jax.numpy as jnp
from jax import lax
from jax.experimental import pallas as pl
from jax.experimental.pallas import tpu as pltpu
from jax.sharding import PartitionSpec as P


MESH = pl.DeviceIdType.MESH
BF16 = jnp.bfloat16
F32 = jnp.float32


def dot(left, right, over_left=1, over_right=0):
    return lax.dot_general(
        left, right, (((over_left,), (over_right,)), ((), ())), preferred_element_type=F32
    )


class Chain:
    def __init__(self):
        self.g = lax.axis_index("dp")
        self.me = lax.axis_index("expert")
        self.c = self.me % 2
        self.z = self.me // 2
        self.half = self.z // 2
        self.far = 1 - self.half
        self.is_mid = (self.z + self.half) % 2 == 1
        self.is_end = (self.z + self.half) % 2 == 0
        self.z_mid = 1 + self.half
        self.z_end = 3 * self.half
        self.z_far_mid = 1 + self.far
        self.z_far_end = 3 * self.far
        self.z_near = self.z_mid + self.z_end - self.z

    def at(self, z, c):
        return (self.g, 2 * z + c)


def greet(chain, ranks, groups):
    barrier = pltpu.get_barrier_semaphore()
    for step in range(1, ranks):
        pl.semaphore_signal(
            barrier, inc=1, device_id=(chain.g, (chain.me + step) % ranks), device_id_type=MESH
        )
    for step in range(1, groups):
        pl.semaphore_signal(
            barrier, inc=1, device_id=((chain.g + step) % groups, chain.me), device_id_type=MESH
        )
    pl.semaphore_wait(barrier, ranks + groups - 2)


def neighbours(g):
    along_x = g + 1 - 2 * (g % 2)
    along_y = (g + 2) % 4
    return along_x, along_y


def send(src, dst, send_sem, recv_sem, device):
    return pltpu.make_async_remote_copy(
        src_ref=src, dst_ref=dst, send_sem=send_sem, recv_sem=recv_sem,
        device_id=device, device_id_type=MESH,
    )


def forward_kernel(
    cap,
    ids_ref, weight_ref, tokens_ref, grads_ref, wg_ref, wu_ref, wd_ref,
    full_gate_out, full_up_out, rows_out, hidden_out, gate_delta_out, up_delta_out, dots_out, table_out,
    raw, rows, stage_d, stage_e, full_gate, full_up, full_down, gate_val, up_val, hg_val, select,
    load_sem, raw_ss, raw_rs, e_ss, e_rs, d_ss, d_rs, tab_ss, tab_rs,
    w_ls, wa_ss, wa_rs, wf_ss, wf_rs, out_sem,
):
    chain = Chain()
    g, me, c, z = chain.g, chain.me, chain.c, chain.z
    is_mid, is_end = chain.is_mid, chain.is_end
    groups = lax.axis_size("dp")
    ranks = lax.axis_size("expert")
    steps = 2 * groups
    width = raw.shape[-1]
    count = raw.shape[2]
    slot_rows = rows.shape[2]
    along_x, along_y = neighbours(g)
    fulls = (full_gate, full_up, full_down)
    shards = (wg_ref, wu_ref, wd_ref)

    def load(k):
        source = tokens_ref if k < groups else grads_ref
        return pltpu.make_async_copy(
            source.at[:, pl.ds((k % groups) * width, width)], raw.at[0, k], load_sem.at[k]
        )

    for k in range(steps):
        load(k).start()
    for w in range(3):
        pltpu.make_async_copy(shards[w].at[0], fulls[w].at[g], w_ls.at[w]).start()

    greet(chain, ranks, groups)

    def shard_to(w, way):
        device = (along_x, me) if way == 0 else (along_y, me)
        return send(shards[w].at[0], fulls[w].at[g], wa_ss.at[w, way], wa_rs.at[w, way], device)

    def forward_half(w, way):
        owner = along_y if way == 0 else along_x
        device = (along_x, me) if way == 0 else (along_y, me)
        half = fulls[w].shape[1] // 2
        piece = fulls[w].at[owner, pl.ds(way * half, half)]
        return send(piece, piece, wf_ss.at[w, way], wf_rs.at[w, way], device)

    for w in range(3):
        for way in range(2):
            shard_to(w, way).start()

    experts = lax.broadcasted_iota(jnp.int32, (ranks, count), 0)
    named = [experts == ids_ref[k : k + 1, :] for k in range(ids_ref.shape[0])]
    hits = functools.reduce(jnp.logical_or, named)
    before = lax.broadcasted_iota(jnp.int32, (count, count), 0) < lax.broadcasted_iota(
        jnp.int32, (count, count), 1
    )
    order = dot(hits.astype(F32).astype(BF16), before.astype(F32).astype(BF16))
    table_out[0, 0:ranks, :] = jnp.where(hits, order, -1.0)
    weight = jnp.zeros((ranks, count), F32)
    for k in range(ids_ref.shape[0]):
        weight = jnp.where(named[k], weight_ref[k : k + 1, :], weight)
    table_out[0, ranks : 2 * ranks, :] = weight

    rows[:, :, cap:, :] = jnp.zeros((steps, ranks, slot_rows - cap, width), BF16)

    def table_send(slot, sem, zz):
        return send(
            table_out.at[0], table_out.at[slot], tab_ss.at[sem], tab_rs.at[slot - 1], chain.at(zz, c)
        )

    @pl.when(is_end)
    def _():
        table_send(1, 0, chain.z_mid).start()
        table_send(3, 1, chain.z_far_mid).start()

    @pl.when(is_mid)
    def _():
        table_send(2, 0, chain.z_far_mid).start()

    targets = (me, me + 1 - 2 * c, 2 * chain.z_near, 2 * chain.z_near + 1)

    def selectors(j):
        slots = lax.broadcasted_iota(jnp.int32, (slot_rows, count), 0).astype(F32)
        for i, rank in enumerate(targets):
            hit = table_out[j, pl.ds(rank, 1), :] == slots
            block = pl.ds(i * slot_rows, slot_rows)
            select[0, j, block, :] = jnp.where(hit, 1.0, 0.0).astype(BF16)
            select[1, j, block, :] = jnp.where(
                hit, table_out[j, pl.ds(ranks + rank, 1), :], 0.0
            ).astype(BF16)

    selectors(0)

    def gather(j, k, z_from, blocks, e_slot):
        picked = dot(select[k // groups, j, 0 : blocks * slot_rows, :], raw[j, k]).astype(BF16)
        parts = [picked[i * slot_rows : (i + 1) * slot_rows] for i in range(blocks)]
        rows[k, 4 * c + z_from] = parts[0]
        stage_d[k, z_from] = parts[1]
        for i in range(2, blocks):
            stage_e[k, i - 2, e_slot] = parts[i]

    full = pl.ds(0, cap)

    def own_raw(k):
        return send(raw.at[0, k], raw.at[2, k], raw_ss.at[0, k], raw_rs.at[1, k], chain.at(chain.z_far_mid, c))

    def end_raw(k):
        return send(raw.at[0, k], raw.at[1, k], raw_ss.at[0, k], raw_rs.at[0, k], chain.at(chain.z_mid, c))

    def onward_raw(k):
        return send(raw.at[1, k], raw.at[3, k], raw_ss.at[1, k], raw_rs.at[2, k], chain.at(chain.z_far_mid, c))

    def own_to_end(k, i):
        return send(
            stage_e.at[k, i, 0, full], rows.at[k, 4 * c + z, full],
            e_ss.at[k, 0, i], e_rs.at[k, 0, c], chain.at(chain.z_end, i),
        )

    def far_to_end(k, i):
        return send(
            stage_e.at[k, i, pl.ds(1, 2), full], rows.at[k, pl.ds(4 * c + 2 * chain.far, 2), full],
            e_ss.at[k, 1, i], e_rs.at[k, 1, c], chain.at(chain.z_end, i),
        )

    def mid_to_partner(k):
        return send(
            stage_d.at[k, :, full], rows.at[k, pl.ds(4 * c, 4), full], d_ss.at[k], d_rs.at[k], chain.at(z, 1 - c)
        )

    def end_to_partner(k):
        return send(
            stage_d.at[k, z, full], rows.at[k, 4 * c + z, full], d_ss.at[k], d_rs.at[k], chain.at(z, 1 - c)
        )

    def own_block_from(k, core):
        return send(
            stage_e.at[k, 0, 0, full], rows.at[k, 4 * core + chain.z_mid, full],
            e_ss.at[k, 0, 0], e_rs.at[k, 0, core], chain.at(chain.z_mid, core),
        )

    def far_blocks_from(k, core):
        return send(
            stage_e.at[k, 0, pl.ds(1, 2), full], rows.at[k, pl.ds(4 * core + 2 * chain.far, 2), full],
            e_ss.at[k, 1, 0], e_rs.at[k, 1, core], chain.at(chain.z_mid, core),
        )

    def landed(k):
        @pl.when(is_mid)
        def _():
            mid_to_partner(k).wait_recv()

        @pl.when(is_end)
        def _():
            end_to_partner(k).wait_recv()
            for core in range(2):
                own_block_from(k, core).wait_recv()
                far_blocks_from(k, core).wait_recv()

    def load_wait(k):
        pltpu.make_async_copy(
            tokens_ref.at[:, pl.ds(0, width)], raw.at[0, k], load_sem.at[k]
        ).wait()

    def step(k, carry):
        @pl.when(is_mid & (k < steps))
        def _():
            load_wait(k)
            own_raw(k).start()
            gather(0, k, z, 4, 0)
            own_to_end(k, 0).start()
            own_to_end(k, 1).start()

            @pl.when(k == 0)
            def _():
                table_send(1, 0, chain.z_mid).wait_recv()
                selectors(1)

            end_raw(k).wait_recv()
            onward_raw(k).start()
            gather(1, k, chain.z_end, 2, 0)

        @pl.when(is_mid & (k >= 1))
        def _():
            @pl.when(k == 1)
            def _():
                table_send(2, 0, chain.z_far_mid).wait_recv()
                table_send(3, 0, chain.z_far_mid).wait_recv()
                selectors(2)
                selectors(3)

            j = k - 1
            own_raw(j).wait_recv()
            gather(2, j, chain.z_far_mid, 4, 1 + chain.half)
            onward_raw(j).wait_recv()
            gather(3, j, chain.z_far_end, 4, 1 + chain.far)
            far_to_end(j, 0).start()
            far_to_end(j, 1).start()
            mid_to_partner(j).start()

        @pl.when(is_end & (k < steps))
        def _():
            load_wait(k)
            end_raw(k).start()
            gather(0, k, z, 2, 0)
            end_to_partner(k).start()

        for w in range(3):
            @pl.when(k == w + 1)
            def _():
                for way in range(2):
                    shard_to(w, 1 - way).wait_recv()
                    forward_half(w, way).start()

        @pl.when(k == groups + 1)
        def _():
            for kk in range(groups):
                landed(kk)
            for w in range(2):
                pltpu.make_async_copy(shards[w].at[0], fulls[w].at[g], w_ls.at[w]).wait()
                for way in range(2):
                    forward_half(w, way).wait_recv()

        @pl.when(k >= groups + 1)
        def _():
            b = 2 * (k - groups - 1)
            for half in range(2):
                block = b + half
                piece = [rows[kk, block] for kk in range(groups)]
                gate = functools.reduce(jnp.add, [dot(piece[kk], full_gate[kk]) for kk in range(groups)])
                up = functools.reduce(jnp.add, [dot(piece[kk], full_up[kk]) for kk in range(groups)])
                gate_val[block] = gate
                up_val[block] = up
                hidden_out[block] = (gate * jax.nn.sigmoid(gate) * up).astype(BF16)

        return carry

    lax.fori_loop(0, steps + 1, step, 0)

    outs = [
        pltpu.make_async_copy(full_gate, full_gate_out, out_sem.at[0]),
        pltpu.make_async_copy(full_up, full_up_out, out_sem.at[1]),
    ]
    for copy in outs:
        copy.start()
    first = pltpu.make_async_copy(rows.at[pl.ds(0, groups)], rows_out.at[pl.ds(0, groups)], out_sem.at[2])
    first.start()

    pltpu.make_async_copy(shards[2].at[0], fulls[2].at[g], w_ls.at[2]).wait()
    for way in range(2):
        forward_half(2, way).wait_recv()

    def hidden_grad(q, carry):
        landed(groups + q)
        pltpu.make_async_copy(rows.at[groups + q], rows_out.at[groups + q], out_sem.at[3 + q]).start()

        def tile(t, carry):
            value = dot(rows[groups + q, t], full_down[q], 1, 1)

            @pl.when(q == 0)
            def _():
                hg_val[t] = value

            @pl.when(q > 0)
            def _():
                hg_val[t] += value

            return carry

        return lax.fori_loop(0, ranks, tile, carry)

    lax.fori_loop(0, groups, hidden_grad, 0)

    def deltas(t, carry):
        gate, up, grad = gate_val[t], up_val[t], hg_val[t]
        sig = jax.nn.sigmoid(gate)
        gate_delta_out[t] = (grad * up * sig * (1.0 + gate * (1.0 - sig))).astype(BF16)
        up_delta_out[t] = (grad * (gate * sig)).astype(BF16)
        dots_out[t] = jnp.broadcast_to(
            jnp.sum(hidden_out[t].astype(F32) * grad, axis=1, keepdims=True), dots_out.shape[1:]
        )
        return carry

    lax.fori_loop(0, ranks, deltas, 0)

    for copy in outs:
        copy.wait()
    first.wait()
    for q in range(groups):
        pltpu.make_async_copy(rows.at[groups + q], rows_out.at[groups + q], out_sem.at[3 + q]).wait()
    for w in range(3):
        for way in range(2):
            shard_to(w, way).wait_send()
            forward_half(w, way).wait_send()

    def drain(k, carry):
        @pl.when(is_mid)
        def _():
            own_raw(k).wait_send()
            onward_raw(k).wait_send()
            for i in range(2):
                own_to_end(k, i).wait_send()
                far_to_end(k, i).wait_send()
            mid_to_partner(k).wait_send()

        @pl.when(is_end)
        def _():
            end_raw(k).wait_send()
            end_to_partner(k).wait_send()

        return carry

    lax.fori_loop(0, steps, drain, 0)

    @pl.when(is_mid)
    def _():
        table_send(2, 0, chain.z_far_mid).wait_send()

    @pl.when(is_end)
    def _():
        table_send(1, 0, chain.z_mid).wait_send()
        table_send(3, 1, chain.z_far_mid).wait_send()


def forward_call(ids_t, weight_t, tokens, out_grad, w_gate, w_up, w_down, cap):
    count, depth = tokens.shape
    groups, ranks = lax.axis_size("dp"), lax.axis_size("expert")
    inner = w_gate.shape[2]
    width = depth // groups
    slot_rows = -(-cap // 16) * 16
    steps = 2 * groups
    hbm = pl.BlockSpec(memory_space=pl.ANY)
    vmem = pl.BlockSpec(memory_space=pltpu.VMEM)
    dma = pltpu.SemaphoreType.DMA
    blocked = jax.ShapeDtypeStruct((ranks, slot_rows, inner), BF16)
    return pl.pallas_call(
        functools.partial(forward_kernel, cap),
        out_shape=(
            jax.ShapeDtypeStruct((groups, width, inner), BF16),
            jax.ShapeDtypeStruct((groups, width, inner), BF16),
            jax.ShapeDtypeStruct((steps, ranks, slot_rows, width), BF16),
            blocked, blocked, blocked,
            jax.ShapeDtypeStruct((ranks, slot_rows, 128), F32),
            jax.ShapeDtypeStruct((4, 2 * ranks, count), F32),
        ),
        in_specs=[vmem, vmem, hbm, hbm, hbm, hbm, hbm],
        out_specs=(hbm, hbm, hbm, vmem, vmem, vmem, vmem, vmem),
        scratch_shapes=[
            pltpu.VMEM((4, steps, count, width), BF16),
            pltpu.VMEM((steps, ranks, slot_rows, width), BF16),
            pltpu.VMEM((steps, 4, slot_rows, width), BF16),
            pltpu.VMEM((steps, 2, 3, slot_rows, width), BF16),
            pltpu.VMEM((groups, width, inner), BF16),
            pltpu.VMEM((groups, width, inner), BF16),
            pltpu.VMEM((groups, inner, width), BF16),
            pltpu.VMEM((ranks, slot_rows, inner), F32),
            pltpu.VMEM((ranks, slot_rows, inner), F32),
            pltpu.VMEM((ranks, slot_rows, inner), F32),
            pltpu.VMEM((2, 4, 4 * slot_rows, count), BF16),
            dma((steps,)), dma((2, steps)), dma((3, steps)), dma((steps, 2, 2)), dma((steps, 2, 2)),
            dma((steps,)), dma((steps,)), dma((2,)), dma((3,)),
            dma((3,)), dma((3, 2)), dma((3, 2)), dma((3, 2)), dma((3, 2)), dma((3 + groups,)),
        ],
        compiler_params=pltpu.CompilerParams(
            collective_id=0, has_side_effects=True, vmem_limit_bytes=67000000
        ),
    )(ids_t, weight_t, tokens, out_grad, w_gate, w_up, w_down)


def swap(block, axis, distance):
    ranks = lax.axis_size(axis)
    return lax.ppermute(block, axis, [(rank, rank ^ distance) for rank in range(ranks)])


def any_mesh(tokens, out_grad, expert_ids, route_weight, w_gate, w_up, w_down):
    tok_count = tokens.shape[0]
    route_count = expert_ids.shape[1]
    ranks = lax.axis_size("expert")
    groups = lax.axis_size("dp")
    me = lax.axis_index("expert")
    group = lax.axis_index("dp")
    capacity = 3 * tok_count * route_count // (2 * ranks)
    routes = tok_count * route_count
    total_slots = ranks * capacity
    full_gate = lax.all_gather(w_gate[0], "dp", axis=0, tiled=True)
    full_up = lax.all_gather(w_up[0], "dp", axis=0, tiled=True)
    full_down = lax.all_gather(w_down[0], "dp", axis=1, tiled=True)
    half = ranks // 2
    flat_ids = expert_ids.reshape(routes)
    one_hot = (flat_ids[:, None] == jnp.arange(ranks, dtype=jnp.int32)[None, :]).astype(jnp.int32)
    slot_order = jnp.sum((jnp.cumsum(one_hot, axis=0) - 1) * one_hot, axis=1)
    slot_order = slot_order.reshape(tok_count, route_count)
    routing = jnp.concatenate(
        [
            expert_ids.astype(jnp.float32),
            slot_order.astype(jnp.float32),
            route_weight.astype(jnp.float32),
        ],
        axis=1,
    )
    far_routing = swap(routing, "expert", half)
    far_ids = far_routing[:, :route_count].astype(jnp.int32)
    far_order = far_routing[:, route_count : 2 * route_count].astype(jnp.int32)
    far_weight = far_routing[:, 2 * route_count :].astype(jnp.bfloat16)
    far_tokens = swap(tokens, "expert", half)
    late_grad, slot_order = lax.optimization_barrier((out_grad, slot_order))
    far_grad = swap(late_grad, "expert", half)
    slots = jnp.arange(total_slots, dtype=jnp.int32)

    def selectors(destination, weight, count):
        picks = jnp.zeros((count, tok_count), jnp.bfloat16)
        weighted = jnp.zeros((count, tok_count), jnp.bfloat16)
        for k in range(route_count):
            hit = slots[:count, None] == destination[:, k][None, :]
            picks = jnp.where(hit, jnp.ones((), jnp.bfloat16), picks)
            weighted = jnp.where(hit, weight[:, k][None, :], weighted)
        return picks, weighted

    destination = (expert_ids ^ me) * capacity + slot_order
    far_destination = (far_ids ^ me) * capacity + far_order
    near_slots = half * capacity
    picks, _ = selectors(destination, route_weight, total_slots)
    near_picks, near_weighted = selectors(destination, route_weight, near_slots)
    far_picks, far_weighted = selectors(far_destination, far_weight, near_slots)

    def blocks(buffer, count=ranks):
        return [buffer[d * capacity : (d + 1) * capacity] for d in range(count)]

    def exchange(buffer, count=ranks):
        return [
            swap(block, "expert", d) if d else block for d, block in enumerate(blocks(buffer, count))
        ]

    rows_in = jnp.concatenate(
        exchange(dot(near_picks, tokens, 1, 0).astype(jnp.bfloat16), half)
        + exchange(dot(far_picks, far_tokens, 1, 0).astype(jnp.bfloat16), half)
    )
    gate_value = dot(rows_in, full_gate, 1, 0)
    up_value = dot(rows_in, full_up, 1, 0)
    sigmoid_gate = jax.nn.sigmoid(gate_value)
    activated = gate_value * sigmoid_gate
    hidden = (activated * up_value).astype(jnp.bfloat16)
    scaled_blocks = exchange(
        dot(near_weighted, late_grad, 1, 0).astype(jnp.bfloat16), half
    ) + exchange(dot(far_weighted, far_grad, 1, 0).astype(jnp.bfloat16), half)
    scaled_blocks, hidden = lax.optimization_barrier((scaled_blocks, hidden))
    scaled = jnp.concatenate(scaled_blocks)
    hidden_grad = dot(scaled, full_down, 1, 1)
    gate_delta = (
        hidden_grad * up_value * sigmoid_gate * (1.0 + gate_value * (1.0 - sigmoid_gate))
    ).astype(jnp.bfloat16)
    up_delta = (hidden_grad * activated).astype(jnp.bfloat16)
    input_grad = (
        dot(gate_delta, full_gate, 1, 1) + dot(up_delta, full_up, 1, 1)
    ).astype(jnp.bfloat16)
    back_blocks = []
    for d, block in enumerate(blocks(input_grad)):
        back_blocks.append(swap(block, "expert", d) if d else block)
    down_part = dot(hidden, scaled, 0, 0).astype(jnp.bfloat16)
    input_grad, rows_in, hidden = lax.optimization_barrier((input_grad, rows_in, hidden))
    expert_out = dot(hidden, full_down, 1, 0)
    weighted_dot = jnp.sum(expert_out * scaled.astype(jnp.float32), axis=1)
    gate_part = dot(rows_in, gate_delta, 0, 0).astype(jnp.bfloat16)
    up_part = dot(rows_in, up_delta, 0, 0).astype(jnp.bfloat16)
    down_grad = lax.psum_scatter(down_part, "dp", scatter_dimension=1, tiled=True)[None]
    gate_grad = lax.psum_scatter(gate_part, "dp", scatter_dimension=0, tiled=True)[None]
    depth = up_part.shape[0] // groups
    up_sum = jnp.zeros((depth, up_part.shape[1]), jnp.float32)
    for d in range(groups):
        piece = lax.dynamic_slice_in_dim(up_part, (group ^ d) * depth, depth, 0)
        up_sum = up_sum + (swap(piece, "dp", d) if d else piece).astype(jnp.float32)
    up_grad = up_sum.astype(jnp.bfloat16)[None]

    token_sum = jnp.zeros(tokens.shape, jnp.float32)
    for pick, block in zip(blocks(picks), back_blocks):
        token_sum = token_sum + dot(pick, block, 0, 0)
    token_grad = token_sum.astype(jnp.bfloat16)

    order = jnp.arange(ranks, dtype=jnp.int32)
    dots = weighted_dot.reshape(ranks, capacity)
    by_rank = jnp.sum(
        jnp.where(((order ^ me)[:, None] == order[None, :])[:, :, None], dots[None], 0.0), axis=1
    )
    back_dots = lax.all_to_all(by_rank, "expert", split_axis=0, concat_axis=0, tiled=True)
    arrival = expert_ids * capacity + slot_order
    hits = arrival.reshape(tok_count, route_count, 1) == slots[None, None, :]
    own_dots = jnp.sum(jnp.where(hits, back_dots.reshape(total_slots)[None, None, :], 0.0), axis=2)
    route_grad = (own_dots / route_weight.astype(jnp.float32)).astype(jnp.bfloat16)
    return (token_grad, route_grad, gate_grad, up_grad, down_grad)


def on_device(tokens, out_grad, expert_ids, route_weight, w_gate, w_up, w_down):
    count, depth = tokens.shape
    top = expert_ids.shape[1]
    groups, ranks = lax.axis_size("dp"), lax.axis_size("expert")
    cap = 3 * count * top // (2 * ranks)
    fg, fu, rows, hidden, gd, ud, dots, table = forward_call(
        expert_ids.T, route_weight.T.astype(F32), tokens, out_grad, w_gate, w_up, w_down, cap)
    slot_rows = rows.shape[2]
    total = ranks * slot_rows
    inner = w_gate.shape[2]
    perm = [4 * (r % 2) + r // 2 for r in range(ranks)]
    perm = jnp.array(perm)
    x = rows[:groups].transpose(1, 2, 0, 3).reshape(ranks, slot_rows, depth)[perm].reshape(total, depth)
    sc = rows[groups:].transpose(1, 2, 0, 3).reshape(ranks, slot_rows, depth)[perm].reshape(total, depth)
    hidden, gd, ud = [v[perm].reshape(total, inner) for v in (hidden, gd, ud)]
    dots = dots[:, :, 0][perm]
    full_gate, full_up = fg.reshape(depth, inner), fu.reshape(depth, inner)
    gate_part = dot(x, gd, 0, 0).astype(BF16)
    up_part = dot(x, ud, 0, 0).astype(BF16)
    down_part = dot(hidden, sc, 0, 0).astype(BF16)
    down_grad = lax.psum_scatter(down_part, "dp", scatter_dimension=1, tiled=True)[None]
    gate_grad = lax.psum_scatter(gate_part, "dp", scatter_dimension=0, tiled=True)[None]
    up_grad = lax.psum_scatter(up_part, "dp", scatter_dimension=0, tiled=True)[None]
    ig = (dot(gd, full_gate, 1, 1) + dot(ud, full_up, 1, 1)).astype(BF16).reshape(ranks, slot_rows, depth)
    back = lax.all_to_all(ig, "expert", split_axis=0, concat_axis=0, tiled=True)
    back_dots = lax.all_to_all(dots, "expert", split_axis=0, concat_axis=0, tiled=True)
    slot = table[0, :ranks]
    pick = (slot[:, None, :] == jnp.arange(slot_rows, dtype=F32)[None, :, None])
    token_grad = dot(pick.astype(BF16).reshape(total, count), back.reshape(total, depth), 0, 0).astype(BF16)
    val = jnp.sum(jnp.where(pick, back_dots[:, :, None], 0.0), axis=1)
    hit = expert_ids.T[:, None, :] == jnp.arange(ranks)[None, :, None]
    rg = jnp.sum(jnp.where(hit, val[None], 0.0), axis=1).T
    route_grad = (rg / route_weight.astype(F32)).astype(BF16)
    return token_grad, route_grad, gate_grad, up_grad, down_grad


def solution(mesh):
    placed = (
        P(("dp", "expert"), None),
        P(("dp", "expert"), None),
        P(("dp", "expert"), None),
        P(("dp", "expert"), None),
        P("expert", "dp", None),
        P("expert", "dp", None),
        P("expert", None, "dp"),
    )
    chained = mesh.shape["expert"] == 8 and mesh.shape["dp"] == 4
    return jax.shard_map(
        on_device if chained else any_mesh, mesh=mesh, in_specs=placed,
        out_specs=(
            P(("dp", "expert"), None),
            P(("dp", "expert"), None),
            P("expert", "dp", None),
            P("expert", "dp", None),
            P("expert", None, "dp"),
        ),
        check_vma=False,
    )
```

```python
import functools
import jax
import jax.numpy as jnp
from jax import lax
from jax.experimental import pallas as pl
from jax.experimental.pallas import tpu as pltpu
from jax.sharding import PartitionSpec as P


MESH = pl.DeviceIdType.MESH
BF16 = jnp.bfloat16
F32 = jnp.float32


def dot(left, right, over_left=1, over_right=0):
    return lax.dot_general(
        left, right, (((over_left,), (over_right,)), ((), ())), preferred_element_type=F32
    )


class Chain:
    def __init__(self):
        self.g = lax.axis_index("dp")
        self.me = lax.axis_index("expert")
        self.c = self.me % 2
        self.z = self.me // 2
        self.half = self.z // 2
        self.far = 1 - self.half
        self.is_mid = (self.z + self.half) % 2 == 1
        self.is_end = (self.z + self.half) % 2 == 0
        self.z_mid = 1 + self.half
        self.z_end = 3 * self.half
        self.z_far_mid = 1 + self.far
        self.z_far_end = 3 * self.far
        self.z_near = self.z_mid + self.z_end - self.z

    def at(self, z, c):
        return (self.g, 2 * z + c)


def greet(chain, ranks, groups):
    barrier = pltpu.get_barrier_semaphore()
    for step in range(1, ranks):
        pl.semaphore_signal(
            barrier, inc=1, device_id=(chain.g, (chain.me + step) % ranks), device_id_type=MESH
        )
    for step in range(1, groups):
        pl.semaphore_signal(
            barrier, inc=1, device_id=((chain.g + step) % groups, chain.me), device_id_type=MESH
        )
    pl.semaphore_wait(barrier, ranks + groups - 2)


def neighbours(g):
    along_x = g + 1 - 2 * (g % 2)
    along_y = (g + 2) % 4
    return along_x, along_y


def send(src, dst, send_sem, recv_sem, device):
    return pltpu.make_async_remote_copy(
        src_ref=src, dst_ref=dst, send_sem=send_sem, recv_sem=recv_sem,
        device_id=device, device_id_type=MESH,
    )


def forward_kernel(
    cap,
    ids_ref, weight_ref, tokens_ref, grads_ref, wg_ref, wu_ref, wd_ref,
    full_out, rows_out, hidden_out, delta_out, dots_out, table_out,
    raw, rows, stage_d, stage_e, full_gate, full_up, full_down, gate_val, up_val, hg_val, select,
    load_sem, raw_ss, raw_rs, e_ss, e_rs, d_ss, d_rs, tab_ss, tab_rs,
    w_ls, wa_ss, wa_rs, wf_ss, wf_rs, out_sem,
):
    chain = Chain()
    g, me, c, z = chain.g, chain.me, chain.c, chain.z
    is_mid, is_end = chain.is_mid, chain.is_end
    groups = lax.axis_size("dp")
    ranks = lax.axis_size("expert")
    steps = 2 * groups
    width = raw.shape[-1]
    count = raw.shape[2]
    slot_rows = rows.shape[2]
    along_x, along_y = neighbours(g)
    fulls = (full_gate, full_up, full_down)
    shards = (wg_ref, wu_ref, wd_ref)

    def load(k):
        source = tokens_ref if k < groups else grads_ref
        return pltpu.make_async_copy(
            source.at[:, pl.ds((k % groups) * width, width)], raw.at[0, k], load_sem.at[k]
        )

    for k in range(steps):
        load(k).start()
    for w in range(3):
        pltpu.make_async_copy(shards[w].at[0], fulls[w].at[g], w_ls.at[w]).start()

    greet(chain, ranks, groups)

    def shard_to(w, way):
        device = (along_x, me) if way == 0 else (along_y, me)
        return send(shards[w].at[0], fulls[w].at[g], wa_ss.at[w, way], wa_rs.at[w, way], device)

    def forward_half(w, way):
        owner = along_y if way == 0 else along_x
        device = (along_x, me) if way == 0 else (along_y, me)
        half = fulls[w].shape[1] // 2
        piece = fulls[w].at[owner, pl.ds(way * half, half)]
        return send(piece, piece, wf_ss.at[w, way], wf_rs.at[w, way], device)

    for w in range(3):
        for way in range(2):
            shard_to(w, way).start()

    experts = lax.broadcasted_iota(jnp.int32, (ranks, count), 0)
    named = [experts == ids_ref[k : k + 1, :] for k in range(ids_ref.shape[0])]
    hits = functools.reduce(jnp.logical_or, named)
    before = lax.broadcasted_iota(jnp.int32, (count, count), 0) < lax.broadcasted_iota(
        jnp.int32, (count, count), 1
    )
    order = dot(hits.astype(F32).astype(BF16), before.astype(F32).astype(BF16))
    table_out[0, 0:ranks, :] = jnp.where(hits, order, -1.0)
    weight = jnp.zeros((ranks, count), F32)
    for k in range(ids_ref.shape[0]):
        weight = jnp.where(named[k], weight_ref[k : k + 1, :], weight)
    table_out[0, ranks : 2 * ranks, :] = weight

    rows[:, :, cap:, :] = jnp.zeros((steps, ranks, slot_rows - cap, width), BF16)

    def table_send(slot, sem, zz):
        return send(
            table_out.at[0], table_out.at[slot], tab_ss.at[sem], tab_rs.at[slot - 1], chain.at(zz, c)
        )

    @pl.when(is_end)
    def _():
        table_send(1, 0, chain.z_mid).start()
        table_send(3, 1, chain.z_far_mid).start()

    @pl.when(is_mid)
    def _():
        table_send(2, 0, chain.z_far_mid).start()

    targets = (me, me + 1 - 2 * c, 2 * chain.z_near, 2 * chain.z_near + 1)

    def selectors(j):
        slots = lax.broadcasted_iota(jnp.int32, (slot_rows, count), 0).astype(F32)
        for i, rank in enumerate(targets):
            hit = table_out[j, pl.ds(rank, 1), :] == slots
            block = pl.ds(i * slot_rows, slot_rows)
            select[0, j, block, :] = jnp.where(hit, 1.0, 0.0).astype(BF16)
            select[1, j, block, :] = jnp.where(
                hit, table_out[j, pl.ds(ranks + rank, 1), :], 0.0
            ).astype(BF16)

    selectors(0)

    def gather(j, k, z_from, blocks, e_slot):
        picked = dot(select[k // groups, j, 0 : blocks * slot_rows, :], raw[j, k]).astype(BF16)
        parts = [picked[i * slot_rows : (i + 1) * slot_rows] for i in range(blocks)]
        rows[k, 4 * c + z_from] = parts[0]
        stage_d[k, z_from] = parts[1]
        for i in range(2, blocks):
            stage_e[k, i - 2, e_slot] = parts[i]

    full = pl.ds(0, cap)

    def own_raw(k):
        return send(raw.at[0, k], raw.at[2, k], raw_ss.at[0, k], raw_rs.at[1, k], chain.at(chain.z_far_mid, c))

    def end_raw(k):
        return send(raw.at[0, k], raw.at[1, k], raw_ss.at[0, k], raw_rs.at[0, k], chain.at(chain.z_mid, c))

    def onward_raw(k):
        return send(raw.at[1, k], raw.at[3, k], raw_ss.at[1, k], raw_rs.at[2, k], chain.at(chain.z_far_mid, c))

    def own_to_end(k, i):
        return send(
            stage_e.at[k, i, 0, full], rows.at[k, 4 * c + z, full],
            e_ss.at[k, 0, i], e_rs.at[k, 0, c], chain.at(chain.z_end, i),
        )

    def far_to_end(k, i):
        return send(
            stage_e.at[k, i, pl.ds(1, 2), full], rows.at[k, pl.ds(4 * c + 2 * chain.far, 2), full],
            e_ss.at[k, 1, i], e_rs.at[k, 1, c], chain.at(chain.z_end, i),
        )

    def mid_to_partner(k):
        return send(
            stage_d.at[k, :, full], rows.at[k, pl.ds(4 * c, 4), full], d_ss.at[k], d_rs.at[k], chain.at(z, 1 - c)
        )

    def end_to_partner(k):
        return send(
            stage_d.at[k, z, full], rows.at[k, 4 * c + z, full], d_ss.at[k], d_rs.at[k], chain.at(z, 1 - c)
        )

    def own_block_from(k, core):
        return send(
            stage_e.at[k, 0, 0, full], rows.at[k, 4 * core + chain.z_mid, full],
            e_ss.at[k, 0, 0], e_rs.at[k, 0, core], chain.at(chain.z_mid, core),
        )

    def far_blocks_from(k, core):
        return send(
            stage_e.at[k, 0, pl.ds(1, 2), full], rows.at[k, pl.ds(4 * core + 2 * chain.far, 2), full],
            e_ss.at[k, 1, 0], e_rs.at[k, 1, core], chain.at(chain.z_mid, core),
        )

    def landed(k):
        @pl.when(is_mid)
        def _():
            mid_to_partner(k).wait_recv()

        @pl.when(is_end)
        def _():
            end_to_partner(k).wait_recv()
            for core in range(2):
                own_block_from(k, core).wait_recv()
                far_blocks_from(k, core).wait_recv()

    def load_wait(k):
        pltpu.make_async_copy(
            tokens_ref.at[:, pl.ds(0, width)], raw.at[0, k], load_sem.at[k]
        ).wait()

    def step(k, carry):
        @pl.when(is_mid & (k < steps))
        def _():
            load_wait(k)
            own_raw(k).start()
            gather(0, k, z, 4, 0)
            own_to_end(k, 0).start()
            own_to_end(k, 1).start()

            @pl.when(k == 0)
            def _():
                table_send(1, 0, chain.z_mid).wait_recv()
                selectors(1)

            end_raw(k).wait_recv()
            onward_raw(k).start()
            gather(1, k, chain.z_end, 2, 0)

        @pl.when(is_mid & (k >= 1))
        def _():
            @pl.when(k == 1)
            def _():
                table_send(2, 0, chain.z_far_mid).wait_recv()
                table_send(3, 0, chain.z_far_mid).wait_recv()
                selectors(2)
                selectors(3)

            j = k - 1
            own_raw(j).wait_recv()
            gather(2, j, chain.z_far_mid, 4, 1 + chain.half)
            onward_raw(j).wait_recv()
            gather(3, j, chain.z_far_end, 4, 1 + chain.far)
            far_to_end(j, 0).start()
            far_to_end(j, 1).start()
            mid_to_partner(j).start()

        @pl.when(is_end & (k < steps))
        def _():
            load_wait(k)
            end_raw(k).start()
            gather(0, k, z, 2, 0)
            end_to_partner(k).start()

        for w in range(3):
            @pl.when(k == w + 1)
            def _():
                for way in range(2):
                    shard_to(w, 1 - way).wait_recv()
                    forward_half(w, way).start()

        @pl.when(k == groups + 1)
        def _():
            for kk in range(groups):
                landed(kk)
            for w in range(2):
                pltpu.make_async_copy(shards[w].at[0], fulls[w].at[g], w_ls.at[w]).wait()
                for way in range(2):
                    forward_half(w, way).wait_recv()

        @pl.when(k >= groups + 1)
        def _():
            pair = pl.ds(2 * (k - groups - 1), 2)
            shape = (2, slot_rows, gate_val.shape[2])
            piece = [rows[kk, pair].reshape(2 * slot_rows, width) for kk in range(groups)]
            gate = functools.reduce(jnp.add, [dot(piece[kk], full_gate[kk]) for kk in range(groups)])
            up = functools.reduce(jnp.add, [dot(piece[kk], full_up[kk]) for kk in range(groups)])
            gate_val[pair] = gate.reshape(shape)
            up_val[pair] = up.reshape(shape)
            hidden_out[pair] = (gate * jax.nn.sigmoid(gate) * up).astype(BF16).reshape(shape)

        return carry

    lax.fori_loop(0, steps + 1, step, 0)

    outs = [
        pltpu.make_async_copy(full_gate, full_out.at[0], out_sem.at[0]),
        pltpu.make_async_copy(full_up, full_out.at[1], out_sem.at[1]),
    ]
    for copy in outs:
        copy.start()
    first = pltpu.make_async_copy(rows.at[pl.ds(0, groups)], rows_out.at[pl.ds(0, groups)], out_sem.at[2])
    first.start()

    pltpu.make_async_copy(shards[2].at[0], fulls[2].at[g], w_ls.at[2]).wait()
    for way in range(2):
        forward_half(2, way).wait_recv()

    def hidden_grad(q, carry):
        landed(groups + q)
        pltpu.make_async_copy(rows.at[groups + q], rows_out.at[groups + q], out_sem.at[3 + q]).start()

        def tile(t, carry):
            four = pl.ds(4 * t, 4)
            left = rows[groups + q, four].reshape(4 * slot_rows, width)
            value = dot(left, full_down[q], 1, 1).reshape(4, slot_rows, hg_val.shape[2])

            @pl.when(q == 0)
            def _():
                hg_val[four] = value

            @pl.when(q > 0)
            def _():
                hg_val[four] += value

            return carry

        return lax.fori_loop(0, ranks // 4, tile, carry)

    lax.fori_loop(0, groups, hidden_grad, 0)

    def deltas(t, carry):
        gate, up, grad = gate_val[t], up_val[t], hg_val[t]
        sig = jax.nn.sigmoid(gate)
        delta_out[0, t] = (grad * up * sig * (1.0 + gate * (1.0 - sig))).astype(BF16)
        delta_out[1, t] = (grad * (gate * sig)).astype(BF16)
        total = jnp.sum(hidden_out[t].astype(F32) * grad, axis=1, keepdims=True)
        dots_out[t] = jnp.broadcast_to(total, (total.shape[0], total.shape[0])).T[0:8, :]
        return carry

    lax.fori_loop(0, ranks, deltas, 0)

    for copy in outs:
        copy.wait()
    first.wait()
    for q in range(groups):
        pltpu.make_async_copy(rows.at[groups + q], rows_out.at[groups + q], out_sem.at[3 + q]).wait()
    for w in range(3):
        for way in range(2):
            shard_to(w, way).wait_send()
            forward_half(w, way).wait_send()

    def drain(k, carry):
        @pl.when(is_mid)
        def _():
            own_raw(k).wait_send()
            onward_raw(k).wait_send()
            for i in range(2):
                own_to_end(k, i).wait_send()
                far_to_end(k, i).wait_send()
            mid_to_partner(k).wait_send()

        @pl.when(is_end)
        def _():
            end_raw(k).wait_send()
            end_to_partner(k).wait_send()

        return carry

    lax.fori_loop(0, steps, drain, 0)

    @pl.when(is_mid)
    def _():
        table_send(2, 0, chain.z_far_mid).wait_send()

    @pl.when(is_end)
    def _():
        table_send(1, 0, chain.z_mid).wait_send()
        table_send(3, 1, chain.z_far_mid).wait_send()


def forward_call(ids_t, weight_t, tokens, out_grad, w_gate, w_up, w_down, cap):
    count, depth = tokens.shape
    groups, ranks = lax.axis_size("dp"), lax.axis_size("expert")
    inner = w_gate.shape[2]
    width = depth // groups
    slot_rows = -(-cap // 16) * 16
    steps = 2 * groups
    hbm = pl.BlockSpec(memory_space=pl.ANY)
    vmem = pl.BlockSpec(memory_space=pltpu.VMEM)
    dma = pltpu.SemaphoreType.DMA
    return pl.pallas_call(
        functools.partial(forward_kernel, cap),
        out_shape=(
            jax.ShapeDtypeStruct((2, groups, width, inner), BF16),
            jax.ShapeDtypeStruct((steps, ranks, slot_rows, width), BF16),
            jax.ShapeDtypeStruct((ranks, slot_rows, inner), BF16),
            jax.ShapeDtypeStruct((2, ranks, slot_rows, inner), BF16),
            jax.ShapeDtypeStruct((ranks, 8, slot_rows), F32),
            jax.ShapeDtypeStruct((4, 2 * ranks, count), F32),
        ),
        in_specs=[vmem, vmem, hbm, hbm, hbm, hbm, hbm],
        out_specs=(hbm, hbm, vmem, vmem, vmem, vmem),
        scratch_shapes=[
            pltpu.VMEM((4, steps, count, width), BF16),
            pltpu.VMEM((steps, ranks, slot_rows, width), BF16),
            pltpu.VMEM((steps, 4, slot_rows, width), BF16),
            pltpu.VMEM((steps, 2, 3, slot_rows, width), BF16),
            pltpu.VMEM((groups, width, inner), BF16),
            pltpu.VMEM((groups, width, inner), BF16),
            pltpu.VMEM((groups, inner, width), BF16),
            pltpu.VMEM((ranks, slot_rows, inner), F32),
            pltpu.VMEM((ranks, slot_rows, inner), F32),
            pltpu.VMEM((ranks, slot_rows, inner), F32),
            pltpu.VMEM((2, 4, 4 * slot_rows, count), BF16),
            dma((steps,)), dma((2, steps)), dma((3, steps)), dma((steps, 2, 2)), dma((steps, 2, 2)),
            dma((steps,)), dma((steps,)), dma((2,)), dma((3,)),
            dma((3,)), dma((3, 2)), dma((3, 2)), dma((3, 2)), dma((3, 2)), dma((3 + groups,)),
        ],
        compiler_params=pltpu.CompilerParams(
            collective_id=0, has_side_effects=True, vmem_limit_bytes=67000000
        ),
    )(ids_t, weight_t, tokens, out_grad, w_gate, w_up, w_down)


def backward_kernel(
    cap,
    ids_ref, weight_ref, table_ref, dots_ref, full_ref, rows_ref, hidden_ref, delta_ref,
    token_out, route_out, gate_out, up_out, down_out,
    full, rows, hidden, delta, grads, comb, gf_send, gf_in, end_send, select,
    diag_gu, diag_d, pair_gu, pair_d, relay_gu, relay_d, in_gu, in_d, dots_in,
    load_sem, d_ss, d_rs, far_ss, far_rs, near_ss, near_rs, gf_ss, gf_rs, es_ss, es_rs,
    dots_ss, dots_rs, relay_ss, relay_rs, pair_ss, pair_rs,
):
    chain = Chain()
    g, me, c, z = chain.g, chain.me, chain.c, chain.z
    is_mid, is_end = chain.is_mid, chain.is_end
    groups = lax.axis_size("dp")
    ranks = lax.axis_size("expert")
    _, slot_rows, width = rows.shape[1:]
    count = table_ref.shape[2]
    inner = hidden.shape[2]
    along_x, along_y = neighbours(g)
    across = groups - 1 - g
    slots = ranks * slot_rows

    loads = [
        pltpu.make_async_copy(delta_ref, delta, load_sem.at[0]),
        pltpu.make_async_copy(rows_ref.at[across], rows.at[across], load_sem.at[1]),
        pltpu.make_async_copy(full_ref.at[:, 0], full.at[:, 0], load_sem.at[2]),
        pltpu.make_async_copy(hidden_ref, hidden, load_sem.at[3]),
        pltpu.make_async_copy(rows_ref.at[groups + across], rows.at[groups + across], load_sem.at[4]),
        pltpu.make_async_copy(full_ref.at[:, pl.ds(1, groups - 1)], full.at[:, pl.ds(1, groups - 1)], load_sem.at[5]),
    ]
    for i, shard in enumerate((along_x, along_y, g)):
        loads.append(pltpu.make_async_copy(rows_ref.at[shard], rows.at[shard], load_sem.at[6 + i]))
        loads.append(
            pltpu.make_async_copy(rows_ref.at[groups + shard], rows.at[groups + shard], load_sem.at[9 + i])
        )
    for copy in loads:
        copy.start()

    greet(chain, ranks, groups)

    real = pl.ds(0, cap)

    def dots_to(peer):
        return send(
            dots_ref.at[4 * (peer % 2) + peer // 2], dots_in.at[me],
            dots_ss.at[peer], dots_rs.at[me], (g, peer),
        )

    def dots_from(peer):
        return send(
            dots_ref.at[4 * c + z], dots_in.at[peer], dots_ss.at[peer], dots_rs.at[peer], (g, peer)
        )

    for step in range(1, ranks):
        dots_to((me + step) % ranks).start()

    comb[:, :, :, cap:, :] = jnp.zeros((groups, 4, 4, slot_rows - cap, width), BF16)
    targets = (me, me + 1 - 2 * c, 2 * chain.z_near, 2 * chain.z_near + 1)

    def selectors(j, z_from):
        slot = lax.broadcasted_iota(jnp.int32, (slot_rows, count), 0).astype(F32)
        for i, rank in enumerate(targets):
            hit = table_ref[j, pl.ds(rank, 1), :] == slot
            select[z_from, i * slot_rows : (i + 1) * slot_rows, :] = jnp.where(hit, 1.0, 0.0).astype(BF16)

    selectors(0, z)

    @pl.when(is_mid)
    def _():
        selectors(1, chain.z_end)
        selectors(2, chain.z_far_mid)
        selectors(3, chain.z_far_end)

    def to_partner(k):
        return send(
            grads.at[k, pl.ds(4 * (1 - c), 4), real], comb.at[k, :, 1, real],
            d_ss.at[k], d_rs.at[k], chain.at(z, 1 - c),
        )

    def end_to_partner(k):
        return send(
            grads.at[k, 4 * (1 - c) + z, real], comb.at[k, z, 1, real],
            d_ss.at[k], d_rs.at[k], chain.at(z, 1 - c),
        )

    def far_home(k, core):
        return send(
            grads.at[k, pl.ds(4 * core + 2 * chain.far, 2), real],
            comb.at[k, pl.ds(2 * chain.far, 2), 2 + c, real],
            far_ss.at[k, core], far_rs.at[k, c], chain.at(chain.z_mid, core),
        )

    def far_from(k, core):
        return send(
            grads.at[k, pl.ds(4 * core + 2 * chain.far, 2), real],
            comb.at[k, pl.ds(2 * chain.far, 2), 2 + core, real],
            far_ss.at[k, core], far_rs.at[k, core], chain.at(chain.z_end, core),
        )

    def near_home(k, core):
        return send(
            grads.at[k, 4 * core + chain.z_mid, real], comb.at[k, chain.z_mid, 2 + c, real],
            near_ss.at[k, core], near_rs.at[k, c], chain.at(chain.z_mid, core),
        )

    def near_from(k, core):
        return send(
            grads.at[k, 4 * core + chain.z_mid, real], comb.at[k, chain.z_mid, 2 + core, real],
            near_ss.at[k, core], near_rs.at[k, core], chain.at(chain.z_end, core),
        )

    def sums_across(k):
        return send(gf_send.at[k], gf_in.at[k], gf_ss.at[k], gf_rs.at[k], chain.at(chain.z_far_mid, c))

    def sums_to_end(k):
        return send(end_send.at[k], gf_in.at[k, 0], es_ss.at[k], es_rs.at[k], chain.at(chain.z_end, c))

    def device_on(way):
        return ((along_x if way == 0 else along_y), me)

    def relay_to(w, way):
        if w == 2:
            half = diag_d.shape[0] // 2
            src, dst = diag_d.at[pl.ds(way * half, half)], relay_d.at[way]
        else:
            half = diag_gu.shape[1] // 2
            src, dst = diag_gu.at[w, pl.ds(way * half, half)], relay_gu.at[w, way]
        return send(src, dst, relay_ss.at[w, way], relay_rs.at[w, way], device_on(way))

    def pair_to(w, way):
        src, dst = (pair_d.at[way], in_d.at[way]) if w == 2 else (pair_gu.at[w, way], in_gu.at[w, way])
        return send(src, dst, pair_ss.at[w, way], pair_rs.at[w, way], device_on(way))

    def part(w, shard, tile):
        if w == 2:
            half = inner // 2
            left = hidden[:, :, pl.ds(tile * half, half)].reshape(slots, half)
            return dot(left, rows[groups + shard].reshape(slots, width), 0, 0)
        half = width // 2
        left = rows[shard, :, :, pl.ds(tile * half, half)].reshape(slots, half)
        return dot(left, delta[w].reshape(slots, inner), 0, 0)

    def over_two(body):
        for tile in range(2):
            body(tile)

    def diagonal(w):
        def body(tile):
            value = part(w, across, tile).astype(BF16)
            half = value.shape[0]
            if w == 2:
                diag_d[pl.ds(tile * half, half), :] = value
            else:
                diag_gu[w, pl.ds(tile * half, half), :] = value

        over_two(body)
        for way in range(2):
            relay_to(w, way).start()

    def pairs(w):
        for way in range(2):
            shard = along_x if way == 0 else along_y
            relay_to(w, 1 - way).wait_recv()

            def body(tile):
                value = part(w, shard, tile)
                half = value.shape[0]
                if tile == 1 - way:
                    come = relay_d[1 - way] if w == 2 else relay_gu[w, 1 - way]
                    value = value.astype(BF16).astype(F32) + come.astype(F32)
                value = value.astype(BF16)
                if w == 2:
                    pair_d[way, pl.ds(tile * half, half), :] = value
                else:
                    pair_gu[w, way, pl.ds(tile * half, half), :] = value

            over_two(body)
            pair_to(w, way).start()

    def finish(w):
        for way in range(2):
            pair_to(w, way).wait_recv()

        def body(tile):
            value = part(w, g, tile)
            half = value.shape[0]
            block = pl.ds(tile * half, half)
            for way in range(2):
                come = in_d[way, block, :] if w == 2 else in_gu[w, way, block, :]
                value = value + come.astype(F32)
            (gate_out, up_out, down_out)[w][block, :] = value.astype(BF16)

        over_two(body)

    def input_grad(k):
        for hc in range(2):
            left = [delta[w, pl.ds(4 * hc, 4)].reshape(4 * slot_rows, inner) for w in range(2)]
            value = (dot(left[0], full[0, k], 1, 1) + dot(left[1], full[1, k], 1, 1)).astype(BF16)
            value = value.reshape(4, slot_rows, width)
            grads[k, pl.ds(4 * hc, 4)] = value

            @pl.when(c == hc)
            def _():
                comb[k, :, 0] = value

    def summed(k, z_from, blocks):
        return dot(
            select[z_from, 0 : blocks * slot_rows, :],
            comb[k, z_from, 0:blocks].reshape(blocks * slot_rows, width), 0, 0,
        )

    for i in range(3):
        loads[i].wait()

    def first(k, carry):
        for w in range(3):
            @pl.when(k == w)
            def _():
                if w == 2:
                    loads[3].wait()
                    loads[4].wait()
                diagonal(w)

        @pl.when(k == 1)
        def _():
            loads[5].wait()

        input_grad(k)

        @pl.when(is_mid)
        def _():
            to_partner(k).start()

        @pl.when(is_end)
        def _():
            for core in range(2):
                far_home(k, core).start()
            end_to_partner(k).start()

        return carry

    lax.fori_loop(0, groups, first, 0)

    @pl.when(is_end)
    def _():
        for k in range(groups):
            for core in range(2):
                near_home(k, core).start()

    for copy in loads[6:]:
        copy.wait()

    def second(k, carry):
        for w in range(3):
            @pl.when(k == w)
            def _():
                pairs(w)

        @pl.when(is_mid)
        def _():
            to_partner(k).wait_recv()
            for core in range(2):
                far_from(k, core).wait_recv()
            gf_send[k, 0] = summed(k, chain.z_far_mid, 4).astype(BF16)
            gf_send[k, 1] = summed(k, chain.z_far_end, 4).astype(BF16)
            sums_across(k).start()

        return carry

    lax.fori_loop(0, groups, second, 0)

    for step in range(1, ranks):
        dots_from((me + step) % ranks).wait_recv()
    dots_in[me] = dots_ref[4 * c + z]
    found = jnp.zeros(route_out.shape, F32)
    slot = lax.broadcasted_iota(jnp.int32, (slot_rows, count), 0).astype(F32)
    for rank in range(ranks):
        hit = jnp.where(table_ref[0, rank : rank + 1, :] == slot, 1.0, 0.0)
        value = lax.dot_general(
            dots_in[rank], hit, (((1,), (0,)), ((), ())),
            precision=lax.Precision.HIGHEST, preferred_element_type=F32,
        )[0:1, :]
        found = jnp.where(ids_ref[...] == rank, value, found)
    route_out[...] = found / weight_ref[...]

    def third(k, carry):
        columns = pl.ds(pl.multiple_of(k * width, 128), width)

        @pl.when(is_mid)
        def _():
            sums_across(k).wait_recv()
            end_send[k] = (summed(k, chain.z_end, 2) + gf_in[k, 1].astype(F32)).astype(BF16)
            sums_to_end(k).start()
            for core in range(2):
                near_from(k, core).wait_recv()
            token_out[:, columns] = (summed(k, z, 4) + gf_in[k, 0].astype(F32)).astype(BF16)

        for w in range(3):
            @pl.when(k == w + 1)
            def _():
                finish(w)

        @pl.when(is_end)
        def _():
            end_to_partner(k).wait_recv()
            sums_to_end(k).wait_recv()
            token_out[:, columns] = (summed(k, z, 2) + gf_in[k, 0].astype(F32)).astype(BF16)

        return carry

    lax.fori_loop(0, groups, third, 0)

    for w in range(3):
        for way in range(2):
            relay_to(w, way).wait_send()
            pair_to(w, way).wait_send()
    for step in range(1, ranks):
        dots_to((me + step) % ranks).wait_send()

    def drain(k, carry):
        @pl.when(is_mid)
        def _():
            to_partner(k).wait_send()
            sums_across(k).wait_send()
            sums_to_end(k).wait_send()

        @pl.when(is_end)
        def _():
            for core in range(2):
                far_home(k, core).wait_send()
                near_home(k, core).wait_send()
            end_to_partner(k).wait_send()

        return carry

    lax.fori_loop(0, groups, drain, 0)


def backward_call(ids_t, weight_t, table, dots, full, rows, hidden, delta, cap):
    groups, ranks = lax.axis_size("dp"), lax.axis_size("expert")
    _, _, slot_rows, width = rows.shape
    count = table.shape[2]
    inner = hidden.shape[2]
    hbm = pl.BlockSpec(memory_space=pl.ANY)
    vmem = pl.BlockSpec(memory_space=pltpu.VMEM)
    dma = pltpu.SemaphoreType.DMA
    return pl.pallas_call(
        functools.partial(backward_kernel, cap),
        out_shape=(
            jax.ShapeDtypeStruct((count, groups * width), BF16),
            jax.ShapeDtypeStruct(ids_t.shape, F32),
            jax.ShapeDtypeStruct((width, inner), BF16),
            jax.ShapeDtypeStruct((width, inner), BF16),
            jax.ShapeDtypeStruct((inner, width), BF16),
        ),
        in_specs=[vmem, vmem, vmem, vmem, hbm, hbm, hbm, hbm],
        out_specs=(vmem,) * 5,
        scratch_shapes=[
            pltpu.VMEM(full.shape, BF16),
            pltpu.VMEM(rows.shape, BF16),
            pltpu.VMEM(hidden.shape, BF16),
            pltpu.VMEM(delta.shape, BF16),
            pltpu.VMEM((groups, ranks, slot_rows, width), BF16),
            pltpu.VMEM((groups, 4, 4, slot_rows, width), BF16),
            pltpu.VMEM((groups, 2, count, width), BF16),
            pltpu.VMEM((groups, 2, count, width), BF16),
            pltpu.VMEM((groups, count, width), BF16),
            pltpu.VMEM((4, 4 * slot_rows, count), BF16),
            pltpu.VMEM((2, width, inner), BF16),
            pltpu.VMEM((inner, width), BF16),
            pltpu.VMEM((2, 2, width, inner), BF16),
            pltpu.VMEM((2, inner, width), BF16),
            pltpu.VMEM((2, 2, width // 2, inner), BF16),
            pltpu.VMEM((2, inner // 2, width), BF16),
            pltpu.VMEM((2, 2, width, inner), BF16),
            pltpu.VMEM((2, inner, width), BF16),
            pltpu.VMEM(dots.shape, F32),
            dma((12,)), dma((groups,)), dma((groups,)), dma((groups, 2)), dma((groups, 2)),
            dma((groups, 2)), dma((groups, 2)), dma((groups,)), dma((groups,)), dma((groups,)), dma((groups,)),
            dma((ranks,)), dma((ranks,)), dma((3, 2)), dma((3, 2)), dma((3, 2)), dma((3, 2)),
        ],
        compiler_params=pltpu.CompilerParams(
            collective_id=1, has_side_effects=True, vmem_limit_bytes=67000000
        ),
    )(ids_t, weight_t, table, dots, full, rows, hidden, delta)


def swap(block, axis, distance):
    ranks = lax.axis_size(axis)
    return lax.ppermute(block, axis, [(rank, rank ^ distance) for rank in range(ranks)])


def any_mesh(tokens, out_grad, expert_ids, route_weight, w_gate, w_up, w_down):
    tok_count = tokens.shape[0]
    route_count = expert_ids.shape[1]
    ranks = lax.axis_size("expert")
    groups = lax.axis_size("dp")
    me = lax.axis_index("expert")
    group = lax.axis_index("dp")
    capacity = 3 * tok_count * route_count // (2 * ranks)
    routes = tok_count * route_count
    total_slots = ranks * capacity
    full_gate = lax.all_gather(w_gate[0], "dp", axis=0, tiled=True)
    full_up = lax.all_gather(w_up[0], "dp", axis=0, tiled=True)
    full_down = lax.all_gather(w_down[0], "dp", axis=1, tiled=True)
    half = ranks // 2
    flat_ids = expert_ids.reshape(routes)
    one_hot = (flat_ids[:, None] == jnp.arange(ranks, dtype=jnp.int32)[None, :]).astype(jnp.int32)
    slot_order = jnp.sum((jnp.cumsum(one_hot, axis=0) - 1) * one_hot, axis=1)
    slot_order = slot_order.reshape(tok_count, route_count)
    routing = jnp.concatenate(
        [
            expert_ids.astype(jnp.float32),
            slot_order.astype(jnp.float32),
            route_weight.astype(jnp.float32),
        ],
        axis=1,
    )
    far_routing = swap(routing, "expert", half)
    far_ids = far_routing[:, :route_count].astype(jnp.int32)
    far_order = far_routing[:, route_count : 2 * route_count].astype(jnp.int32)
    far_weight = far_routing[:, 2 * route_count :].astype(jnp.bfloat16)
    far_tokens = swap(tokens, "expert", half)
    late_grad, slot_order = lax.optimization_barrier((out_grad, slot_order))
    far_grad = swap(late_grad, "expert", half)
    slots = jnp.arange(total_slots, dtype=jnp.int32)

    def selectors(destination, weight, count):
        picks = jnp.zeros((count, tok_count), jnp.bfloat16)
        weighted = jnp.zeros((count, tok_count), jnp.bfloat16)
        for k in range(route_count):
            hit = slots[:count, None] == destination[:, k][None, :]
            picks = jnp.where(hit, jnp.ones((), jnp.bfloat16), picks)
            weighted = jnp.where(hit, weight[:, k][None, :], weighted)
        return picks, weighted

    destination = (expert_ids ^ me) * capacity + slot_order
    far_destination = (far_ids ^ me) * capacity + far_order
    near_slots = half * capacity
    picks, _ = selectors(destination, route_weight, total_slots)
    near_picks, near_weighted = selectors(destination, route_weight, near_slots)
    far_picks, far_weighted = selectors(far_destination, far_weight, near_slots)

    def blocks(buffer, count=ranks):
        return [buffer[d * capacity : (d + 1) * capacity] for d in range(count)]

    def exchange(buffer, count=ranks):
        return [
            swap(block, "expert", d) if d else block for d, block in enumerate(blocks(buffer, count))
        ]

    rows_in = jnp.concatenate(
        exchange(dot(near_picks, tokens, 1, 0).astype(jnp.bfloat16), half)
        + exchange(dot(far_picks, far_tokens, 1, 0).astype(jnp.bfloat16), half)
    )
    gate_value = dot(rows_in, full_gate, 1, 0)
    up_value = dot(rows_in, full_up, 1, 0)
    sigmoid_gate = jax.nn.sigmoid(gate_value)
    activated = gate_value * sigmoid_gate
    hidden = (activated * up_value).astype(jnp.bfloat16)
    scaled_blocks = exchange(
        dot(near_weighted, late_grad, 1, 0).astype(jnp.bfloat16), half
    ) + exchange(dot(far_weighted, far_grad, 1, 0).astype(jnp.bfloat16), half)
    scaled_blocks, hidden = lax.optimization_barrier((scaled_blocks, hidden))
    scaled = jnp.concatenate(scaled_blocks)
    hidden_grad = dot(scaled, full_down, 1, 1)
    gate_delta = (
        hidden_grad * up_value * sigmoid_gate * (1.0 + gate_value * (1.0 - sigmoid_gate))
    ).astype(jnp.bfloat16)
    up_delta = (hidden_grad * activated).astype(jnp.bfloat16)
    input_grad = (
        dot(gate_delta, full_gate, 1, 1) + dot(up_delta, full_up, 1, 1)
    ).astype(jnp.bfloat16)
    back_blocks = []
    for d, block in enumerate(blocks(input_grad)):
        back_blocks.append(swap(block, "expert", d) if d else block)
    down_part = dot(hidden, scaled, 0, 0).astype(jnp.bfloat16)
    input_grad, rows_in, hidden = lax.optimization_barrier((input_grad, rows_in, hidden))
    expert_out = dot(hidden, full_down, 1, 0)
    weighted_dot = jnp.sum(expert_out * scaled.astype(jnp.float32), axis=1)
    gate_part = dot(rows_in, gate_delta, 0, 0).astype(jnp.bfloat16)
    up_part = dot(rows_in, up_delta, 0, 0).astype(jnp.bfloat16)
    down_grad = lax.psum_scatter(down_part, "dp", scatter_dimension=1, tiled=True)[None]
    gate_grad = lax.psum_scatter(gate_part, "dp", scatter_dimension=0, tiled=True)[None]
    depth = up_part.shape[0] // groups
    up_sum = jnp.zeros((depth, up_part.shape[1]), jnp.float32)
    for d in range(groups):
        piece = lax.dynamic_slice_in_dim(up_part, (group ^ d) * depth, depth, 0)
        up_sum = up_sum + (swap(piece, "dp", d) if d else piece).astype(jnp.float32)
    up_grad = up_sum.astype(jnp.bfloat16)[None]

    token_sum = jnp.zeros(tokens.shape, jnp.float32)
    for pick, block in zip(blocks(picks), back_blocks):
        token_sum = token_sum + dot(pick, block, 0, 0)
    token_grad = token_sum.astype(jnp.bfloat16)

    order = jnp.arange(ranks, dtype=jnp.int32)
    dots = weighted_dot.reshape(ranks, capacity)
    by_rank = jnp.sum(
        jnp.where(((order ^ me)[:, None] == order[None, :])[:, :, None], dots[None], 0.0), axis=1
    )
    back_dots = lax.all_to_all(by_rank, "expert", split_axis=0, concat_axis=0, tiled=True)
    arrival = expert_ids * capacity + slot_order
    hits = arrival.reshape(tok_count, route_count, 1) == slots[None, None, :]
    own_dots = jnp.sum(jnp.where(hits, back_dots.reshape(total_slots)[None, None, :], 0.0), axis=2)
    route_grad = (own_dots / route_weight.astype(jnp.float32)).astype(jnp.bfloat16)
    return (token_grad, route_grad, gate_grad, up_grad, down_grad)


def on_device(tokens, out_grad, expert_ids, route_weight, w_gate, w_up, w_down):
    count = tokens.shape[0]
    cap = 3 * count * expert_ids.shape[1] // (2 * lax.axis_size("expert"))
    ids_t, weight_t = expert_ids.T, route_weight.T.astype(F32)
    full, rows, hidden, delta, dots, table = forward_call(
        ids_t, weight_t, tokens, out_grad, w_gate, w_up, w_down, cap
    )
    token_grad, route_grad, gate_grad, up_grad, down_grad = backward_call(
        ids_t, weight_t, table, dots, full, rows, hidden, delta, cap
    )
    return token_grad, route_grad.T.astype(BF16), gate_grad[None], up_grad[None], down_grad[None]


def solution(mesh):
    placed = (
        P(("dp", "expert"), None),
        P(("dp", "expert"), None),
        P(("dp", "expert"), None),
        P(("dp", "expert"), None),
        P("expert", "dp", None),
        P("expert", "dp", None),
        P("expert", None, "dp"),
    )
    chained = mesh.shape["expert"] == 8 and mesh.shape["dp"] == 4
    return jax.shard_map(
        on_device if chained else any_mesh, mesh=mesh, in_specs=placed,
        out_specs=(
            P(("dp", "expert"), None),
            P(("dp", "expert"), None),
            P("expert", "dp", None),
            P("expert", "dp", None),
            P("expert", None, "dp"),
        ),
        check_vma=False,
    )
```

```python
import functools
import jax
import jax.numpy as jnp
from jax import lax
from jax.experimental import pallas as pl
from jax.experimental.pallas import tpu as pltpu
from jax.sharding import PartitionSpec as P


MESH = pl.DeviceIdType.MESH
BF16 = jnp.bfloat16
F32 = jnp.float32


def dot(left, right, over_left=1, over_right=0):
    return lax.dot_general(
        left, right, (((over_left,), (over_right,)), ((), ())), preferred_element_type=F32
    )


class Chain:
    def __init__(self):
        self.g = lax.axis_index("dp")
        self.me = lax.axis_index("expert")
        self.c = self.me % 2
        self.z = self.me // 2
        self.half = self.z // 2
        self.far = 1 - self.half
        self.is_mid = (self.z + self.half) % 2 == 1
        self.is_end = (self.z + self.half) % 2 == 0
        self.z_mid = 1 + self.half
        self.z_end = 3 * self.half
        self.z_far_mid = 1 + self.far
        self.z_far_end = 3 * self.far
        self.z_near = self.z_mid + self.z_end - self.z

    def at(self, z, c):
        return (self.g, 2 * z + c)


def greet(chain, ranks, groups, meanwhile=None):
    barrier = pltpu.get_barrier_semaphore()
    for step in range(1, ranks):
        pl.semaphore_signal(
            barrier, inc=1, device_id=(chain.g, (chain.me + step) % ranks), device_id_type=MESH
        )
    for step in range(1, groups):
        pl.semaphore_signal(
            barrier, inc=1, device_id=((chain.g + step) % groups, chain.me), device_id_type=MESH
        )
    if meanwhile is not None:
        meanwhile()
    pl.semaphore_wait(barrier, ranks + groups - 2)


def neighbours(g):
    along_x = g + 1 - 2 * (g % 2)
    along_y = (g + 2) % 4
    return along_x, along_y


def send(src, dst, send_sem, recv_sem, device):
    return pltpu.make_async_remote_copy(
        src_ref=src, dst_ref=dst, send_sem=send_sem, recv_sem=recv_sem,
        device_id=device, device_id_type=MESH,
    )


def forward_kernel(
    cap,
    ids_ref, weight_ref, tokens_ref, grads_ref, wg_ref, wu_ref, wd_ref,
    full_out, rows_out, hidden_out, delta_out, dots_out, table_out, down_out,
    raw, rows, stage_d, stage_e, full_gate, full_up, full_down, gate_val, up_val, hg_val, select,
    down_part, down_relay, down_in,
    load_sem, raw_ss, raw_rs, e_ss, e_rs, d_ss, d_rs, tab_ss, tab_rs,
    w_ls, wa_ss, wa_rs, wf_ss, wf_rs, out_sem, relay_ss, relay_rs, pair_ss, pair_rs,
):
    chain = Chain()
    g, me, c, z = chain.g, chain.me, chain.c, chain.z
    is_mid, is_end = chain.is_mid, chain.is_end
    groups = lax.axis_size("dp")
    ranks = lax.axis_size("expert")
    steps = 2 * groups
    width = raw.shape[-1]
    count = raw.shape[2]
    slot_rows = rows.shape[2]
    along_x, along_y = neighbours(g)
    fulls = (full_gate, full_up, full_down)
    shards = (wg_ref, wu_ref, wd_ref)

    sub = width // groups
    for k in range(groups):
        pltpu.make_async_copy(
            tokens_ref.at[:, pl.ds(k * width, width)], raw.at[0, k], load_sem.at[k]
        ).start()
    for i in range(groups):
        for owner in range(groups):
            pltpu.make_async_copy(
                grads_ref.at[:, pl.ds(owner * width + i * sub, sub)],
                raw.at[0, groups + i, :, pl.ds(owner * sub, sub)], load_sem.at[groups + i],
            ).start()
    for w in range(3):
        pltpu.make_async_copy(shards[w].at[0], fulls[w].at[g], w_ls.at[w]).start()

    def shard_to(w, way):
        device = (along_x, me) if way == 0 else (along_y, me)
        return send(shards[w].at[0], fulls[w].at[g], wa_ss.at[w, way], wa_rs.at[w, way], device)

    def forward_half(w, way):
        owner = along_y if way == 0 else along_x
        device = (along_x, me) if way == 0 else (along_y, me)
        half = fulls[w].shape[1] // 2
        piece = fulls[w].at[owner, pl.ds(way * half, half)]
        return send(piece, piece, wf_ss.at[w, way], wf_rs.at[w, way], device)

    def build_table():
        experts = lax.broadcasted_iota(jnp.int32, (ranks, count), 0)
        named = [experts == ids_ref[k : k + 1, :] for k in range(ids_ref.shape[0])]
        hits = functools.reduce(jnp.logical_or, named)
        before = lax.broadcasted_iota(jnp.int32, (count, count), 0) < lax.broadcasted_iota(
            jnp.int32, (count, count), 1
        )
        order = dot(hits.astype(F32).astype(BF16), before.astype(F32).astype(BF16))
        table_out[0, 0:ranks, :] = jnp.where(hits, order, -1.0)
        weight = jnp.zeros((ranks, count), F32)
        for k in range(ids_ref.shape[0]):
            weight = jnp.where(named[k], weight_ref[k : k + 1, :], weight)
        table_out[0, ranks : 2 * ranks, :] = weight

        rows[:, :, cap:, :] = jnp.zeros((steps, ranks, slot_rows - cap, width), BF16)

    def table_send(slot, sem, zz):
        return send(
            table_out.at[0], table_out.at[slot], tab_ss.at[sem], tab_rs.at[slot - 1], chain.at(zz, c)
        )

    targets = (me, me + 1 - 2 * c, 2 * chain.z_near, 2 * chain.z_near + 1)

    def selectors(j):
        slots = lax.broadcasted_iota(jnp.int32, (slot_rows, count), 0).astype(F32)
        for i, rank in enumerate(targets):
            hit = table_out[j, pl.ds(rank, 1), :] == slots
            block = pl.ds(i * slot_rows, slot_rows)
            select[0, j, block, :] = jnp.where(hit, 1.0, 0.0).astype(BF16)
            select[1, j, block, :] = jnp.where(
                hit, table_out[j, pl.ds(ranks + rank, 1), :], 0.0
            ).astype(BF16)

    def gather(j, k, z_from, blocks, e_slot):
        picked = dot(select[k // groups, j, 0 : blocks * slot_rows, :], raw[j, k]).astype(BF16)
        parts = [picked[i * slot_rows : (i + 1) * slot_rows] for i in range(blocks)]
        rows[k, 4 * c + z_from] = parts[0]
        stage_d[k, z_from] = parts[1]
        for i in range(2, blocks):
            stage_e[k, i - 2, e_slot] = parts[i]

    full = pl.ds(0, cap)
    far_places = ((chain.z_far_mid, 1), (chain.z_far_end, 2))

    def own_raw(k):
        return send(raw.at[0, k], raw.at[2, k], raw_ss.at[0, k], raw_rs.at[1, k], chain.at(chain.z_far_mid, c))

    def end_raw(k):
        return send(raw.at[0, k], raw.at[1, k], raw_ss.at[0, k], raw_rs.at[0, k], chain.at(chain.z_mid, c))

    def onward_raw(k):
        return send(raw.at[1, k], raw.at[3, k], raw_ss.at[1, k], raw_rs.at[2, k], chain.at(chain.z_far_mid, c))

    def own_to_end(k, i):
        return send(
            stage_e.at[k, i, 0, full], rows.at[k, 4 * c + z, full],
            e_ss.at[k, 0, i], e_rs.at[k, 0, c], chain.at(chain.z_end, i),
        )

    def far_to_end(k, i, which):
        z_from, slot = far_places[which]
        return send(
            stage_e.at[k, i, slot, full], rows.at[k, 4 * c + z_from, full],
            e_ss.at[k, 1 + which, i], e_rs.at[k, 1 + which, c], chain.at(chain.z_end, i),
        )

    def mid_to_partner(k):
        return send(
            stage_d.at[k, :, full], rows.at[k, pl.ds(4 * c, 4), full], d_ss.at[k], d_rs.at[k], chain.at(z, 1 - c)
        )

    def end_to_partner(k):
        return send(
            stage_d.at[k, z, full], rows.at[k, 4 * c + z, full], d_ss.at[k], d_rs.at[k], chain.at(z, 1 - c)
        )

    def own_block_from(k, core):
        return send(
            stage_e.at[k, 0, 0, full], rows.at[k, 4 * core + chain.z_mid, full],
            e_ss.at[k, 0, 0], e_rs.at[k, 0, core], chain.at(chain.z_mid, core),
        )

    def far_block_from(k, core, which):
        return send(
            stage_e.at[k, 0, 1, full], rows.at[k, 4 * core + far_places[which][0], full],
            e_ss.at[k, 1 + which, 0], e_rs.at[k, 1 + which, core], chain.at(chain.z_mid, core),
        )

    def landed(k):
        @pl.when(is_mid)
        def _():
            mid_to_partner(k).wait_recv()

        @pl.when(is_end)
        def _():
            end_to_partner(k).wait_recv()
            for core in range(2):
                own_block_from(k, core).wait_recv()
                for which in range(2):
                    far_block_from(k, core, which).wait_recv()

    def load_wait(k):
        pltpu.make_async_copy(
            tokens_ref.at[:, pl.ds(0, width)], raw.at[0, k], load_sem.at[k]
        ).wait()

    across = groups - 1 - g
    slots = ranks * slot_rows
    half_inner = hidden_out.shape[2] // 2

    def hidden_grad(q, carry):
        landed(groups + q)

        def tile(t, carry):
            four = pl.ds(4 * t, 4)
            value = functools.reduce(jnp.add, [
                dot(
                    rows[groups + q, four, :, owner * sub : (owner + 1) * sub].reshape(4 * slot_rows, sub),
                    full_down[owner, :, pl.ds(pl.multiple_of(q * sub, 128), sub)], 1, 1,
                )
                for owner in range(groups)
            ]).reshape(4, slot_rows, hg_val.shape[2])

            @pl.when(q == 0)
            def _():
                hg_val[four] = value

            @pl.when(q > 0)
            def _():
                hg_val[four] += value

            return carry

        return lax.fori_loop(0, ranks // 4, tile, carry)

    def block_of(tile):
        return pl.ds(tile * half_inner, half_inner)

    def of_owner(owner):
        return pl.ds(pl.multiple_of(owner * sub, 128), sub)

    def relay_to(i, way):
        device = (along_x, me) if way == 0 else (along_y, me)
        return send(
            down_part.at[i, block_of(way), of_owner(across)], down_relay.at[i, way],
            relay_ss.at[i, way], relay_rs.at[i, way], device,
        )

    def pair_to(i, way):
        owner = along_x if way == 0 else along_y
        return send(
            down_part.at[i, :, of_owner(owner)], down_in.at[i, way],
            pair_ss.at[i, way], pair_rs.at[i, way], (owner, me),
        )

    def down_make(i):
        for tile in range(2):
            left = hidden_out[:, :, tile * half_inner : (tile + 1) * half_inner].reshape(slots, half_inner)
            down_part[i, block_of(tile), :] = dot(
                left, rows[groups + i].reshape(slots, width), 0, 0
            ).astype(BF16)
        for way in range(2):
            relay_to(i, way).start()

    def down_pass(i):
        for way in range(2):
            owner = along_x if way == 0 else along_y
            relay_to(i, 1 - way).wait_recv()
            place = (i, block_of(1 - way), of_owner(owner))
            down_part[place] = (
                down_part[place].astype(F32) + down_relay[i, 1 - way].astype(F32)
            ).astype(BF16)
            pair_to(i, way).start()

    def down_own(i):
        for way in range(2):
            pair_to(i, way).wait_recv()
        total = down_part[i, :, of_owner(g)].astype(F32)
        for way in range(2):
            total = total + down_in[i, way].astype(F32)
        down_out[:, of_owner(i)] = total.astype(BF16)

    ahead = 2

    def prologue():
        build_table()
        selectors(0)
        for k in range(ahead):
            load_wait(k)

            @pl.when(is_mid)
            def _():
                gather(0, k, z, 4, 0)

    greet(chain, ranks, groups, prologue)
    for way in range(2):
        shard_to(0, way).start()

    @pl.when(is_mid)
    def _():
        own_raw(0).start()
        for k in range(ahead):
            own_to_end(k, 0).start()
            own_to_end(k, 1).start()

    @pl.when(is_end)
    def _():
        end_raw(0).start()
        table_send(1, 0, chain.z_mid).start()
        table_send(3, 1, chain.z_far_mid).start()

    @pl.when(is_mid)
    def _():
        table_send(2, 0, chain.z_far_mid).start()

    for w in range(1, 3):
        for way in range(2):
            shard_to(w, way).start()
    for k in range(ahead, steps):
        load_wait(k)

    @pl.when(is_end)
    def _():
        for k in range(1, steps):
            end_raw(k).start()

    def step(k, carry):
        @pl.when(is_mid & (k < steps))
        def _():
            @pl.when(k > 0)
            def _():
                own_raw(k).start()

            @pl.when(k == 0)
            def _():
                table_send(1, 0, chain.z_mid).wait_recv()
                selectors(1)

            end_raw(k).wait_recv()
            onward_raw(k).start()

            @pl.when(k + ahead < steps)
            def _():
                gather(0, k + ahead, z, 4, 0)
                own_to_end(k + ahead, 0).start()
                own_to_end(k + ahead, 1).start()

            gather(1, k, chain.z_end, 2, 0)

        @pl.when(is_mid & (k >= 1))
        def _():
            @pl.when(k == 1)
            def _():
                table_send(2, 0, chain.z_far_mid).wait_recv()
                table_send(3, 0, chain.z_far_mid).wait_recv()
                selectors(2)
                selectors(3)

            j = k - 1
            own_raw(j).wait_recv()
            gather(2, j, chain.z_far_mid, 4, 1)
            far_to_end(j, 0, 0).start()
            far_to_end(j, 1, 0).start()
            onward_raw(j).wait_recv()
            gather(3, j, chain.z_far_end, 4, 2)
            far_to_end(j, 0, 1).start()
            far_to_end(j, 1, 1).start()
            mid_to_partner(j).start()

        @pl.when(is_end & (k < steps))
        def _():
            gather(0, k, z, 2, 0)
            end_to_partner(k).start()

        for w in range(3):
            @pl.when(k == w + 2)
            def _():
                for way in range(2):
                    shard_to(w, 1 - way).wait_recv()
                    forward_half(w, way).start()

        @pl.when(k == groups + 1)
        def _():
            for kk in range(groups):
                landed(kk)
            for w in range(2):
                pltpu.make_async_copy(shards[w].at[0], fulls[w].at[g], w_ls.at[w]).wait()
                for way in range(2):
                    forward_half(w, way).wait_recv()

        @pl.when((k == groups + 1) | (k == groups + 2))
        def _():
            def forward(p, carry):
                pair = pl.ds(2 * p, 2)
                shape = (2, slot_rows, gate_val.shape[2])
                piece = [rows[kk, pair].reshape(2 * slot_rows, width) for kk in range(groups)]
                gate = functools.reduce(jnp.add, [dot(piece[kk], full_gate[kk]) for kk in range(groups)])
                up = functools.reduce(jnp.add, [dot(piece[kk], full_up[kk]) for kk in range(groups)])
                gate_val[pair] = gate.reshape(shape)
                up_val[pair] = up.reshape(shape)
                hidden_out[pair] = (gate * jax.nn.sigmoid(gate) * up).astype(BF16).reshape(shape)
                return carry

            start = (k - groups - 1) * (ranks // 4)
            lax.fori_loop(start, start + ranks // 4, forward, 0)

        @pl.when(k == groups + 2)
        def _():
            pltpu.make_async_copy(shards[2].at[0], fulls[2].at[g], w_ls.at[2]).wait()
            for way in range(2):
                forward_half(2, way).wait_recv()

        @pl.when(k >= groups + 2)
        def _():
            q = k - groups - 2

            @pl.when(q >= 1)
            def _():
                down_pass(q - 1)

            hidden_grad(q, 0)
            down_make(q)

        return carry

    lax.fori_loop(0, steps + 1, step, 0)

    outs = [
        pltpu.make_async_copy(full_gate, full_out.at[0], out_sem.at[0]),
        pltpu.make_async_copy(full_up, full_out.at[1], out_sem.at[1]),
    ]
    for copy in outs:
        copy.start()
    first = pltpu.make_async_copy(rows.at[pl.ds(0, groups)], rows_out.at[pl.ds(0, groups)], out_sem.at[2])
    first.start()

    down_pass(groups - 2)
    hidden_grad(groups - 1, 0)
    late = pltpu.make_async_copy(rows.at[steps - 1], rows_out.at[groups], out_sem.at[3])
    late.start()

    def deltas(t, carry):
        gate, up, grad = gate_val[t], up_val[t], hg_val[t]
        sig = jax.nn.sigmoid(gate)
        delta_out[0, t] = (grad * up * sig * (1.0 + gate * (1.0 - sig))).astype(BF16)
        delta_out[1, t] = (grad * (gate * sig)).astype(BF16)
        total = jnp.sum(hidden_out[t].astype(F32) * grad, axis=1, keepdims=True)
        dots_out[t] = jnp.broadcast_to(total, (total.shape[0], total.shape[0])).T[0:8, :]
        return carry

    lax.fori_loop(0, ranks, deltas, 0)

    for copy in outs:
        copy.wait()
    first.wait()
    late.wait()

    def finish_down(i, carry):
        down_own(i)
        for way in range(2):
            relay_to(i, way).wait_send()
            pair_to(i, way).wait_send()
        return carry

    lax.fori_loop(0, groups - 1, finish_down, 0)
    for w in range(3):
        for way in range(2):
            shard_to(w, way).wait_send()
            forward_half(w, way).wait_send()

    def drain(k, carry):
        @pl.when(is_mid)
        def _():
            own_raw(k).wait_send()
            onward_raw(k).wait_send()
            for i in range(2):
                own_to_end(k, i).wait_send()
                for which in range(2):
                    far_to_end(k, i, which).wait_send()
            mid_to_partner(k).wait_send()

        @pl.when(is_end)
        def _():
            end_raw(k).wait_send()
            end_to_partner(k).wait_send()

        return carry

    lax.fori_loop(0, steps, drain, 0)

    @pl.when(is_mid)
    def _():
        table_send(2, 0, chain.z_far_mid).wait_send()

    @pl.when(is_end)
    def _():
        table_send(1, 0, chain.z_mid).wait_send()
        table_send(3, 1, chain.z_far_mid).wait_send()


def forward_call(ids_t, weight_t, tokens, out_grad, w_gate, w_up, w_down, cap):
    count, depth = tokens.shape
    groups, ranks = lax.axis_size("dp"), lax.axis_size("expert")
    inner = w_gate.shape[2]
    width = depth // groups
    slot_rows = -(-cap // 16) * 16
    steps = 2 * groups
    hbm = pl.BlockSpec(memory_space=pl.ANY)
    vmem = pl.BlockSpec(memory_space=pltpu.VMEM)
    dma = pltpu.SemaphoreType.DMA
    return pl.pallas_call(
        functools.partial(forward_kernel, cap),
        out_shape=(
            jax.ShapeDtypeStruct((2, groups, width, inner), BF16),
            jax.ShapeDtypeStruct((groups + 1, ranks, slot_rows, width), BF16),
            jax.ShapeDtypeStruct((ranks, slot_rows, inner), BF16),
            jax.ShapeDtypeStruct((2, ranks, slot_rows, inner), BF16),
            jax.ShapeDtypeStruct((ranks, 8, slot_rows), F32),
            jax.ShapeDtypeStruct((4, 2 * ranks, count), F32),
            jax.ShapeDtypeStruct((inner, width), BF16),
        ),
        in_specs=[vmem, vmem, hbm, hbm, hbm, hbm, hbm],
        out_specs=(hbm, hbm, vmem, vmem, vmem, vmem, vmem),
        scratch_shapes=[
            pltpu.VMEM((4, steps, count, width), BF16),
            pltpu.VMEM((steps, ranks, slot_rows, width), BF16),
            pltpu.VMEM((steps, 4, slot_rows, width), BF16),
            pltpu.VMEM((steps, 2, 3, slot_rows, width), BF16),
            pltpu.VMEM((groups, width, inner), BF16),
            pltpu.VMEM((groups, width, inner), BF16),
            pltpu.VMEM((groups, inner, width), BF16),
            pltpu.VMEM((ranks, slot_rows, inner), F32),
            pltpu.VMEM((ranks, slot_rows, inner), F32),
            pltpu.VMEM((ranks, slot_rows, inner), F32),
            pltpu.VMEM((2, 4, 4 * slot_rows, count), BF16),
            pltpu.VMEM((groups - 1, inner, width), BF16),
            pltpu.VMEM((groups - 1, 2, inner // 2, width // groups), BF16),
            pltpu.VMEM((groups - 1, 2, inner, width // groups), BF16),
            dma((steps,)), dma((2, steps)), dma((3, steps)), dma((steps, 3, 2)), dma((steps, 3, 2)),
            dma((steps,)), dma((steps,)), dma((2,)), dma((3,)),
            dma((3,)), dma((3, 2)), dma((3, 2)), dma((3, 2)), dma((3, 2)), dma((4,)),
            dma((groups - 1, 2)), dma((groups - 1, 2)), dma((groups - 1, 2)), dma((groups - 1, 2)),
        ],
        compiler_params=pltpu.CompilerParams(
            collective_id=0, has_side_effects=True, vmem_limit_bytes=67000000
        ),
    )(ids_t, weight_t, tokens, out_grad, w_gate, w_up, w_down)


def backward_kernel(
    cap,
    ids_ref, weight_ref, table_ref, dots_ref, full_ref, rows_ref, hidden_ref, delta_ref, down_ref,
    token_out, route_out, gate_out, up_out, down_out,
    full, rows, hidden, delta, grads, comb, gf_send, gf_in, end_send, select,
    diag_gu, pair_gu, pair_d, relay_gu, relay_d, in_gu, in_d, dots_in,
    load_sem, d_ss, d_rs, far_ss, far_rs, near_ss, near_rs, gf_ss, gf_rs, es_ss, es_rs,
    dots_ss, dots_rs, relay_ss, relay_rs, pair_ss, pair_rs,
):
    chain = Chain()
    g, me, c, z = chain.g, chain.me, chain.c, chain.z
    is_mid, is_end = chain.is_mid, chain.is_end
    groups = lax.axis_size("dp")
    ranks = lax.axis_size("expert")
    _, slot_rows, width = rows.shape[1:]
    count = table_ref.shape[2]
    inner = hidden.shape[2]
    along_x, along_y = neighbours(g)
    across = groups - 1 - g
    slots = ranks * slot_rows
    subs, narrow = grads.shape[0], grads.shape[3]

    loads = [
        pltpu.make_async_copy(delta_ref, delta, load_sem.at[0]),
        pltpu.make_async_copy(full_ref.at[:, 0], full.at[:, 0], load_sem.at[1]),
        pltpu.make_async_copy(rows_ref.at[across], rows.at[across], load_sem.at[2]),
        pltpu.make_async_copy(full_ref.at[:, pl.ds(1, subs - 1)], full.at[:, pl.ds(1, subs - 1)], load_sem.at[3]),
        pltpu.make_async_copy(rows_ref.at[groups], rows.at[groups], load_sem.at[4]),
        pltpu.make_async_copy(hidden_ref, hidden, load_sem.at[5]),
    ]
    for i, shard in enumerate((along_x, along_y, g)):
        loads.append(pltpu.make_async_copy(rows_ref.at[shard], rows.at[shard], load_sem.at[6 + i]))
    for copy in loads:
        copy.start()
    sub = width // groups
    half_inner = inner // 2
    down_ready = pltpu.make_async_copy(down_ref, down_out, load_sem.at[9])
    down_ready.start()

    def of_owner(owner):
        return pl.ds(pl.multiple_of(owner * sub, 128), sub)

    greet(chain, ranks, groups)

    real = pl.ds(0, cap)

    def dots_to(peer):
        return send(
            dots_ref.at[4 * (peer % 2) + peer // 2], dots_in.at[me],
            dots_ss.at[peer], dots_rs.at[me], (g, peer),
        )

    def dots_from(peer):
        return send(
            dots_ref.at[4 * c + z], dots_in.at[peer], dots_ss.at[peer], dots_rs.at[peer], (g, peer)
        )

    for step in range(1, ranks):
        dots_to((me + step) % ranks).start()

    comb[:, :, :, cap:, :] = jnp.zeros((subs, 4, 4, slot_rows - cap, narrow), BF16)
    targets = (me, me + 1 - 2 * c, 2 * chain.z_near, 2 * chain.z_near + 1)

    def selectors(j, z_from):
        slot = lax.broadcasted_iota(jnp.int32, (slot_rows, count), 0).astype(F32)
        for i, rank in enumerate(targets):
            hit = table_ref[j, pl.ds(rank, 1), :] == slot
            select[z_from, i * slot_rows : (i + 1) * slot_rows, :] = jnp.where(hit, 1.0, 0.0).astype(BF16)

    selectors(0, z)

    @pl.when(is_mid)
    def _():
        selectors(1, chain.z_end)
        selectors(2, chain.z_far_mid)
        selectors(3, chain.z_far_end)

    def to_partner(k):
        return send(
            grads.at[k, pl.ds(4 * (1 - c), 4), real], comb.at[k, :, 1, real],
            d_ss.at[k], d_rs.at[k], chain.at(z, 1 - c),
        )

    def end_to_partner(k):
        return send(
            grads.at[k, 4 * (1 - c) + z, real], comb.at[k, z, 1, real],
            d_ss.at[k], d_rs.at[k], chain.at(z, 1 - c),
        )

    def far_home(k, core):
        return send(
            grads.at[k, pl.ds(4 * core + 2 * chain.far, 2), real],
            comb.at[k, pl.ds(2 * chain.far, 2), 2 + c, real],
            far_ss.at[k, core], far_rs.at[k, c], chain.at(chain.z_mid, core),
        )

    def far_from(k, core):
        return send(
            grads.at[k, pl.ds(4 * core + 2 * chain.far, 2), real],
            comb.at[k, pl.ds(2 * chain.far, 2), 2 + core, real],
            far_ss.at[k, core], far_rs.at[k, core], chain.at(chain.z_end, core),
        )

    def near_home(k, core):
        return send(
            grads.at[k, 4 * core + chain.z_mid, real], comb.at[k, chain.z_mid, 2 + c, real],
            near_ss.at[k, core], near_rs.at[k, c], chain.at(chain.z_mid, core),
        )

    def near_from(k, core):
        return send(
            grads.at[k, 4 * core + chain.z_mid, real], comb.at[k, chain.z_mid, 2 + core, real],
            near_ss.at[k, core], near_rs.at[k, core], chain.at(chain.z_end, core),
        )

    def sums_across(k, home):
        return send(
            gf_send.at[k, home], gf_in.at[k, home], gf_ss.at[k, home], gf_rs.at[k, home], chain.at(chain.z_far_mid, c)
        )

    def sums_to_end(k):
        return send(end_send.at[k], gf_in.at[k, 0], es_ss.at[k], es_rs.at[k], chain.at(chain.z_end, c))

    def device_on(way):
        return ((along_x if way == 0 else along_y), me)

    def relay_to(w, way):
        if w == 2:
            src, dst = pair_d.at[pl.ds(way * half_inner, half_inner), of_owner(across)], relay_d.at[way]
        else:
            half = width // 2
            src, dst = diag_gu.at[w, pl.ds(way * half, half)], relay_gu.at[w, way]
        return send(src, dst, relay_ss.at[w, way], relay_rs.at[w, way], device_on(way))

    def pair_to(w, way):
        if w == 2:
            src, dst = pair_d.at[:, of_owner(along_x if way == 0 else along_y)], in_d.at[way]
        else:
            src, dst = pair_gu.at[w, way], in_gu.at[w, way]
        return send(src, dst, pair_ss.at[w, way], pair_rs.at[w, way], device_on(way))

    def part(w, shard, tile):
        half = width // 2
        left = rows[shard, :, :, tile * half : (tile + 1) * half].reshape(slots, half)
        return dot(left, delta[w].reshape(slots, inner), 0, 0)

    def diagonal(w):
        if w == 2:
            for tile in range(2):
                left = hidden[:, :, tile * half_inner : (tile + 1) * half_inner].reshape(slots, half_inner)
                pair_d[pl.ds(tile * half_inner, half_inner), :] = dot(
                    left, rows[groups].reshape(slots, width), 0, 0
                ).astype(BF16)
        else:
            half = width // 2
            for tile in range(2):
                diag_gu[w, pl.ds(tile * half, half), :] = part(w, across, tile).astype(BF16)
        for way in range(2):
            relay_to(w, way).start()

    def pairs(w):
        for way in range(2):
            shard = along_x if way == 0 else along_y
            relay_to(w, 1 - way).wait_recv()
            if w == 2:
                place = (pl.ds((1 - way) * half_inner, half_inner), of_owner(shard))
                pair_d[place] = (pair_d[place].astype(F32) + relay_d[1 - way].astype(F32)).astype(BF16)
            else:
                half = width // 2
                for tile in range(2):
                    value = part(w, shard, tile).astype(BF16)
                    if tile == 1 - way:
                        value = (value.astype(F32) + relay_gu[w, 1 - way].astype(F32)).astype(BF16)
                    pair_gu[w, way, pl.ds(tile * half, half), :] = value
            pair_to(w, way).start()

    def finish(w):
        for way in range(2):
            pair_to(w, way).wait_recv()
        if w == 2:
            total = pair_d[:, of_owner(g)].astype(F32)
            for way in range(2):
                total = total + in_d[way].astype(F32)
            down_ready.wait()
            down_out[:, of_owner(groups - 1)] = total.astype(BF16)
        else:
            half = width // 2
            for tile in range(2):
                value = part(w, g, tile)
                block = pl.ds(tile * half, half)
                for way in range(2):
                    value = value + in_gu[w, way, block, :].astype(F32)
                (gate_out, up_out)[w][block, :] = value.astype(BF16)

    def input_grad(k):
        for hc in range(2):
            left = [delta[w, pl.ds(4 * hc, 4)].reshape(4 * slot_rows, inner) for w in range(2)]
            value = (dot(left[0], full[0, k], 1, 1) + dot(left[1], full[1, k], 1, 1)).astype(BF16)
            value = value.reshape(4, slot_rows, narrow)
            grads[k, pl.ds(4 * hc, 4)] = value

            @pl.when(c == hc)
            def _():
                comb[k, :, 0] = value

    def summed(k, z_from, blocks):
        return dot(
            select[z_from, 0 : blocks * slot_rows, :],
            comb[k, z_from, 0:blocks].reshape(blocks * slot_rows, narrow), 0, 0,
        )

    for i in range(2):
        loads[i].wait()

    lag = 2

    def along(k, carry):
        @pl.when(k == 1)
        def _():
            loads[3].wait()

        @pl.when(k < subs)
        def _():
            input_grad(k)

            @pl.when(is_mid)
            def _():
                to_partner(k).start()

            @pl.when(is_end)
            def _():
                for core in range(2):
                    far_home(k, core).start()
                end_to_partner(k).start()

        @pl.when(is_end & (k == subs - 1))
        def _():
            for j in range(subs):
                for core in range(2):
                    near_home(j, core).start()

        for w in range(2):
            @pl.when(k == w)
            def _():
                if w == 0:
                    loads[2].wait()
                diagonal(w)

        @pl.when(k == 2)
        def _():
            loads[4].wait()
            loads[5].wait()

            diagonal(2)

        @pl.when(is_mid & (k >= 1) & (k <= subs))
        def _():
            j = k - 1
            to_partner(j).wait_recv()
            for core in range(2):
                far_from(j, core).wait_recv()
            gf_send[j, 1] = summed(j, chain.z_far_end, 4).astype(BF16)
            sums_across(j, 1).start()
            gf_send[j, 0] = summed(j, chain.z_far_mid, 4).astype(BF16)
            sums_across(j, 0).start()

        @pl.when(k == 3)
        def _():
            for copy in loads[6:]:
                copy.wait()

        for at, w in ((3, 0), (4, 2), (5, 1)):
            @pl.when(k == at)
            def _():
                pairs(w)

        @pl.when(is_mid & (k > lag))
        def _():
            j = k - 1 - lag
            sums_across(j, 1).wait_recv()
            end_send[j] = (summed(j, chain.z_end, 2) + gf_in[j, 1].astype(F32)).astype(BF16)
            sums_to_end(j).start()

        return carry

    lax.fori_loop(0, subs + 1 + lag, along, 0)

    for step in range(1, ranks):
        dots_from((me + step) % ranks).wait_recv()
    dots_in[me] = dots_ref[4 * c + z]
    found = jnp.zeros(route_out.shape, F32)
    slot = lax.broadcasted_iota(jnp.int32, (slot_rows, count), 0).astype(F32)
    for rank in range(ranks):
        hit = jnp.where(table_ref[0, rank : rank + 1, :] == slot, 1.0, 0.0)
        value = lax.dot_general(
            dots_in[rank], hit, (((1,), (0,)), ((), ())),
            precision=lax.Precision.HIGHEST, preferred_element_type=F32,
        )[0:1, :]
        found = jnp.where(ids_ref[...] == rank, value, found)
    route_out[...] = found / weight_ref[...]

    def third(k, carry):
        columns = pl.ds(pl.multiple_of(k * narrow, 128), narrow)

        @pl.when(k == 0)
        def _():
            finish(0)

        @pl.when(k == 3)
        def _():
            finish(2)

        @pl.when(is_mid)
        def _():
            sums_across(k, 0).wait_recv()
            for core in range(2):
                near_from(k, core).wait_recv()
            token_out[:, columns] = (summed(k, z, 4) + gf_in[k, 0].astype(F32)).astype(BF16)

        @pl.when(is_end)
        def _():
            end_to_partner(k).wait_recv()
            sums_to_end(k).wait_recv()
            token_out[:, columns] = (summed(k, z, 2) + gf_in[k, 0].astype(F32)).astype(BF16)

        return carry

    lax.fori_loop(0, subs, third, 0)

    finish(1)
    for w in range(3):
        for way in range(2):
            relay_to(w, way).wait_send()
            pair_to(w, way).wait_send()
    for step in range(1, ranks):
        dots_to((me + step) % ranks).wait_send()

    def drain(k, carry):
        @pl.when(is_mid)
        def _():
            to_partner(k).wait_send()
            for home in range(2):
                sums_across(k, home).wait_send()
            sums_to_end(k).wait_send()

        @pl.when(is_end)
        def _():
            for core in range(2):
                far_home(k, core).wait_send()
                near_home(k, core).wait_send()
            end_to_partner(k).wait_send()

        return carry

    lax.fori_loop(0, subs, drain, 0)


def backward_call(ids_t, weight_t, table, dots, full, rows, hidden, delta, down, cap):
    groups, ranks = lax.axis_size("dp"), lax.axis_size("expert")
    _, _, slot_rows, width = rows.shape
    count = table.shape[2]
    inner = hidden.shape[2]
    subs, narrow = 2 * groups, width // 2
    full = full.reshape(2, subs, narrow, inner)
    hbm = pl.BlockSpec(memory_space=pl.ANY)
    vmem = pl.BlockSpec(memory_space=pltpu.VMEM)
    dma = pltpu.SemaphoreType.DMA
    return pl.pallas_call(
        functools.partial(backward_kernel, cap),
        out_shape=(
            jax.ShapeDtypeStruct((count, groups * width), BF16),
            jax.ShapeDtypeStruct(ids_t.shape, F32),
            jax.ShapeDtypeStruct((width, inner), BF16),
            jax.ShapeDtypeStruct((width, inner), BF16),
            jax.ShapeDtypeStruct((inner, width), BF16),
        ),
        in_specs=[vmem, vmem, vmem, vmem, hbm, hbm, hbm, hbm, hbm],
        out_specs=(vmem,) * 5,
        scratch_shapes=[
            pltpu.VMEM(full.shape, BF16),
            pltpu.VMEM(rows.shape, BF16),
            pltpu.VMEM(hidden.shape, BF16),
            pltpu.VMEM(delta.shape, BF16),
            pltpu.VMEM((subs, ranks, slot_rows, narrow), BF16),
            pltpu.VMEM((subs, 4, 4, slot_rows, narrow), BF16),
            pltpu.VMEM((subs, 2, count, narrow), BF16),
            pltpu.VMEM((subs, 2, count, narrow), BF16),
            pltpu.VMEM((subs, count, narrow), BF16),
            pltpu.VMEM((4, 4 * slot_rows, count), BF16),
            pltpu.VMEM((2, width, inner), BF16),
            pltpu.VMEM((2, 2, width, inner), BF16),
            pltpu.VMEM((inner, width), BF16),
            pltpu.VMEM((2, 2, width // 2, inner), BF16),
            pltpu.VMEM((2, inner // 2, width // groups), BF16),
            pltpu.VMEM((2, 2, width, inner), BF16),
            pltpu.VMEM((2, inner, width // groups), BF16),
            pltpu.VMEM(dots.shape, F32),
            dma((12,)), dma((subs,)), dma((subs,)), dma((subs, 2)), dma((subs, 2)),
            dma((subs, 2)), dma((subs, 2)), dma((subs, 2)), dma((subs, 2)), dma((subs,)), dma((subs,)),
            dma((ranks,)), dma((ranks,)), dma((3, 2)), dma((3, 2)), dma((3, 2)), dma((3, 2)),
        ],
        compiler_params=pltpu.CompilerParams(
            collective_id=1, has_side_effects=True, vmem_limit_bytes=67000000
        ),
    )(ids_t, weight_t, table, dots, full, rows, hidden, delta, down)


def swap(block, axis, distance):
    ranks = lax.axis_size(axis)
    return lax.ppermute(block, axis, [(rank, rank ^ distance) for rank in range(ranks)])


def any_mesh(tokens, out_grad, expert_ids, route_weight, w_gate, w_up, w_down):
    tok_count = tokens.shape[0]
    route_count = expert_ids.shape[1]
    ranks = lax.axis_size("expert")
    groups = lax.axis_size("dp")
    me = lax.axis_index("expert")
    group = lax.axis_index("dp")
    capacity = 3 * tok_count * route_count // (2 * ranks)
    routes = tok_count * route_count
    total_slots = ranks * capacity
    full_gate = lax.all_gather(w_gate[0], "dp", axis=0, tiled=True)
    full_up = lax.all_gather(w_up[0], "dp", axis=0, tiled=True)
    full_down = lax.all_gather(w_down[0], "dp", axis=1, tiled=True)
    half = ranks // 2
    flat_ids = expert_ids.reshape(routes)
    one_hot = (flat_ids[:, None] == jnp.arange(ranks, dtype=jnp.int32)[None, :]).astype(jnp.int32)
    slot_order = jnp.sum((jnp.cumsum(one_hot, axis=0) - 1) * one_hot, axis=1)
    slot_order = slot_order.reshape(tok_count, route_count)
    routing = jnp.concatenate(
        [
            expert_ids.astype(jnp.float32),
            slot_order.astype(jnp.float32),
            route_weight.astype(jnp.float32),
        ],
        axis=1,
    )
    far_routing = swap(routing, "expert", half)
    far_ids = far_routing[:, :route_count].astype(jnp.int32)
    far_order = far_routing[:, route_count : 2 * route_count].astype(jnp.int32)
    far_weight = far_routing[:, 2 * route_count :].astype(jnp.bfloat16)
    far_tokens = swap(tokens, "expert", half)
    late_grad, slot_order = lax.optimization_barrier((out_grad, slot_order))
    far_grad = swap(late_grad, "expert", half)
    slots = jnp.arange(total_slots, dtype=jnp.int32)

    def selectors(destination, weight, count):
        picks = jnp.zeros((count, tok_count), jnp.bfloat16)
        weighted = jnp.zeros((count, tok_count), jnp.bfloat16)
        for k in range(route_count):
            hit = slots[:count, None] == destination[:, k][None, :]
            picks = jnp.where(hit, jnp.ones((), jnp.bfloat16), picks)
            weighted = jnp.where(hit, weight[:, k][None, :], weighted)
        return picks, weighted

    destination = (expert_ids ^ me) * capacity + slot_order
    far_destination = (far_ids ^ me) * capacity + far_order
    near_slots = half * capacity
    picks, _ = selectors(destination, route_weight, total_slots)
    near_picks, near_weighted = selectors(destination, route_weight, near_slots)
    far_picks, far_weighted = selectors(far_destination, far_weight, near_slots)

    def blocks(buffer, count=ranks):
        return [buffer[d * capacity : (d + 1) * capacity] for d in range(count)]

    def exchange(buffer, count=ranks):
        return [
            swap(block, "expert", d) if d else block for d, block in enumerate(blocks(buffer, count))
        ]

    rows_in = jnp.concatenate(
        exchange(dot(near_picks, tokens, 1, 0).astype(jnp.bfloat16), half)
        + exchange(dot(far_picks, far_tokens, 1, 0).astype(jnp.bfloat16), half)
    )
    gate_value = dot(rows_in, full_gate, 1, 0)
    up_value = dot(rows_in, full_up, 1, 0)
    sigmoid_gate = jax.nn.sigmoid(gate_value)
    activated = gate_value * sigmoid_gate
    hidden = (activated * up_value).astype(jnp.bfloat16)
    scaled_blocks = exchange(
        dot(near_weighted, late_grad, 1, 0).astype(jnp.bfloat16), half
    ) + exchange(dot(far_weighted, far_grad, 1, 0).astype(jnp.bfloat16), half)
    scaled_blocks, hidden = lax.optimization_barrier((scaled_blocks, hidden))
    scaled = jnp.concatenate(scaled_blocks)
    hidden_grad = dot(scaled, full_down, 1, 1)
    gate_delta = (
        hidden_grad * up_value * sigmoid_gate * (1.0 + gate_value * (1.0 - sigmoid_gate))
    ).astype(jnp.bfloat16)
    up_delta = (hidden_grad * activated).astype(jnp.bfloat16)
    input_grad = (
        dot(gate_delta, full_gate, 1, 1) + dot(up_delta, full_up, 1, 1)
    ).astype(jnp.bfloat16)
    back_blocks = []
    for d, block in enumerate(blocks(input_grad)):
        back_blocks.append(swap(block, "expert", d) if d else block)
    down_part = dot(hidden, scaled, 0, 0).astype(jnp.bfloat16)
    input_grad, rows_in, hidden = lax.optimization_barrier((input_grad, rows_in, hidden))
    expert_out = dot(hidden, full_down, 1, 0)
    weighted_dot = jnp.sum(expert_out * scaled.astype(jnp.float32), axis=1)
    gate_part = dot(rows_in, gate_delta, 0, 0).astype(jnp.bfloat16)
    up_part = dot(rows_in, up_delta, 0, 0).astype(jnp.bfloat16)
    down_grad = lax.psum_scatter(down_part, "dp", scatter_dimension=1, tiled=True)[None]
    gate_grad = lax.psum_scatter(gate_part, "dp", scatter_dimension=0, tiled=True)[None]
    depth = up_part.shape[0] // groups
    up_sum = jnp.zeros((depth, up_part.shape[1]), jnp.float32)
    for d in range(groups):
        piece = lax.dynamic_slice_in_dim(up_part, (group ^ d) * depth, depth, 0)
        up_sum = up_sum + (swap(piece, "dp", d) if d else piece).astype(jnp.float32)
    up_grad = up_sum.astype(jnp.bfloat16)[None]

    token_sum = jnp.zeros(tokens.shape, jnp.float32)
    for pick, block in zip(blocks(picks), back_blocks):
        token_sum = token_sum + dot(pick, block, 0, 0)
    token_grad = token_sum.astype(jnp.bfloat16)

    order = jnp.arange(ranks, dtype=jnp.int32)
    dots = weighted_dot.reshape(ranks, capacity)
    by_rank = jnp.sum(
        jnp.where(((order ^ me)[:, None] == order[None, :])[:, :, None], dots[None], 0.0), axis=1
    )
    back_dots = lax.all_to_all(by_rank, "expert", split_axis=0, concat_axis=0, tiled=True)
    arrival = expert_ids * capacity + slot_order
    hits = arrival.reshape(tok_count, route_count, 1) == slots[None, None, :]
    own_dots = jnp.sum(jnp.where(hits, back_dots.reshape(total_slots)[None, None, :], 0.0), axis=2)
    route_grad = (own_dots / route_weight.astype(jnp.float32)).astype(jnp.bfloat16)
    return (token_grad, route_grad, gate_grad, up_grad, down_grad)


def on_device(tokens, out_grad, expert_ids, route_weight, w_gate, w_up, w_down):
    count = tokens.shape[0]
    cap = 3 * count * expert_ids.shape[1] // (2 * lax.axis_size("expert"))
    ids_t, weight_t = expert_ids.T, route_weight.T.astype(F32)
    full, rows, hidden, delta, dots, table, down = forward_call(
        ids_t, weight_t, tokens, out_grad, w_gate, w_up, w_down, cap
    )
    token_grad, route_grad, gate_grad, up_grad, down_grad = backward_call(
        ids_t, weight_t, table, dots, full, rows, hidden, delta, down, cap
    )
    return token_grad, route_grad.T.astype(BF16), gate_grad[None], up_grad[None], down_grad[None]


def solution(mesh):
    placed = (
        P(("dp", "expert"), None),
        P(("dp", "expert"), None),
        P(("dp", "expert"), None),
        P(("dp", "expert"), None),
        P("expert", "dp", None),
        P("expert", "dp", None),
        P("expert", None, "dp"),
    )
    chained = mesh.shape["expert"] == 8 and mesh.shape["dp"] == 4
    return jax.shard_map(
        on_device if chained else any_mesh, mesh=mesh, in_specs=placed,
        out_specs=(
            P(("dp", "expert"), None),
            P(("dp", "expert"), None),
            P("expert", "dp", None),
            P("expert", "dp", None),
            P("expert", None, "dp"),
        ),
        check_vma=False,
    )
```

```python
import functools
import jax
import jax.numpy as jnp
from jax import lax
from jax.experimental import pallas as pl
from jax.experimental.pallas import tpu as pltpu
from jax.sharding import PartitionSpec as P


MESH = pl.DeviceIdType.MESH
BF16 = jnp.bfloat16
F32 = jnp.float32


def dot(left, right, over_left=1, over_right=0):
    return lax.dot_general(
        left, right, (((over_left,), (over_right,)), ((), ())), preferred_element_type=F32
    )


class Chain:
    def __init__(self):
        self.g = lax.axis_index("dp")
        self.me = lax.axis_index("expert")
        self.c = self.me % 2
        self.z = self.me // 2
        self.half = self.z // 2
        self.far = 1 - self.half
        self.is_mid = (self.z + self.half) % 2 == 1
        self.is_end = (self.z + self.half) % 2 == 0
        self.z_mid = 1 + self.half
        self.z_end = 3 * self.half
        self.z_far_mid = 1 + self.far
        self.z_far_end = 3 * self.far
        self.z_near = self.z_mid + self.z_end - self.z

    def at(self, z, c):
        return (self.g, 2 * z + c)


def greet(chain, ranks, groups, meanwhile=None):
    barrier = pltpu.get_barrier_semaphore()
    for step in range(1, ranks):
        pl.semaphore_signal(
            barrier, inc=1, device_id=(chain.g, (chain.me + step) % ranks), device_id_type=MESH
        )
    for step in range(1, groups):
        pl.semaphore_signal(
            barrier, inc=1, device_id=((chain.g + step) % groups, chain.me), device_id_type=MESH
        )
    if meanwhile is not None:
        meanwhile()
    pl.semaphore_wait(barrier, ranks + groups - 2)


def neighbours(g):
    along_x = g + 1 - 2 * (g % 2)
    along_y = (g + 2) % 4
    return along_x, along_y


def send(src, dst, send_sem, recv_sem, device):
    return pltpu.make_async_remote_copy(
        src_ref=src, dst_ref=dst, send_sem=send_sem, recv_sem=recv_sem,
        device_id=device, device_id_type=MESH,
    )


def forward_kernel(
    cap,
    ids_ref, weight_ref, tokens_ref, grads_ref, wg_ref, wu_ref, wd_ref,
    full_out, rows_out, hidden_out, delta_out, dots_out, table_out, down_out,
    raw, rows, stage_d, stage_e, full_gate, full_up, full_down, gate_val, up_val, hg_val, select,
    down_part, down_relay, down_in,
    load_sem, raw_ss, raw_rs, e_ss, e_rs, d_ss, d_rs, tab_ss, tab_rs,
    w_ls, wa_ss, wa_rs, wf_ss, wf_rs, out_sem, relay_ss, relay_rs, pair_ss, pair_rs,
):
    chain = Chain()
    g, me, c, z = chain.g, chain.me, chain.c, chain.z
    is_mid, is_end = chain.is_mid, chain.is_end
    groups = lax.axis_size("dp")
    ranks = lax.axis_size("expert")
    steps = 2 * groups
    width = raw.shape[-1]
    count = raw.shape[2]
    slot_rows = rows.shape[2]
    along_x, along_y = neighbours(g)
    fulls = (full_gate, full_up, full_down)
    shards = (wg_ref, wu_ref, wd_ref)

    sub = width // groups
    for k in range(groups):
        pltpu.make_async_copy(
            tokens_ref.at[:, pl.ds(k * width, width)], raw.at[0, k], load_sem.at[k]
        ).start()
    for i in range(groups):
        for owner in range(groups):
            pltpu.make_async_copy(
                grads_ref.at[:, pl.ds(owner * width + i * sub, sub)],
                raw.at[0, groups + i, :, pl.ds(owner * sub, sub)], load_sem.at[groups + i],
            ).start()
    for w in range(3):
        pltpu.make_async_copy(shards[w].at[0], fulls[w].at[g], w_ls.at[w]).start()

    def shard_to(w, way):
        device = (along_x, me) if way == 0 else (along_y, me)
        return send(shards[w].at[0], fulls[w].at[g], wa_ss.at[w, way], wa_rs.at[w, way], device)

    def forward_half(w, way):
        owner = along_y if way == 0 else along_x
        device = (along_x, me) if way == 0 else (along_y, me)
        half = fulls[w].shape[1] // 2
        piece = fulls[w].at[owner, pl.ds(way * half, half)]
        return send(piece, piece, wf_ss.at[w, way], wf_rs.at[w, way], device)

    def build_table():
        experts = lax.broadcasted_iota(jnp.int32, (ranks, count), 0)
        named = [experts == ids_ref[k : k + 1, :] for k in range(ids_ref.shape[0])]
        hits = functools.reduce(jnp.logical_or, named)
        before = lax.broadcasted_iota(jnp.int32, (count, count), 0) < lax.broadcasted_iota(
            jnp.int32, (count, count), 1
        )
        order = dot(hits.astype(F32).astype(BF16), before.astype(F32).astype(BF16))
        table_out[0, 0:ranks, :] = jnp.where(hits, order, -1.0)
        weight = jnp.zeros((ranks, count), F32)
        for k in range(ids_ref.shape[0]):
            weight = jnp.where(named[k], weight_ref[k : k + 1, :].astype(F32), weight)
        table_out[0, ranks : 2 * ranks, :] = weight

        rows[:, :, cap:, :] = jnp.zeros((steps, ranks, slot_rows - cap, width), BF16)

    def table_send(slot, sem, zz):
        return send(
            table_out.at[0], table_out.at[slot], tab_ss.at[sem], tab_rs.at[slot - 1], chain.at(zz, c)
        )

    targets = (me, me + 1 - 2 * c, 2 * chain.z_near, 2 * chain.z_near + 1)

    def selectors(j):
        slots = lax.broadcasted_iota(jnp.int32, (slot_rows, count), 0).astype(F32)
        for i, rank in enumerate(targets):
            hit = table_out[j, pl.ds(rank, 1), :] == slots
            block = pl.ds(i * slot_rows, slot_rows)
            select[0, j, block, :] = jnp.where(hit, 1.0, 0.0).astype(BF16)
            select[1, j, block, :] = jnp.where(
                hit, table_out[j, pl.ds(ranks + rank, 1), :], 0.0
            ).astype(BF16)

    def gather(j, k, z_from, blocks, e_slot):
        picked = dot(select[k // groups, j, 0 : blocks * slot_rows, :], raw[j, k]).astype(BF16)
        parts = [picked[i * slot_rows : (i + 1) * slot_rows] for i in range(blocks)]
        rows[k, 4 * c + z_from] = parts[0]
        stage_d[k, z_from] = parts[1]
        for i in range(2, blocks):
            stage_e[k, i - 2, e_slot] = parts[i]

    full = pl.ds(0, cap)
    far_places = ((chain.z_far_mid, 1), (chain.z_far_end, 2))

    def own_raw(k):
        return send(raw.at[0, k], raw.at[2, k], raw_ss.at[0, k], raw_rs.at[1, k], chain.at(chain.z_far_mid, c))

    def end_raw(k):
        return send(raw.at[0, k], raw.at[1, k], raw_ss.at[0, k], raw_rs.at[0, k], chain.at(chain.z_mid, c))

    def onward_raw(k):
        return send(raw.at[1, k], raw.at[3, k], raw_ss.at[1, k], raw_rs.at[2, k], chain.at(chain.z_far_mid, c))

    def own_to_end(k, i):
        return send(
            stage_e.at[k, i, 0, full], rows.at[k, 4 * c + z, full],
            e_ss.at[k, 0, i], e_rs.at[k, 0, c], chain.at(chain.z_end, i),
        )

    def far_to_end(k, i, which):
        z_from, slot = far_places[which]
        return send(
            stage_e.at[k, i, slot, full], rows.at[k, 4 * c + z_from, full],
            e_ss.at[k, 1 + which, i], e_rs.at[k, 1 + which, c], chain.at(chain.z_end, i),
        )

    def mid_to_partner(k):
        return send(
            stage_d.at[k, :, full], rows.at[k, pl.ds(4 * c, 4), full], d_ss.at[k], d_rs.at[k], chain.at(z, 1 - c)
        )

    def end_to_partner(k):
        return send(
            stage_d.at[k, z, full], rows.at[k, 4 * c + z, full], d_ss.at[k], d_rs.at[k], chain.at(z, 1 - c)
        )

    def own_block_from(k, core):
        return send(
            stage_e.at[k, 0, 0, full], rows.at[k, 4 * core + chain.z_mid, full],
            e_ss.at[k, 0, 0], e_rs.at[k, 0, core], chain.at(chain.z_mid, core),
        )

    def far_block_from(k, core, which):
        return send(
            stage_e.at[k, 0, 1, full], rows.at[k, 4 * core + far_places[which][0], full],
            e_ss.at[k, 1 + which, 0], e_rs.at[k, 1 + which, core], chain.at(chain.z_mid, core),
        )

    def landed(k):
        @pl.when(is_mid)
        def _():
            mid_to_partner(k).wait_recv()

        @pl.when(is_end)
        def _():
            end_to_partner(k).wait_recv()
            for core in range(2):
                own_block_from(k, core).wait_recv()
                for which in range(2):
                    far_block_from(k, core, which).wait_recv()

    def load_wait(k):
        pltpu.make_async_copy(
            tokens_ref.at[:, pl.ds(0, width)], raw.at[0, k], load_sem.at[k]
        ).wait()

    across = groups - 1 - g
    slots = ranks * slot_rows
    half_inner = hidden_out.shape[2] // 2

    def hidden_grad(q, carry):
        landed(groups + q)

        def tile(t, carry):
            four = pl.ds(4 * t, 4)
            value = functools.reduce(jnp.add, [
                dot(
                    rows[groups + q, four, :, owner * sub : (owner + 1) * sub].reshape(4 * slot_rows, sub),
                    full_down[owner, :, pl.ds(pl.multiple_of(q * sub, 128), sub)], 1, 1,
                )
                for owner in range(groups)
            ]).reshape(4, slot_rows, hg_val.shape[2])

            @pl.when(q == 0)
            def _():
                hg_val[four] = value

            @pl.when(q > 0)
            def _():
                hg_val[four] += value

            return carry

        return lax.fori_loop(0, ranks // 4, tile, carry)

    def block_of(tile):
        return pl.ds(tile * half_inner, half_inner)

    def of_owner(owner):
        return pl.ds(pl.multiple_of(owner * sub, 128), sub)

    def relay_to(i, way):
        device = (along_x, me) if way == 0 else (along_y, me)
        return send(
            down_part.at[i, block_of(way), of_owner(across)], down_relay.at[i, way],
            relay_ss.at[i, way], relay_rs.at[i, way], device,
        )

    def pair_to(i, way):
        owner = along_x if way == 0 else along_y
        return send(
            down_part.at[i, :, of_owner(owner)], down_in.at[i, way],
            pair_ss.at[i, way], pair_rs.at[i, way], (owner, me),
        )

    def down_make(i):
        for tile in range(2):
            left = hidden_out[:, :, tile * half_inner : (tile + 1) * half_inner].reshape(slots, half_inner)
            down_part[i, block_of(tile), :] = dot(
                left, rows[groups + i].reshape(slots, width), 0, 0
            ).astype(BF16)
        for way in range(2):
            relay_to(i, way).start()

    def down_pass(i):
        for way in range(2):
            owner = along_x if way == 0 else along_y
            relay_to(i, 1 - way).wait_recv()
            place = (i, block_of(1 - way), of_owner(owner))
            down_part[place] = (
                down_part[place].astype(F32) + down_relay[i, 1 - way].astype(F32)
            ).astype(BF16)
            pair_to(i, way).start()

    def down_own(i):
        for way in range(2):
            pair_to(i, way).wait_recv()
        total = down_part[i, :, of_owner(g)].astype(F32)
        for way in range(2):
            total = total + down_in[i, way].astype(F32)
        down_out[:, of_owner(i)] = total.astype(BF16)

    ahead = 2

    def prologue():
        build_table()
        selectors(0)
        for k in range(ahead):
            load_wait(k)

            @pl.when(is_mid)
            def _():
                gather(0, k, z, 4, 0)

    greet(chain, ranks, groups, prologue)
    for way in range(2):
        shard_to(0, way).start()

    @pl.when(is_mid)
    def _():
        own_raw(0).start()
        for k in range(ahead):
            own_to_end(k, 0).start()
            own_to_end(k, 1).start()

    @pl.when(is_end)
    def _():
        end_raw(0).start()
        table_send(1, 0, chain.z_mid).start()
        table_send(3, 1, chain.z_far_mid).start()

    @pl.when(is_mid)
    def _():
        table_send(2, 0, chain.z_far_mid).start()

    for w in range(1, 3):
        for way in range(2):
            shard_to(w, way).start()
    for k in range(ahead, steps):
        load_wait(k)

    @pl.when(is_end)
    def _():
        for k in range(1, steps):
            end_raw(k).start()

    def step(k, carry):
        @pl.when(is_mid & (k < steps))
        def _():
            @pl.when(k > 0)
            def _():
                own_raw(k).start()

            @pl.when(k == 0)
            def _():
                table_send(1, 0, chain.z_mid).wait_recv()
                selectors(1)

            end_raw(k).wait_recv()
            onward_raw(k).start()

            @pl.when(k + ahead < steps)
            def _():
                gather(0, k + ahead, z, 4, 0)
                own_to_end(k + ahead, 0).start()
                own_to_end(k + ahead, 1).start()

            gather(1, k, chain.z_end, 2, 0)

        @pl.when(is_mid & (k >= 1))
        def _():
            @pl.when(k == 1)
            def _():
                table_send(2, 0, chain.z_far_mid).wait_recv()
                table_send(3, 0, chain.z_far_mid).wait_recv()
                selectors(2)
                selectors(3)

            j = k - 1
            own_raw(j).wait_recv()
            gather(2, j, chain.z_far_mid, 4, 1)
            far_to_end(j, 0, 0).start()
            far_to_end(j, 1, 0).start()
            onward_raw(j).wait_recv()
            gather(3, j, chain.z_far_end, 4, 2)
            far_to_end(j, 0, 1).start()
            far_to_end(j, 1, 1).start()
            mid_to_partner(j).start()

        @pl.when(is_end & (k < steps))
        def _():
            gather(0, k, z, 2, 0)
            end_to_partner(k).start()

        for w in range(3):
            @pl.when(k == w + 2)
            def _():
                for way in range(2):
                    shard_to(w, 1 - way).wait_recv()
                    forward_half(w, way).start()

        @pl.when(k == groups + 1)
        def _():
            for kk in range(groups):
                landed(kk)
            for w in range(2):
                pltpu.make_async_copy(shards[w].at[0], fulls[w].at[g], w_ls.at[w]).wait()
                for way in range(2):
                    forward_half(w, way).wait_recv()

        @pl.when((k == groups + 1) | (k == groups + 2))
        def _():
            def forward(p, carry):
                pair = pl.ds(2 * p, 2)
                shape = (2, slot_rows, gate_val.shape[2])
                piece = [rows[kk, pair].reshape(2 * slot_rows, width) for kk in range(groups)]
                gate = functools.reduce(jnp.add, [dot(piece[kk], full_gate[kk]) for kk in range(groups)])
                up = functools.reduce(jnp.add, [dot(piece[kk], full_up[kk]) for kk in range(groups)])
                gate_val[pair] = gate.reshape(shape)
                up_val[pair] = up.reshape(shape)
                hidden_out[pair] = (gate * jax.nn.sigmoid(gate) * up).astype(BF16).reshape(shape)
                return carry

            start = (k - groups - 1) * (ranks // 4)
            lax.fori_loop(start, start + ranks // 4, forward, 0)

        @pl.when(k == groups + 2)
        def _():
            pltpu.make_async_copy(shards[2].at[0], fulls[2].at[g], w_ls.at[2]).wait()
            for way in range(2):
                forward_half(2, way).wait_recv()

        @pl.when(k >= groups + 2)
        def _():
            q = k - groups - 2

            @pl.when(q >= 1)
            def _():
                down_pass(q - 1)

            hidden_grad(q, 0)
            down_make(q)

        return carry

    lax.fori_loop(0, steps + 1, step, 0)

    outs = [
        pltpu.make_async_copy(full_gate, full_out.at[0], out_sem.at[0]),
        pltpu.make_async_copy(full_up, full_out.at[1], out_sem.at[1]),
    ]
    for copy in outs:
        copy.start()
    first = pltpu.make_async_copy(rows.at[pl.ds(0, groups)], rows_out.at[pl.ds(0, groups)], out_sem.at[2])
    first.start()

    down_pass(groups - 2)
    hidden_grad(groups - 1, 0)
    late = pltpu.make_async_copy(rows.at[steps - 1], rows_out.at[groups], out_sem.at[3])
    late.start()

    def deltas(t, carry):
        gate, up, grad = gate_val[t], up_val[t], hg_val[t]
        sig = jax.nn.sigmoid(gate)
        delta_out[0, t] = (grad * up * sig * (1.0 + gate * (1.0 - sig))).astype(BF16)
        delta_out[1, t] = (grad * (gate * sig)).astype(BF16)
        total = jnp.sum(hidden_out[t].astype(F32) * grad, axis=1, keepdims=True)
        dots_out[t] = jnp.broadcast_to(total, (total.shape[0], total.shape[0])).T[0:8, :]
        return carry

    lax.fori_loop(0, ranks, deltas, 0)

    for copy in outs:
        copy.wait()
    first.wait()
    late.wait()

    def finish_down(i, carry):
        down_own(i)
        for way in range(2):
            relay_to(i, way).wait_send()
            pair_to(i, way).wait_send()
        return carry

    lax.fori_loop(0, groups - 1, finish_down, 0)
    for w in range(3):
        for way in range(2):
            shard_to(w, way).wait_send()
            forward_half(w, way).wait_send()

    def drain(k, carry):
        @pl.when(is_mid)
        def _():
            own_raw(k).wait_send()
            onward_raw(k).wait_send()
            for i in range(2):
                own_to_end(k, i).wait_send()
                for which in range(2):
                    far_to_end(k, i, which).wait_send()
            mid_to_partner(k).wait_send()

        @pl.when(is_end)
        def _():
            end_raw(k).wait_send()
            end_to_partner(k).wait_send()

        return carry

    lax.fori_loop(0, steps, drain, 0)

    @pl.when(is_mid)
    def _():
        table_send(2, 0, chain.z_far_mid).wait_send()

    @pl.when(is_end)
    def _():
        table_send(1, 0, chain.z_mid).wait_send()
        table_send(3, 1, chain.z_far_mid).wait_send()


def forward_call(ids_t, weight_t, tokens, out_grad, w_gate, w_up, w_down, cap):
    count, depth = tokens.shape
    groups, ranks = lax.axis_size("dp"), lax.axis_size("expert")
    inner = w_gate.shape[2]
    width = depth // groups
    slot_rows = -(-cap // 16) * 16
    steps = 2 * groups
    hbm = pl.BlockSpec(memory_space=pl.ANY)
    vmem = pl.BlockSpec(memory_space=pltpu.VMEM)
    dma = pltpu.SemaphoreType.DMA
    return pl.pallas_call(
        functools.partial(forward_kernel, cap),
        out_shape=(
            jax.ShapeDtypeStruct((2, groups, width, inner), BF16),
            jax.ShapeDtypeStruct((groups + 1, ranks, slot_rows, width), BF16),
            jax.ShapeDtypeStruct((ranks, slot_rows, inner), BF16),
            jax.ShapeDtypeStruct((2, ranks, slot_rows, inner), BF16),
            jax.ShapeDtypeStruct((ranks, 8, slot_rows), F32),
            jax.ShapeDtypeStruct((4, 2 * ranks, count), F32),
            jax.ShapeDtypeStruct((inner, width), BF16),
        ),
        in_specs=[vmem, vmem, hbm, hbm, hbm, hbm, hbm],
        out_specs=(hbm, hbm, vmem, vmem, vmem, vmem, vmem),
        scratch_shapes=[
            pltpu.VMEM((4, steps, count, width), BF16),
            pltpu.VMEM((steps, ranks, slot_rows, width), BF16),
            pltpu.VMEM((steps, 4, slot_rows, width), BF16),
            pltpu.VMEM((steps, 2, 3, slot_rows, width), BF16),
            pltpu.VMEM((groups, width, inner), BF16),
            pltpu.VMEM((groups, width, inner), BF16),
            pltpu.VMEM((groups, inner, width), BF16),
            pltpu.VMEM((ranks, slot_rows, inner), F32),
            pltpu.VMEM((ranks, slot_rows, inner), F32),
            pltpu.VMEM((ranks, slot_rows, inner), F32),
            pltpu.VMEM((2, 4, 4 * slot_rows, count), BF16),
            pltpu.VMEM((groups - 1, inner, width), BF16),
            pltpu.VMEM((groups - 1, 2, inner // 2, width // groups), BF16),
            pltpu.VMEM((groups - 1, 2, inner, width // groups), BF16),
            dma((steps,)), dma((2, steps)), dma((3, steps)), dma((steps, 3, 2)), dma((steps, 3, 2)),
            dma((steps,)), dma((steps,)), dma((2,)), dma((3,)),
            dma((3,)), dma((3, 2)), dma((3, 2)), dma((3, 2)), dma((3, 2)), dma((4,)),
            dma((groups - 1, 2)), dma((groups - 1, 2)), dma((groups - 1, 2)), dma((groups - 1, 2)),
        ],
        compiler_params=pltpu.CompilerParams(
            collective_id=0, has_side_effects=True, vmem_limit_bytes=67000000
        ),
    )(ids_t, weight_t, tokens, out_grad, w_gate, w_up, w_down)


def backward_kernel(
    cap,
    ids_ref, weight_ref, table_ref, dots_ref, full_ref, rows_ref, hidden_ref, delta_ref, down_ref,
    token_out, route_out, gate_out, up_out, down_out,
    full, rows, hidden, delta, grads, comb, gf_send, gf_in, end_send, select,
    diag_gu, pair_gu, pair_d, relay_gu, relay_d, in_gu, in_d, dots_in,
    load_sem, d_ss, d_rs, far_ss, far_rs, near_ss, near_rs, gf_ss, gf_rs, es_ss, es_rs,
    dots_ss, dots_rs, relay_ss, relay_rs, pair_ss, pair_rs,
):
    chain = Chain()
    g, me, c, z = chain.g, chain.me, chain.c, chain.z
    is_mid, is_end = chain.is_mid, chain.is_end
    groups = lax.axis_size("dp")
    ranks = lax.axis_size("expert")
    _, slot_rows, width = rows.shape[1:]
    count = table_ref.shape[2]
    inner = hidden.shape[2]
    along_x, along_y = neighbours(g)
    across = groups - 1 - g
    slots = ranks * slot_rows
    subs, narrow = grads.shape[0], grads.shape[3]

    loads = [
        pltpu.make_async_copy(delta_ref, delta, load_sem.at[0]),
        pltpu.make_async_copy(full_ref.at[:, 0], full.at[:, 0], load_sem.at[1]),
        pltpu.make_async_copy(rows_ref.at[across], rows.at[across], load_sem.at[2]),
        pltpu.make_async_copy(full_ref.at[:, pl.ds(1, subs - 1)], full.at[:, pl.ds(1, subs - 1)], load_sem.at[3]),
        pltpu.make_async_copy(rows_ref.at[groups], rows.at[groups], load_sem.at[4]),
        pltpu.make_async_copy(hidden_ref, hidden, load_sem.at[5]),
    ]
    for i, shard in enumerate((along_x, along_y, g)):
        loads.append(pltpu.make_async_copy(rows_ref.at[shard], rows.at[shard], load_sem.at[6 + i]))
    for copy in loads:
        copy.start()
    sub = width // groups
    half_inner = inner // 2
    down_ready = pltpu.make_async_copy(down_ref, down_out, load_sem.at[9])
    down_ready.start()

    def of_owner(owner):
        return pl.ds(pl.multiple_of(owner * sub, 128), sub)

    greet(chain, ranks, groups)

    real = pl.ds(0, cap)

    def dots_to(peer):
        return send(
            dots_ref.at[4 * (peer % 2) + peer // 2], dots_in.at[me],
            dots_ss.at[peer], dots_rs.at[me], (g, peer),
        )

    def dots_from(peer):
        return send(
            dots_ref.at[4 * c + z], dots_in.at[peer], dots_ss.at[peer], dots_rs.at[peer], (g, peer)
        )

    for step in range(1, ranks):
        dots_to((me + step) % ranks).start()

    comb[:, :, :, cap:, :] = jnp.zeros((subs, 4, 4, slot_rows - cap, narrow), BF16)
    targets = (me, me + 1 - 2 * c, 2 * chain.z_near, 2 * chain.z_near + 1)

    def selectors(j, z_from):
        slot = lax.broadcasted_iota(jnp.int32, (slot_rows, count), 0).astype(F32)
        for i, rank in enumerate(targets):
            hit = table_ref[j, pl.ds(rank, 1), :] == slot
            select[z_from, i * slot_rows : (i + 1) * slot_rows, :] = jnp.where(hit, 1.0, 0.0).astype(BF16)

    selectors(0, z)

    @pl.when(is_mid)
    def _():
        selectors(1, chain.z_end)
        selectors(2, chain.z_far_mid)
        selectors(3, chain.z_far_end)

    def to_partner(k):
        return send(
            grads.at[k, pl.ds(4 * (1 - c), 4), real], comb.at[k, :, 1, real],
            d_ss.at[k], d_rs.at[k], chain.at(z, 1 - c),
        )

    def end_to_partner(k):
        return send(
            grads.at[k, 4 * (1 - c) + z, real], comb.at[k, z, 1, real],
            d_ss.at[k], d_rs.at[k], chain.at(z, 1 - c),
        )

    def far_home(k, core):
        return send(
            grads.at[k, pl.ds(4 * core + 2 * chain.far, 2), real],
            comb.at[k, pl.ds(2 * chain.far, 2), 2 + c, real],
            far_ss.at[k, core], far_rs.at[k, c], chain.at(chain.z_mid, core),
        )

    def far_from(k, core):
        return send(
            grads.at[k, pl.ds(4 * core + 2 * chain.far, 2), real],
            comb.at[k, pl.ds(2 * chain.far, 2), 2 + core, real],
            far_ss.at[k, core], far_rs.at[k, core], chain.at(chain.z_end, core),
        )

    def near_home(k, core):
        return send(
            grads.at[k, 4 * core + chain.z_mid, real], comb.at[k, chain.z_mid, 2 + c, real],
            near_ss.at[k, core], near_rs.at[k, c], chain.at(chain.z_mid, core),
        )

    def near_from(k, core):
        return send(
            grads.at[k, 4 * core + chain.z_mid, real], comb.at[k, chain.z_mid, 2 + core, real],
            near_ss.at[k, core], near_rs.at[k, core], chain.at(chain.z_end, core),
        )

    def sums_across(k, home):
        return send(
            gf_send.at[k, home], gf_in.at[k, home], gf_ss.at[k, home], gf_rs.at[k, home], chain.at(chain.z_far_mid, c)
        )

    def sums_to_end(k):
        return send(end_send.at[k], gf_in.at[k, 0], es_ss.at[k], es_rs.at[k], chain.at(chain.z_end, c))

    def device_on(way):
        return ((along_x if way == 0 else along_y), me)

    def relay_to(w, way):
        if w == 2:
            src, dst = pair_d.at[pl.ds(way * half_inner, half_inner), of_owner(across)], relay_d.at[way]
        else:
            half = width // 2
            src, dst = diag_gu.at[w, pl.ds(way * half, half)], relay_gu.at[w, way]
        return send(src, dst, relay_ss.at[w, way], relay_rs.at[w, way], device_on(way))

    def pair_to(w, way):
        if w == 2:
            src, dst = pair_d.at[:, of_owner(along_x if way == 0 else along_y)], in_d.at[way]
        else:
            src, dst = pair_gu.at[w, way], in_gu.at[w, way]
        return send(src, dst, pair_ss.at[w, way], pair_rs.at[w, way], device_on(way))

    def part(w, shard, tile):
        half = width // 2
        left = rows[shard, :, :, tile * half : (tile + 1) * half].reshape(slots, half)
        return dot(left, delta[w].reshape(slots, inner), 0, 0)

    def diagonal(w):
        if w == 2:
            for tile in range(2):
                left = hidden[:, :, tile * half_inner : (tile + 1) * half_inner].reshape(slots, half_inner)
                pair_d[pl.ds(tile * half_inner, half_inner), :] = dot(
                    left, rows[groups].reshape(slots, width), 0, 0
                ).astype(BF16)
        else:
            half = width // 2
            for tile in range(2):
                diag_gu[w, pl.ds(tile * half, half), :] = part(w, across, tile).astype(BF16)
        for way in range(2):
            relay_to(w, way).start()

    def pairs(w):
        for way in range(2):
            shard = along_x if way == 0 else along_y
            relay_to(w, 1 - way).wait_recv()
            if w == 2:
                place = (pl.ds((1 - way) * half_inner, half_inner), of_owner(shard))
                pair_d[place] = (pair_d[place].astype(F32) + relay_d[1 - way].astype(F32)).astype(BF16)
            else:
                half = width // 2
                for tile in range(2):
                    value = part(w, shard, tile).astype(BF16)
                    if tile == 1 - way:
                        value = (value.astype(F32) + relay_gu[w, 1 - way].astype(F32)).astype(BF16)
                    pair_gu[w, way, pl.ds(tile * half, half), :] = value
            pair_to(w, way).start()

    def finish(w):
        for way in range(2):
            pair_to(w, way).wait_recv()
        if w == 2:
            total = pair_d[:, of_owner(g)].astype(F32)
            for way in range(2):
                total = total + in_d[way].astype(F32)
            down_ready.wait()
            down_out[:, of_owner(groups - 1)] = total.astype(BF16)
        else:
            half = width // 2
            for tile in range(2):
                value = part(w, g, tile)
                block = pl.ds(tile * half, half)
                for way in range(2):
                    value = value + in_gu[w, way, block, :].astype(F32)
                (gate_out, up_out)[w][block, :] = value.astype(BF16)

    def input_grad(k):
        for hc in range(2):
            left = [delta[w, pl.ds(4 * hc, 4)].reshape(4 * slot_rows, inner) for w in range(2)]
            value = (dot(left[0], full[0, k], 1, 1) + dot(left[1], full[1, k], 1, 1)).astype(BF16)
            value = value.reshape(4, slot_rows, narrow)
            grads[k, pl.ds(4 * hc, 4)] = value

            @pl.when(c == hc)
            def _():
                comb[k, :, 0] = value

    def summed(k, z_from, blocks):
        return dot(
            select[z_from, 0 : blocks * slot_rows, :],
            comb[k, z_from, 0:blocks].reshape(blocks * slot_rows, narrow), 0, 0,
        )

    for i in range(2):
        loads[i].wait()

    lag = 2

    def along(k, carry):
        @pl.when(k == 1)
        def _():
            loads[3].wait()

        @pl.when(k < subs)
        def _():
            input_grad(k)

            @pl.when(is_mid)
            def _():
                to_partner(k).start()

            @pl.when(is_end)
            def _():
                for core in range(2):
                    far_home(k, core).start()
                end_to_partner(k).start()

        @pl.when(is_end & (k == subs - 1))
        def _():
            for j in range(subs):
                for core in range(2):
                    near_home(j, core).start()

        for w in range(2):
            @pl.when(k == w)
            def _():
                if w == 0:
                    loads[2].wait()
                diagonal(w)

        @pl.when(k == 2)
        def _():
            loads[4].wait()
            loads[5].wait()

            diagonal(2)

        @pl.when(is_mid & (k >= 1) & (k <= subs))
        def _():
            j = k - 1
            to_partner(j).wait_recv()
            for core in range(2):
                far_from(j, core).wait_recv()
            gf_send[j, 1] = summed(j, chain.z_far_end, 4).astype(BF16)
            sums_across(j, 1).start()
            gf_send[j, 0] = summed(j, chain.z_far_mid, 4).astype(BF16)
            sums_across(j, 0).start()

        @pl.when(k == 3)
        def _():
            for copy in loads[6:]:
                copy.wait()

        for at, w in ((3, 0), (4, 2), (5, 1)):
            @pl.when(k == at)
            def _():
                pairs(w)

        @pl.when(is_mid & (k > lag))
        def _():
            j = k - 1 - lag
            sums_across(j, 1).wait_recv()
            end_send[j] = (summed(j, chain.z_end, 2) + gf_in[j, 1].astype(F32)).astype(BF16)
            sums_to_end(j).start()

        return carry

    lax.fori_loop(0, subs + 1 + lag, along, 0)

    for step in range(1, ranks):
        dots_from((me + step) % ranks).wait_recv()
    dots_in[me] = dots_ref[4 * c + z]
    found = jnp.zeros(ids_ref.shape, F32)
    slot = lax.broadcasted_iota(jnp.int32, (slot_rows, count), 0).astype(F32)
    for rank in range(ranks):
        hit = jnp.where(table_ref[0, rank : rank + 1, :] == slot, 1.0, 0.0)
        value = lax.dot_general(
            dots_in[rank], hit, (((1,), (0,)), ((), ())),
            precision=lax.Precision.HIGHEST, preferred_element_type=F32,
        )[0:1, :]
        found = jnp.where(ids_ref[...] == rank, value, found)
    route_out[...] = (found / weight_ref[...].astype(F32)).astype(BF16)

    def third(k, carry):
        columns = pl.ds(pl.multiple_of(k * narrow, 128), narrow)

        @pl.when(k == 0)
        def _():
            finish(0)

        @pl.when(k == 3)
        def _():
            finish(2)

        @pl.when(is_mid)
        def _():
            sums_across(k, 0).wait_recv()
            for core in range(2):
                near_from(k, core).wait_recv()
            token_out[:, columns] = (summed(k, z, 4) + gf_in[k, 0].astype(F32)).astype(BF16)

        @pl.when(is_end)
        def _():
            end_to_partner(k).wait_recv()
            sums_to_end(k).wait_recv()
            token_out[:, columns] = (summed(k, z, 2) + gf_in[k, 0].astype(F32)).astype(BF16)

        return carry

    lax.fori_loop(0, subs, third, 0)

    finish(1)
    for w in range(3):
        for way in range(2):
            relay_to(w, way).wait_send()
            pair_to(w, way).wait_send()
    for step in range(1, ranks):
        dots_to((me + step) % ranks).wait_send()

    def drain(k, carry):
        @pl.when(is_mid)
        def _():
            to_partner(k).wait_send()
            for home in range(2):
                sums_across(k, home).wait_send()
            sums_to_end(k).wait_send()

        @pl.when(is_end)
        def _():
            for core in range(2):
                far_home(k, core).wait_send()
                near_home(k, core).wait_send()
            end_to_partner(k).wait_send()

        return carry

    lax.fori_loop(0, subs, drain, 0)


def backward_call(ids_t, weight_t, table, dots, full, rows, hidden, delta, down, cap):
    groups, ranks = lax.axis_size("dp"), lax.axis_size("expert")
    _, _, slot_rows, width = rows.shape
    count = table.shape[2]
    inner = hidden.shape[2]
    subs, narrow = 2 * groups, width // 2
    full = full.reshape(2, subs, narrow, inner)
    hbm = pl.BlockSpec(memory_space=pl.ANY)
    vmem = pl.BlockSpec(memory_space=pltpu.VMEM)
    dma = pltpu.SemaphoreType.DMA
    return pl.pallas_call(
        functools.partial(backward_kernel, cap),
        out_shape=(
            pltpu.VMEM((count, groups * width), BF16),
            pltpu.VMEM(ids_t.shape, BF16),
            pltpu.VMEM((width, inner), BF16),
            pltpu.VMEM((width, inner), BF16),
            pltpu.VMEM((inner, width), BF16),
        ),
        in_specs=[vmem, vmem, vmem, vmem, hbm, hbm, hbm, hbm, hbm],
        out_specs=(vmem,) * 5,
        scratch_shapes=[
            pltpu.VMEM(full.shape, BF16),
            pltpu.VMEM(rows.shape, BF16),
            pltpu.VMEM(hidden.shape, BF16),
            pltpu.VMEM(delta.shape, BF16),
            pltpu.VMEM((subs, ranks, slot_rows, narrow), BF16),
            pltpu.VMEM((subs, 4, 4, slot_rows, narrow), BF16),
            pltpu.VMEM((subs, 2, count, narrow), BF16),
            pltpu.VMEM((subs, 2, count, narrow), BF16),
            pltpu.VMEM((subs, count, narrow), BF16),
            pltpu.VMEM((4, 4 * slot_rows, count), BF16),
            pltpu.VMEM((2, width, inner), BF16),
            pltpu.VMEM((2, 2, width, inner), BF16),
            pltpu.VMEM((inner, width), BF16),
            pltpu.VMEM((2, 2, width // 2, inner), BF16),
            pltpu.VMEM((2, inner // 2, width // groups), BF16),
            pltpu.VMEM((2, 2, width, inner), BF16),
            pltpu.VMEM((2, inner, width // groups), BF16),
            pltpu.VMEM(dots.shape, F32),
            dma((12,)), dma((subs,)), dma((subs,)), dma((subs, 2)), dma((subs, 2)),
            dma((subs, 2)), dma((subs, 2)), dma((subs, 2)), dma((subs, 2)), dma((subs,)), dma((subs,)),
            dma((ranks,)), dma((ranks,)), dma((3, 2)), dma((3, 2)), dma((3, 2)), dma((3, 2)),
        ],
        compiler_params=pltpu.CompilerParams(
            collective_id=1, has_side_effects=True, vmem_limit_bytes=58000000
        ),
    )(ids_t, weight_t, table, dots, full, rows, hidden, delta, down)


def hand_over_kernel(*refs):
    ins, outs, sem = refs[0:5], refs[5:10], refs[10]
    copies = [pltpu.make_async_copy(ins[i], outs[i], sem.at[i]) for i in range(5)]
    for copy in copies:
        copy.start()
    for copy in copies:
        copy.wait()


def hand_over(*arrays):
    return pl.pallas_call(
        hand_over_kernel,
        out_shape=tuple(jax.ShapeDtypeStruct(a.shape, a.dtype) for a in arrays),
        in_specs=[pl.BlockSpec(memory_space=pltpu.VMEM)] * 5,
        out_specs=(pl.BlockSpec(memory_space=pl.ANY),) * 5,
        scratch_shapes=[pltpu.SemaphoreType.DMA((5,))],
        compiler_params=pltpu.CompilerParams(vmem_limit_bytes=8000000),
    )(*arrays)


def swap(block, axis, distance):
    ranks = lax.axis_size(axis)
    return lax.ppermute(block, axis, [(rank, rank ^ distance) for rank in range(ranks)])


def any_mesh(tokens, out_grad, expert_ids, route_weight, w_gate, w_up, w_down):
    tok_count = tokens.shape[0]
    route_count = expert_ids.shape[1]
    ranks = lax.axis_size("expert")
    groups = lax.axis_size("dp")
    me = lax.axis_index("expert")
    group = lax.axis_index("dp")
    capacity = 3 * tok_count * route_count // (2 * ranks)
    routes = tok_count * route_count
    total_slots = ranks * capacity
    full_gate = lax.all_gather(w_gate[0], "dp", axis=0, tiled=True)
    full_up = lax.all_gather(w_up[0], "dp", axis=0, tiled=True)
    full_down = lax.all_gather(w_down[0], "dp", axis=1, tiled=True)
    half = ranks // 2
    flat_ids = expert_ids.reshape(routes)
    one_hot = (flat_ids[:, None] == jnp.arange(ranks, dtype=jnp.int32)[None, :]).astype(jnp.int32)
    slot_order = jnp.sum((jnp.cumsum(one_hot, axis=0) - 1) * one_hot, axis=1)
    slot_order = slot_order.reshape(tok_count, route_count)
    routing = jnp.concatenate(
        [
            expert_ids.astype(jnp.float32),
            slot_order.astype(jnp.float32),
            route_weight.astype(jnp.float32),
        ],
        axis=1,
    )
    far_routing = swap(routing, "expert", half)
    far_ids = far_routing[:, :route_count].astype(jnp.int32)
    far_order = far_routing[:, route_count : 2 * route_count].astype(jnp.int32)
    far_weight = far_routing[:, 2 * route_count :].astype(jnp.bfloat16)
    far_tokens = swap(tokens, "expert", half)
    late_grad, slot_order = lax.optimization_barrier((out_grad, slot_order))
    far_grad = swap(late_grad, "expert", half)
    slots = jnp.arange(total_slots, dtype=jnp.int32)

    def selectors(destination, weight, count):
        picks = jnp.zeros((count, tok_count), jnp.bfloat16)
        weighted = jnp.zeros((count, tok_count), jnp.bfloat16)
        for k in range(route_count):
            hit = slots[:count, None] == destination[:, k][None, :]
            picks = jnp.where(hit, jnp.ones((), jnp.bfloat16), picks)
            weighted = jnp.where(hit, weight[:, k][None, :], weighted)
        return picks, weighted

    destination = (expert_ids ^ me) * capacity + slot_order
    far_destination = (far_ids ^ me) * capacity + far_order
    near_slots = half * capacity
    picks, _ = selectors(destination, route_weight, total_slots)
    near_picks, near_weighted = selectors(destination, route_weight, near_slots)
    far_picks, far_weighted = selectors(far_destination, far_weight, near_slots)

    def blocks(buffer, count=ranks):
        return [buffer[d * capacity : (d + 1) * capacity] for d in range(count)]

    def exchange(buffer, count=ranks):
        return [
            swap(block, "expert", d) if d else block for d, block in enumerate(blocks(buffer, count))
        ]

    rows_in = jnp.concatenate(
        exchange(dot(near_picks, tokens, 1, 0).astype(jnp.bfloat16), half)
        + exchange(dot(far_picks, far_tokens, 1, 0).astype(jnp.bfloat16), half)
    )
    gate_value = dot(rows_in, full_gate, 1, 0)
    up_value = dot(rows_in, full_up, 1, 0)
    sigmoid_gate = jax.nn.sigmoid(gate_value)
    activated = gate_value * sigmoid_gate
    hidden = (activated * up_value).astype(jnp.bfloat16)
    scaled_blocks = exchange(
        dot(near_weighted, late_grad, 1, 0).astype(jnp.bfloat16), half
    ) + exchange(dot(far_weighted, far_grad, 1, 0).astype(jnp.bfloat16), half)
    scaled_blocks, hidden = lax.optimization_barrier((scaled_blocks, hidden))
    scaled = jnp.concatenate(scaled_blocks)
    hidden_grad = dot(scaled, full_down, 1, 1)
    gate_delta = (
        hidden_grad * up_value * sigmoid_gate * (1.0 + gate_value * (1.0 - sigmoid_gate))
    ).astype(jnp.bfloat16)
    up_delta = (hidden_grad * activated).astype(jnp.bfloat16)
    input_grad = (
        dot(gate_delta, full_gate, 1, 1) + dot(up_delta, full_up, 1, 1)
    ).astype(jnp.bfloat16)
    back_blocks = []
    for d, block in enumerate(blocks(input_grad)):
        back_blocks.append(swap(block, "expert", d) if d else block)
    down_part = dot(hidden, scaled, 0, 0).astype(jnp.bfloat16)
    input_grad, rows_in, hidden = lax.optimization_barrier((input_grad, rows_in, hidden))
    expert_out = dot(hidden, full_down, 1, 0)
    weighted_dot = jnp.sum(expert_out * scaled.astype(jnp.float32), axis=1)
    gate_part = dot(rows_in, gate_delta, 0, 0).astype(jnp.bfloat16)
    up_part = dot(rows_in, up_delta, 0, 0).astype(jnp.bfloat16)
    down_grad = lax.psum_scatter(down_part, "dp", scatter_dimension=1, tiled=True)[None]
    gate_grad = lax.psum_scatter(gate_part, "dp", scatter_dimension=0, tiled=True)[None]
    depth = up_part.shape[0] // groups
    up_sum = jnp.zeros((depth, up_part.shape[1]), jnp.float32)
    for d in range(groups):
        piece = lax.dynamic_slice_in_dim(up_part, (group ^ d) * depth, depth, 0)
        up_sum = up_sum + (swap(piece, "dp", d) if d else piece).astype(jnp.float32)
    up_grad = up_sum.astype(jnp.bfloat16)[None]

    token_sum = jnp.zeros(tokens.shape, jnp.float32)
    for pick, block in zip(blocks(picks), back_blocks):
        token_sum = token_sum + dot(pick, block, 0, 0)
    token_grad = token_sum.astype(jnp.bfloat16)

    order = jnp.arange(ranks, dtype=jnp.int32)
    dots = weighted_dot.reshape(ranks, capacity)
    by_rank = jnp.sum(
        jnp.where(((order ^ me)[:, None] == order[None, :])[:, :, None], dots[None], 0.0), axis=1
    )
    back_dots = lax.all_to_all(by_rank, "expert", split_axis=0, concat_axis=0, tiled=True)
    arrival = expert_ids * capacity + slot_order
    hits = arrival.reshape(tok_count, route_count, 1) == slots[None, None, :]
    own_dots = jnp.sum(jnp.where(hits, back_dots.reshape(total_slots)[None, None, :], 0.0), axis=2)
    route_grad = (own_dots / route_weight.astype(jnp.float32)).astype(jnp.bfloat16)
    return (token_grad, route_grad, gate_grad, up_grad, down_grad)


def on_device(tokens, out_grad, expert_ids, route_weight, w_gate, w_up, w_down):
    count = tokens.shape[0]
    cap = 3 * count * expert_ids.shape[1] // (2 * lax.axis_size("expert"))
    ids_t, weight_t = expert_ids.T, route_weight.T
    full, rows, hidden, delta, dots, table, down = forward_call(
        ids_t, weight_t, tokens, out_grad, w_gate, w_up, w_down, cap
    )
    token_grad, route_grad, gate_grad, up_grad, down_grad = backward_call(
        ids_t, weight_t, table, dots, full, rows, hidden, delta, down, cap
    )
    token_grad, gate_grad, up_grad, down_grad, route_grad = hand_over(
        token_grad, gate_grad, up_grad, down_grad, route_grad
    )
    return token_grad, route_grad.T, gate_grad[None], up_grad[None], down_grad[None]


def solution(mesh):
    placed = (
        P(("dp", "expert"), None),
        P(("dp", "expert"), None),
        P(("dp", "expert"), None),
        P(("dp", "expert"), None),
        P("expert", "dp", None),
        P("expert", "dp", None),
        P("expert", None, "dp"),
    )
    chained = mesh.shape["expert"] == 8 and mesh.shape["dp"] == 4
    return jax.shard_map(
        on_device if chained else any_mesh, mesh=mesh, in_specs=placed,
        out_specs=(
            P(("dp", "expert"), None),
            P(("dp", "expert"), None),
            P("expert", "dp", None),
            P("expert", "dp", None),
            P("expert", None, "dp"),
        ),
        check_vma=False,
    )
```

```python
import functools
import jax
import jax.numpy as jnp
from jax import lax
from jax.experimental import pallas as pl
from jax.experimental.pallas import tpu as pltpu
from jax.sharding import PartitionSpec as P


MESH = pl.DeviceIdType.MESH
BF16 = jnp.bfloat16
F32 = jnp.float32


def dot(left, right, over_left=1, over_right=0):
    return lax.dot_general(
        left, right, (((over_left,), (over_right,)), ((), ())), preferred_element_type=F32
    )


class Chain:
    def __init__(self):
        self.g = lax.axis_index("dp")
        self.me = lax.axis_index("expert")
        self.c = self.me % 2
        self.z = self.me // 2
        self.half = self.z // 2
        self.far = 1 - self.half
        self.is_mid = (self.z + self.half) % 2 == 1
        self.is_end = (self.z + self.half) % 2 == 0
        self.z_mid = 1 + self.half
        self.z_end = 3 * self.half
        self.z_far_mid = 1 + self.far
        self.z_far_end = 3 * self.far
        self.z_near = self.z_mid + self.z_end - self.z

    def at(self, z, c):
        return (self.g, 2 * z + c)


def greet(chain, ranks, groups, meanwhile=None):
    barrier = pltpu.get_barrier_semaphore()
    for step in range(1, ranks):
        pl.semaphore_signal(
            barrier, inc=1, device_id=(chain.g, (chain.me + step) % ranks), device_id_type=MESH
        )
    for step in range(1, groups):
        pl.semaphore_signal(
            barrier, inc=1, device_id=((chain.g + step) % groups, chain.me), device_id_type=MESH
        )
    if meanwhile is not None:
        meanwhile()
    pl.semaphore_wait(barrier, ranks + groups - 2)


def neighbours(g):
    along_x = g + 1 - 2 * (g % 2)
    along_y = (g + 2) % 4
    return along_x, along_y


def send(src, dst, send_sem, recv_sem, device):
    return pltpu.make_async_remote_copy(
        src_ref=src, dst_ref=dst, send_sem=send_sem, recv_sem=recv_sem,
        device_id=device, device_id_type=MESH,
    )


def forward_kernel(
    cap,
    ids_ref, weight_ref, tokens_ref, grads_ref, wg_ref, wu_ref, wd_ref,
    full_out, rows_out, hidden_hbm, delta_hbm, down_hbm, dots_out, table_out,
    raw, rows, stage_d, stage_e, full_gate, full_up, full_down, gate_val, up_val, hg_val, select,
    down_part, down_relay, down_in, hidden_out, delta_out, down_out,
    load_sem, raw_ss, raw_rs, e_ss, e_rs, d_ss, d_rs, tab_ss, tab_rs,
    w_ls, wa_ss, wa_rs, wf_ss, wf_rs, out_sem, relay_ss, relay_rs, pair_ss, pair_rs,
):
    chain = Chain()
    g, me, c, z = chain.g, chain.me, chain.c, chain.z
    is_mid, is_end = chain.is_mid, chain.is_end
    groups = lax.axis_size("dp")
    ranks = lax.axis_size("expert")
    steps = 2 * groups
    width = raw.shape[-1]
    count = raw.shape[2]
    slot_rows = rows.shape[2]
    along_x, along_y = neighbours(g)
    fulls = (full_gate, full_up, full_down)
    shards = (wg_ref, wu_ref, wd_ref)

    sub = width // groups

    def load_x(k):
        return pltpu.make_async_copy(
            tokens_ref.at[:, pl.ds(k * width, width)], raw.at[0, k], load_sem.at[k]
        )

    def load_rest():
        for k in range(ahead, groups):
            load_x(k).start()
        for i in range(groups):
            for owner in range(groups):
                pltpu.make_async_copy(
                    grads_ref.at[:, pl.ds(owner * width + i * sub, sub)],
                    raw.at[0, groups + i, :, pl.ds(owner * sub, sub)], load_sem.at[groups + i],
                ).start()
        for w in range(3):
            pltpu.make_async_copy(shards[w].at[0], fulls[w].at[g], w_ls.at[w]).start()

    ahead = 3
    for k in range(ahead):
        load_x(k).start()

    def shard_to(w, way):
        device = (along_x, me) if way == 0 else (along_y, me)
        return send(shards[w].at[0], fulls[w].at[g], wa_ss.at[w, way], wa_rs.at[w, way], device)

    def forward_half(w, way):
        owner = along_y if way == 0 else along_x
        device = (along_x, me) if way == 0 else (along_y, me)
        half = fulls[w].shape[1] // 2
        piece = fulls[w].at[owner, pl.ds(way * half, half)]
        return send(piece, piece, wf_ss.at[w, way], wf_rs.at[w, way], device)

    def build_table():
        experts = lax.broadcasted_iota(jnp.int32, (ranks, count), 0)
        named = [experts == ids_ref[k : k + 1, :] for k in range(ids_ref.shape[0])]
        hits = functools.reduce(jnp.logical_or, named)
        before = lax.broadcasted_iota(jnp.int32, (count, count), 0) < lax.broadcasted_iota(
            jnp.int32, (count, count), 1
        )
        order = dot(hits.astype(F32).astype(BF16), before.astype(F32).astype(BF16))
        table_out[0, 0:ranks, :] = jnp.where(hits, order, -1.0)
        weight = jnp.zeros((ranks, count), F32)
        for k in range(ids_ref.shape[0]):
            weight = jnp.where(named[k], weight_ref[k : k + 1, :].astype(F32), weight)
        table_out[0, ranks : 2 * ranks, :] = weight

        rows[:, :, cap:, :] = jnp.zeros((steps, ranks, slot_rows - cap, width), BF16)

    def table_send(slot, sem, zz):
        return send(
            table_out.at[0], table_out.at[slot], tab_ss.at[sem], tab_rs.at[slot - 1], chain.at(zz, c)
        )

    targets = (me, me + 1 - 2 * c, 2 * chain.z_near, 2 * chain.z_near + 1)

    def selectors(j):
        slots = lax.broadcasted_iota(jnp.int32, (slot_rows, count), 0).astype(F32)
        for i, rank in enumerate(targets):
            hit = table_out[j, pl.ds(rank, 1), :] == slots
            block = pl.ds(i * slot_rows, slot_rows)
            select[0, j, block, :] = jnp.where(hit, 1.0, 0.0).astype(BF16)
            select[1, j, block, :] = jnp.where(
                hit, table_out[j, pl.ds(ranks + rank, 1), :], 0.0
            ).astype(BF16)

    def gather(j, k, z_from, blocks, e_slot):
        picked = dot(select[k // groups, j, 0 : blocks * slot_rows, :], raw[j, k]).astype(BF16)
        parts = [picked[i * slot_rows : (i + 1) * slot_rows] for i in range(blocks)]
        rows[k, 4 * c + z_from] = parts[0]
        stage_d[k, z_from] = parts[1]
        for i in range(2, blocks):
            stage_e[k, i - 2, e_slot] = parts[i]

    full = pl.ds(0, cap)
    far_places = ((chain.z_far_mid, 1), (chain.z_far_end, 2))

    def own_raw(k):
        return send(raw.at[0, k], raw.at[2, k], raw_ss.at[0, k], raw_rs.at[1, k], chain.at(chain.z_far_mid, c))

    def end_raw(k):
        return send(raw.at[0, k], raw.at[1, k], raw_ss.at[0, k], raw_rs.at[0, k], chain.at(chain.z_mid, c))

    def onward_raw(k):
        return send(raw.at[1, k], raw.at[3, k], raw_ss.at[1, k], raw_rs.at[2, k], chain.at(chain.z_far_mid, c))

    def own_to_end(k, i):
        return send(
            stage_e.at[k, i, 0, full], rows.at[k, 4 * c + z, full],
            e_ss.at[k, 0, i], e_rs.at[k, 0, c], chain.at(chain.z_end, i),
        )

    def far_to_end(k, i, which):
        z_from, slot = far_places[which]
        return send(
            stage_e.at[k, i, slot, full], rows.at[k, 4 * c + z_from, full],
            e_ss.at[k, 1 + which, i], e_rs.at[k, 1 + which, c], chain.at(chain.z_end, i),
        )

    def mid_to_partner(k):
        return send(
            stage_d.at[k, :, full], rows.at[k, pl.ds(4 * c, 4), full], d_ss.at[k], d_rs.at[k], chain.at(z, 1 - c)
        )

    def end_to_partner(k):
        return send(
            stage_d.at[k, z, full], rows.at[k, 4 * c + z, full], d_ss.at[k], d_rs.at[k], chain.at(z, 1 - c)
        )

    def own_block_from(k, core):
        return send(
            stage_e.at[k, 0, 0, full], rows.at[k, 4 * core + chain.z_mid, full],
            e_ss.at[k, 0, 0], e_rs.at[k, 0, core], chain.at(chain.z_mid, core),
        )

    def far_block_from(k, core, which):
        return send(
            stage_e.at[k, 0, 1, full], rows.at[k, 4 * core + far_places[which][0], full],
            e_ss.at[k, 1 + which, 0], e_rs.at[k, 1 + which, core], chain.at(chain.z_mid, core),
        )

    def landed_near(k):
        @pl.when(is_mid)
        def _():
            mid_to_partner(k).wait_recv()

        @pl.when(is_end)
        def _():
            end_to_partner(k).wait_recv()
            for core in range(2):
                own_block_from(k, core).wait_recv()

    def landed_far(k):
        @pl.when(is_end)
        def _():
            for core in range(2):
                for which in range(2):
                    far_block_from(k, core, which).wait_recv()

    def landed(k):
        landed_near(k)
        landed_far(k)

    def load_wait(k):
        pltpu.make_async_copy(
            tokens_ref.at[:, pl.ds(0, width)], raw.at[0, k], load_sem.at[k]
        ).wait()

    across = groups - 1 - g
    slots = ranks * slot_rows
    half_inner = hidden_out.shape[2] // 2

    def hidden_grad(q, carry):
        def tile(t, carry):
            four = pl.ds(4 * t, 4)
            value = functools.reduce(jnp.add, [
                dot(
                    rows[groups + q, four, :, owner * sub : (owner + 1) * sub].reshape(4 * slot_rows, sub),
                    full_down[owner, :, pl.ds(pl.multiple_of(q * sub, 128), sub)], 1, 1,
                )
                for owner in range(groups)
            ]).reshape(4, slot_rows, hg_val.shape[2])

            @pl.when(q == 0)
            def _():
                hg_val[four] = value

            @pl.when(q > 0)
            def _():
                hg_val[four] += value

            return carry

        return lax.fori_loop(0, ranks // 4, tile, carry)

    hidden_copy = pltpu.make_async_copy(hidden_out, hidden_hbm, out_sem.at[4])

    def block_of(tile):
        return pl.ds(tile * half_inner, half_inner)

    def of_owner(owner):
        return pl.ds(pl.multiple_of(owner * sub, 128), sub)

    def relay_to(i, way):
        device = (along_x, me) if way == 0 else (along_y, me)
        return send(
            down_part.at[i, block_of(way), of_owner(across)], down_relay.at[i, way],
            relay_ss.at[i, way], relay_rs.at[i, way], device,
        )

    def pair_to(i, way):
        owner = along_x if way == 0 else along_y
        return send(
            down_part.at[i, :, of_owner(owner)], down_in.at[i, way],
            pair_ss.at[i, way], pair_rs.at[i, way], (owner, me),
        )

    def down_make(i):
        for tile in range(2):
            left = hidden_out[:, :, tile * half_inner : (tile + 1) * half_inner].reshape(slots, half_inner)
            down_part[i, block_of(tile), :] = dot(
                left, rows[groups + i].reshape(slots, width), 0, 0
            ).astype(BF16)
        for way in range(2):
            relay_to(i, way).start()

    def down_pass(i):
        for way in range(2):
            owner = along_x if way == 0 else along_y
            relay_to(i, 1 - way).wait_recv()
            place = (i, block_of(1 - way), of_owner(owner))
            down_part[place] = (
                down_part[place].astype(F32) + down_relay[i, 1 - way].astype(F32)
            ).astype(BF16)
            pair_to(i, way).start()

    def down_own(i):
        for way in range(2):
            pair_to(i, way).wait_recv()
        total = down_part[i, :, of_owner(g)].astype(F32)
        for way in range(2):
            total = total + down_in[i, way].astype(F32)
        down_out[:, of_owner(i)] = total.astype(BF16)

    def prologue():
        build_table()
        selectors(0)
        for k in range(ahead):
            load_wait(k)

            @pl.when(is_mid)
            def _():
                gather(0, k, z, 4, 0)

    greet(chain, ranks, groups, prologue)
    for way in range(2):
        shard_to(0, way).start()

    @pl.when(is_mid)
    def _():
        own_raw(0).start()
        for k in range(ahead):
            own_to_end(k, 0).start()
            own_to_end(k, 1).start()

    @pl.when(is_end)
    def _():
        end_raw(0).start()
        table_send(1, 0, chain.z_mid).start()
        table_send(3, 1, chain.z_far_mid).start()

    @pl.when(is_mid)
    def _():
        table_send(2, 0, chain.z_far_mid).start()

    load_rest()
    for w in range(1, 3):
        for way in range(2):
            shard_to(w, way).start()
    for k in range(ahead, steps):
        load_wait(k)

    @pl.when(is_end)
    def _():
        for k in range(1, steps):
            end_raw(k).start()

    def step(k, carry):
        @pl.when(is_mid & (k < steps))
        def _():
            @pl.when(k > 0)
            def _():
                own_raw(k).start()

            @pl.when(k == 0)
            def _():
                table_send(1, 0, chain.z_mid).wait_recv()
                selectors(1)

            end_raw(k).wait_recv()
            onward_raw(k).start()

            @pl.when(k + ahead < steps)
            def _():
                gather(0, k + ahead, z, 4, 0)
                own_to_end(k + ahead, 0).start()
                own_to_end(k + ahead, 1).start()

            gather(1, k, chain.z_end, 2, 0)

        @pl.when(is_end & (k < steps))
        def _():
            gather(0, k, z, 2, 0)
            end_to_partner(k).start()

        for w in range(3):
            @pl.when(k == w + 2)
            def _():
                for way in range(2):
                    shard_to(w, 1 - way).wait_recv()
                    forward_half(w, way).start()

        @pl.when(k == groups + 1)
        def _():
            for kk in range(groups):
                landed(kk)
            for w in range(2):
                pltpu.make_async_copy(shards[w].at[0], fulls[w].at[g], w_ls.at[w]).wait()
                for way in range(2):
                    forward_half(w, way).wait_recv()

        @pl.when((k == groups + 1) | (k == groups + 2))
        def _():
            def forward(p, carry):
                pair = pl.ds(2 * p, 2)
                shape = (2, slot_rows, gate_val.shape[2])
                piece = [rows[kk, pair].reshape(2 * slot_rows, width) for kk in range(groups)]
                gate = functools.reduce(jnp.add, [dot(piece[kk], full_gate[kk]) for kk in range(groups)])
                up = functools.reduce(jnp.add, [dot(piece[kk], full_up[kk]) for kk in range(groups)])
                gate_val[pair] = gate.reshape(shape)
                up_val[pair] = up.reshape(shape)
                hidden_out[pair] = (gate * jax.nn.sigmoid(gate) * up).astype(BF16).reshape(shape)
                return carry

            start = (k - groups - 1) * (ranks // 4)
            lax.fori_loop(start, start + ranks // 4, forward, 0)

        @pl.when(k == groups + 2)
        def _():
            pltpu.make_async_copy(shards[2].at[0], fulls[2].at[g], w_ls.at[2]).wait()
            for way in range(2):
                forward_half(2, way).wait_recv()

        @pl.when(k >= groups + 2)
        def _():
            q = k - groups - 2

            @pl.when(q >= 1)
            def _():
                down_pass(q - 1)

            landed(groups + q)
            down_make(q)
            hidden_grad(q, 0)

            @pl.when(q == 0)
            def _():
                hidden_copy.start()

        @pl.when(is_mid & (k >= 1))
        def _():
            @pl.when(k == 1)
            def _():
                table_send(2, 0, chain.z_far_mid).wait_recv()
                table_send(3, 0, chain.z_far_mid).wait_recv()
                selectors(2)
                selectors(3)

            j = k - 1
            own_raw(j).wait_recv()
            gather(2, j, chain.z_far_mid, 4, 1)
            far_to_end(j, 0, 0).start()
            far_to_end(j, 1, 0).start()
            onward_raw(j).wait_recv()
            gather(3, j, chain.z_far_end, 4, 2)
            far_to_end(j, 0, 1).start()
            far_to_end(j, 1, 1).start()
            mid_to_partner(j).start()

        return carry

    lax.fori_loop(0, steps + 1, step, 0)

    outs = [
        pltpu.make_async_copy(full_gate, full_out.at[0], out_sem.at[0]),
        pltpu.make_async_copy(full_up, full_out.at[1], out_sem.at[1]),
    ]
    for copy in outs:
        copy.start()
    first = pltpu.make_async_copy(rows.at[pl.ds(0, groups)], rows_out.at[pl.ds(0, groups)], out_sem.at[2])
    first.start()

    down_pass(groups - 2)

    def deltas(t, carry):
        gate, up, grad = gate_val[t], up_val[t], hg_val[t]
        sig = jax.nn.sigmoid(gate)
        delta_out[0, t] = (grad * up * sig * (1.0 + gate * (1.0 - sig))).astype(BF16)
        delta_out[1, t] = (grad * (gate * sig)).astype(BF16)
        total = jnp.sum(hidden_out[t].astype(F32) * grad, axis=1, keepdims=True)
        dots_out[t] = jnp.broadcast_to(total, (total.shape[0], total.shape[0])).T[0:8, :]
        return carry

    late = pltpu.make_async_copy(rows.at[steps - 1], rows_out.at[groups], out_sem.at[3])

    def delta_copy(side, core, half):
        pair = pl.ds(4 * core + 2 * half, 2)
        return pltpu.make_async_copy(
            delta_out.at[:, pair], delta_hbm.at[:, pair], out_sem.at[6 + 2 * side + core]
        )

    for side, half in enumerate((chain.half, chain.far)):
        if side == 0:
            landed_near(steps - 1)
        else:
            landed_far(steps - 1)
            late.start()

        def last_rows(core, carry):
            pair = pl.ds(4 * core + 2 * half, 2)
            value = functools.reduce(jnp.add, [
                dot(
                    rows[steps - 1, pair, :, owner * sub : (owner + 1) * sub].reshape(2 * slot_rows, sub),
                    full_down[owner, :, (groups - 1) * sub : groups * sub], 1, 1,
                )
                for owner in range(groups)
            ])
            hg_val[pair] += value.reshape(2, slot_rows, hg_val.shape[2])
            for block in range(2):
                deltas(4 * core + 2 * half + block, 0)
            delta_copy(side, core, half).start()
            return carry

        lax.fori_loop(0, 2, last_rows, 0)

    for copy in outs:
        copy.wait()
    first.wait()
    late.wait()

    def finish_down(i, carry):
        down_own(i)
        for way in range(2):
            relay_to(i, way).wait_send()
            pair_to(i, way).wait_send()
        return carry

    lax.fori_loop(0, groups - 1, finish_down, 0)
    down_copy = pltpu.make_async_copy(down_out, down_hbm, out_sem.at[5])
    down_copy.start()
    for w in range(3):
        for way in range(2):
            shard_to(w, way).wait_send()
            forward_half(w, way).wait_send()

    def drain(k, carry):
        @pl.when(is_mid)
        def _():
            own_raw(k).wait_send()
            onward_raw(k).wait_send()
            for i in range(2):
                own_to_end(k, i).wait_send()
                for which in range(2):
                    far_to_end(k, i, which).wait_send()
            mid_to_partner(k).wait_send()

        @pl.when(is_end)
        def _():
            end_raw(k).wait_send()
            end_to_partner(k).wait_send()

        return carry

    lax.fori_loop(0, steps, drain, 0)

    @pl.when(is_mid)
    def _():
        table_send(2, 0, chain.z_far_mid).wait_send()

    @pl.when(is_end)
    def _():
        table_send(1, 0, chain.z_mid).wait_send()
        table_send(3, 1, chain.z_far_mid).wait_send()

    hidden_copy.wait()
    down_copy.wait()
    for side, half in enumerate((chain.half, chain.far)):
        for core in range(2):
            delta_copy(side, core, half).wait()


def forward_call(ids_t, weight_t, tokens, out_grad, w_gate, w_up, w_down, cap):
    count, depth = tokens.shape
    groups, ranks = lax.axis_size("dp"), lax.axis_size("expert")
    inner = w_gate.shape[2]
    width = depth // groups
    slot_rows = -(-cap // 16) * 16
    steps = 2 * groups
    hbm = pl.BlockSpec(memory_space=pl.ANY)
    vmem = pl.BlockSpec(memory_space=pltpu.VMEM)
    dma = pltpu.SemaphoreType.DMA
    return pl.pallas_call(
        functools.partial(forward_kernel, cap),
        out_shape=(
            jax.ShapeDtypeStruct((2, groups, width, inner), BF16),
            jax.ShapeDtypeStruct((groups + 1, ranks, slot_rows, width), BF16),
            jax.ShapeDtypeStruct((ranks, slot_rows, inner), BF16),
            jax.ShapeDtypeStruct((2, ranks, slot_rows, inner), BF16),
            jax.ShapeDtypeStruct((inner, width), BF16),
            jax.ShapeDtypeStruct((ranks, 8, slot_rows), F32),
            jax.ShapeDtypeStruct((4, 2 * ranks, count), F32),
        ),
        in_specs=[vmem, vmem, hbm, hbm, hbm, hbm, hbm],
        out_specs=(hbm,) * 5 + (vmem,) * 2,
        scratch_shapes=[
            pltpu.VMEM((4, steps, count, width), BF16),
            pltpu.VMEM((steps, ranks, slot_rows, width), BF16),
            pltpu.VMEM((steps, 4, slot_rows, width), BF16),
            pltpu.VMEM((steps, 2, 3, slot_rows, width), BF16),
            pltpu.VMEM((groups, width, inner), BF16),
            pltpu.VMEM((groups, width, inner), BF16),
            pltpu.VMEM((groups, inner, width), BF16),
            pltpu.VMEM((ranks, slot_rows, inner), F32),
            pltpu.VMEM((ranks, slot_rows, inner), F32),
            pltpu.VMEM((ranks, slot_rows, inner), F32),
            pltpu.VMEM((2, 4, 4 * slot_rows, count), BF16),
            pltpu.VMEM((groups - 1, inner, width), BF16),
            pltpu.VMEM((groups - 1, 2, inner // 2, width // groups), BF16),
            pltpu.VMEM((groups - 1, 2, inner, width // groups), BF16),
            pltpu.VMEM((ranks, slot_rows, inner), BF16),
            pltpu.VMEM((2, ranks, slot_rows, inner), BF16),
            pltpu.VMEM((inner, width), BF16),
            dma((steps,)), dma((2, steps)), dma((3, steps)), dma((steps, 3, 2)), dma((steps, 3, 2)),
            dma((steps,)), dma((steps,)), dma((2,)), dma((3,)),
            dma((3,)), dma((3, 2)), dma((3, 2)), dma((3, 2)), dma((3, 2)), dma((10,)),
            dma((groups - 1, 2)), dma((groups - 1, 2)), dma((groups - 1, 2)), dma((groups - 1, 2)),
        ],
        compiler_params=pltpu.CompilerParams(
            collective_id=0, has_side_effects=True, vmem_limit_bytes=67000000
        ),
    )(ids_t, weight_t, tokens, out_grad, w_gate, w_up, w_down)


def backward_kernel(
    cap,
    ids_ref, weight_ref, table_ref, dots_ref, full_ref, rows_ref, hidden_ref, delta_ref, down_ref,
    token_out, route_out, gate_out, up_out, down_out,
    full, rows, hidden, delta, grads, comb, gf_send, gf_in, end_send, select,
    diag_gu, pair_gu, pair_d, relay_gu, relay_d, in_gu, in_d, dots_in,
    load_sem, d_ss, d_rs, far_ss, far_rs, near_ss, near_rs, gf_ss, gf_rs, es_ss, es_rs,
    dots_ss, dots_rs, relay_ss, relay_rs, pair_ss, pair_rs,
):
    chain = Chain()
    g, me, c, z = chain.g, chain.me, chain.c, chain.z
    is_mid, is_end = chain.is_mid, chain.is_end
    groups = lax.axis_size("dp")
    ranks = lax.axis_size("expert")
    _, slot_rows, width = rows.shape[1:]
    count = table_ref.shape[2]
    inner = hidden.shape[2]
    along_x, along_y = neighbours(g)
    across = groups - 1 - g
    slots = ranks * slot_rows
    subs, narrow = grads.shape[0], grads.shape[3]

    loads = [
        pltpu.make_async_copy(delta_ref, delta, load_sem.at[0]),
        pltpu.make_async_copy(full_ref.at[:, 0], full.at[:, 0], load_sem.at[1]),
        pltpu.make_async_copy(rows_ref.at[across], rows.at[across], load_sem.at[2]),
        pltpu.make_async_copy(full_ref.at[:, pl.ds(1, subs - 1)], full.at[:, pl.ds(1, subs - 1)], load_sem.at[3]),
        pltpu.make_async_copy(rows_ref.at[groups], rows.at[groups], load_sem.at[4]),
        pltpu.make_async_copy(hidden_ref, hidden, load_sem.at[5]),
    ]
    for i, shard in enumerate((along_x, along_y, g)):
        loads.append(pltpu.make_async_copy(rows_ref.at[shard], rows.at[shard], load_sem.at[6 + i]))
    for copy in loads:
        copy.start()
    sub = width // groups
    half_inner = inner // 2
    down_ready = pltpu.make_async_copy(down_ref, down_out, load_sem.at[9])
    down_ready.start()

    def of_owner(owner):
        return pl.ds(pl.multiple_of(owner * sub, 128), sub)

    greet(chain, ranks, groups)

    real = pl.ds(0, cap)

    def dots_to(peer):
        return send(
            dots_ref.at[4 * (peer % 2) + peer // 2], dots_in.at[me],
            dots_ss.at[peer], dots_rs.at[me], (g, peer),
        )

    def dots_from(peer):
        return send(
            dots_ref.at[4 * c + z], dots_in.at[peer], dots_ss.at[peer], dots_rs.at[peer], (g, peer)
        )

    for step in range(1, ranks):
        dots_to((me + step) % ranks).start()

    comb[:, :, :, cap:, :] = jnp.zeros((subs, 4, 4, slot_rows - cap, narrow), BF16)
    targets = (me, me + 1 - 2 * c, 2 * chain.z_near, 2 * chain.z_near + 1)

    def selectors(j, z_from):
        slot = lax.broadcasted_iota(jnp.int32, (slot_rows, count), 0).astype(F32)
        for i, rank in enumerate(targets):
            hit = table_ref[j, pl.ds(rank, 1), :] == slot
            select[z_from, i * slot_rows : (i + 1) * slot_rows, :] = jnp.where(hit, 1.0, 0.0).astype(BF16)

    selectors(0, z)

    @pl.when(is_mid)
    def _():
        selectors(1, chain.z_end)
        selectors(2, chain.z_far_mid)
        selectors(3, chain.z_far_end)

    def to_partner(k):
        return send(
            grads.at[k, pl.ds(4 * (1 - c), 4), real], comb.at[k, :, 1, real],
            d_ss.at[k], d_rs.at[k], chain.at(z, 1 - c),
        )

    def end_to_partner(k):
        return send(
            grads.at[k, 4 * (1 - c) + z, real], comb.at[k, z, 1, real],
            d_ss.at[k], d_rs.at[k], chain.at(z, 1 - c),
        )

    def far_home(k, core):
        return send(
            grads.at[k, pl.ds(4 * core + 2 * chain.far, 2), real],
            comb.at[k, pl.ds(2 * chain.far, 2), 2 + c, real],
            far_ss.at[k, core], far_rs.at[k, c], chain.at(chain.z_mid, core),
        )

    def far_from(k, core):
        return send(
            grads.at[k, pl.ds(4 * core + 2 * chain.far, 2), real],
            comb.at[k, pl.ds(2 * chain.far, 2), 2 + core, real],
            far_ss.at[k, core], far_rs.at[k, core], chain.at(chain.z_end, core),
        )

    def near_home(k, core):
        return send(
            grads.at[k, 4 * core + chain.z_mid, real], comb.at[k, chain.z_mid, 2 + c, real],
            near_ss.at[k, core], near_rs.at[k, c], chain.at(chain.z_mid, core),
        )

    def near_from(k, core):
        return send(
            grads.at[k, 4 * core + chain.z_mid, real], comb.at[k, chain.z_mid, 2 + core, real],
            near_ss.at[k, core], near_rs.at[k, core], chain.at(chain.z_end, core),
        )

    def sums_across(k, home):
        return send(
            gf_send.at[k, home], gf_in.at[k, home], gf_ss.at[k, home], gf_rs.at[k, home], chain.at(chain.z_far_mid, c)
        )

    def sums_to_end(k):
        return send(end_send.at[k], gf_in.at[k, 0], es_ss.at[k], es_rs.at[k], chain.at(chain.z_end, c))

    def device_on(way):
        return ((along_x if way == 0 else along_y), me)

    def relay_to(w, way):
        if w == 2:
            src, dst = pair_d.at[pl.ds(way * half_inner, half_inner), of_owner(across)], relay_d.at[way]
        else:
            half = width // 2
            src, dst = diag_gu.at[w, pl.ds(way * half, half)], relay_gu.at[w, way]
        return send(src, dst, relay_ss.at[w, way], relay_rs.at[w, way], device_on(way))

    def pair_to(w, way):
        if w == 2:
            src, dst = pair_d.at[:, of_owner(along_x if way == 0 else along_y)], in_d.at[way]
        else:
            src, dst = pair_gu.at[w, way], in_gu.at[w, way]
        return send(src, dst, pair_ss.at[w, way], pair_rs.at[w, way], device_on(way))

    def part(w, shard, tile):
        half = width // 2
        left = rows[shard, :, :, tile * half : (tile + 1) * half].reshape(slots, half)
        return dot(left, delta[w].reshape(slots, inner), 0, 0)

    def diagonal(w):
        if w == 2:
            for tile in range(2):
                left = hidden[:, :, tile * half_inner : (tile + 1) * half_inner].reshape(slots, half_inner)
                pair_d[pl.ds(tile * half_inner, half_inner), :] = dot(
                    left, rows[groups].reshape(slots, width), 0, 0
                ).astype(BF16)
        else:
            half = width // 2
            for tile in range(2):
                diag_gu[w, pl.ds(tile * half, half), :] = part(w, across, tile).astype(BF16)
        for way in range(2):
            relay_to(w, way).start()

    def pairs(w):
        for way in range(2):
            shard = along_x if way == 0 else along_y
            relay_to(w, 1 - way).wait_recv()
            if w == 2:
                place = (pl.ds((1 - way) * half_inner, half_inner), of_owner(shard))
                pair_d[place] = (pair_d[place].astype(F32) + relay_d[1 - way].astype(F32)).astype(BF16)
            else:
                half = width // 2
                for tile in range(2):
                    value = part(w, shard, tile).astype(BF16)
                    if tile == 1 - way:
                        value = (value.astype(F32) + relay_gu[w, 1 - way].astype(F32)).astype(BF16)
                    pair_gu[w, way, pl.ds(tile * half, half), :] = value
            pair_to(w, way).start()

    def finish(w):
        for way in range(2):
            pair_to(w, way).wait_recv()
        if w == 2:
            total = pair_d[:, of_owner(g)].astype(F32)
            for way in range(2):
                total = total + in_d[way].astype(F32)
            down_ready.wait()
            down_out[:, of_owner(groups - 1)] = total.astype(BF16)
        else:
            half = width // 2
            for tile in range(2):
                value = part(w, g, tile)
                block = pl.ds(tile * half, half)
                for way in range(2):
                    value = value + in_gu[w, way, block, :].astype(F32)
                (gate_out, up_out)[w][block, :] = value.astype(BF16)

    def input_grad(k):
        for hc in range(2):
            left = [delta[w, pl.ds(4 * hc, 4)].reshape(4 * slot_rows, inner) for w in range(2)]
            value = (dot(left[0], full[0, k], 1, 1) + dot(left[1], full[1, k], 1, 1)).astype(BF16)
            value = value.reshape(4, slot_rows, narrow)
            grads[k, pl.ds(4 * hc, 4)] = value

            @pl.when(is_end)
            def _():
                far_home(k, hc).start()

            @pl.when(c == hc)
            def _():
                comb[k, :, 0] = value

    def summed(k, z_from, blocks):
        return dot(
            select[z_from, 0 : blocks * slot_rows, :],
            comb[k, z_from, 0:blocks].reshape(blocks * slot_rows, narrow), 0, 0,
        )

    for i in range(2):
        loads[i].wait()

    lag = 2

    def along(k, carry):
        @pl.when(k == 1)
        def _():
            loads[3].wait()

        @pl.when(k < subs)
        def _():
            input_grad(k)

            @pl.when(is_mid)
            def _():
                to_partner(k).start()

            @pl.when(is_end)
            def _():
                end_to_partner(k).start()

        @pl.when(is_end & (k == subs - 1))
        def _():
            for j in range(subs):
                for core in range(2):
                    near_home(j, core).start()

        for w in range(2):
            @pl.when(k == w)
            def _():
                if w == 0:
                    loads[2].wait()
                diagonal(w)

        @pl.when(k == 2)
        def _():
            loads[4].wait()
            loads[5].wait()

            diagonal(2)

        @pl.when(is_mid & (k >= 1) & (k <= subs))
        def _():
            j = k - 1
            to_partner(j).wait_recv()
            for core in range(2):
                far_from(j, core).wait_recv()
            gf_send[j, 1] = summed(j, chain.z_far_end, 4).astype(BF16)
            sums_across(j, 1).start()
            gf_send[j, 0] = summed(j, chain.z_far_mid, 4).astype(BF16)
            sums_across(j, 0).start()

        @pl.when(k == 3)
        def _():
            for copy in loads[6:]:
                copy.wait()

        for at, w in ((3, 0), (4, 2), (5, 1)):
            @pl.when(k == at)
            def _():
                pairs(w)

        @pl.when(is_mid & (k > lag))
        def _():
            j = k - 1 - lag
            sums_across(j, 1).wait_recv()
            end_send[j] = (summed(j, chain.z_end, 2) + gf_in[j, 1].astype(F32)).astype(BF16)
            sums_to_end(j).start()

        return carry

    lax.fori_loop(0, subs + 1 + lag, along, 0)

    for step in range(1, ranks):
        dots_from((me + step) % ranks).wait_recv()
    dots_in[me] = dots_ref[4 * c + z]
    found = jnp.zeros(ids_ref.shape, F32)
    slot = lax.broadcasted_iota(jnp.int32, (slot_rows, count), 0).astype(F32)
    for rank in range(ranks):
        hit = jnp.where(table_ref[0, rank : rank + 1, :] == slot, 1.0, 0.0)
        value = lax.dot_general(
            dots_in[rank], hit, (((1,), (0,)), ((), ())),
            precision=lax.Precision.HIGHEST, preferred_element_type=F32,
        )[0:1, :]
        found = jnp.where(ids_ref[...] == rank, value, found)
    route_out[...] = (found / weight_ref[...].astype(F32)).astype(BF16)

    def third(k, carry):
        columns = pl.ds(pl.multiple_of(k * narrow, 128), narrow)

        @pl.when(k == 0)
        def _():
            finish(0)

        @pl.when(k == 3)
        def _():
            finish(2)

        @pl.when(is_mid)
        def _():
            sums_across(k, 0).wait_recv()
            for core in range(2):
                near_from(k, core).wait_recv()
            token_out[:, columns] = (summed(k, z, 4) + gf_in[k, 0].astype(F32)).astype(BF16)

        @pl.when(is_end)
        def _():
            end_to_partner(k).wait_recv()
            sums_to_end(k).wait_recv()
            token_out[:, columns] = (summed(k, z, 2) + gf_in[k, 0].astype(F32)).astype(BF16)

        return carry

    lax.fori_loop(0, subs, third, 0)

    finish(1)
    for w in range(3):
        for way in range(2):
            relay_to(w, way).wait_send()
            pair_to(w, way).wait_send()
    for step in range(1, ranks):
        dots_to((me + step) % ranks).wait_send()

    def drain(k, carry):
        @pl.when(is_mid)
        def _():
            to_partner(k).wait_send()
            for home in range(2):
                sums_across(k, home).wait_send()
            sums_to_end(k).wait_send()

        @pl.when(is_end)
        def _():
            for core in range(2):
                far_home(k, core).wait_send()
                near_home(k, core).wait_send()
            end_to_partner(k).wait_send()

        return carry

    lax.fori_loop(0, subs, drain, 0)


def backward_call(ids_t, weight_t, table, dots, full, rows, hidden, delta, down, cap):
    groups, ranks = lax.axis_size("dp"), lax.axis_size("expert")
    _, _, slot_rows, width = rows.shape
    count = table.shape[2]
    inner = hidden.shape[2]
    subs, narrow = 2 * groups, width // 2
    full = full.reshape(2, subs, narrow, inner)
    hbm = pl.BlockSpec(memory_space=pl.ANY)
    vmem = pl.BlockSpec(memory_space=pltpu.VMEM)
    dma = pltpu.SemaphoreType.DMA
    return pl.pallas_call(
        functools.partial(backward_kernel, cap),
        out_shape=(
            pltpu.VMEM((count, groups * width), BF16),
            pltpu.VMEM(ids_t.shape, BF16),
            pltpu.VMEM((width, inner), BF16),
            pltpu.VMEM((width, inner), BF16),
            pltpu.VMEM((inner, width), BF16),
        ),
        in_specs=[vmem, vmem, vmem, vmem, hbm, hbm, hbm, hbm, hbm],
        out_specs=(vmem,) * 5,
        scratch_shapes=[
            pltpu.VMEM(full.shape, BF16),
            pltpu.VMEM(rows.shape, BF16),
            pltpu.VMEM(hidden.shape, BF16),
            pltpu.VMEM(delta.shape, BF16),
            pltpu.VMEM((subs, ranks, slot_rows, narrow), BF16),
            pltpu.VMEM((subs, 4, 4, slot_rows, narrow), BF16),
            pltpu.VMEM((subs, 2, count, narrow), BF16),
            pltpu.VMEM((subs, 2, count, narrow), BF16),
            pltpu.VMEM((subs, count, narrow), BF16),
            pltpu.VMEM((4, 4 * slot_rows, count), BF16),
            pltpu.VMEM((2, width, inner), BF16),
            pltpu.VMEM((2, 2, width, inner), BF16),
            pltpu.VMEM((inner, width), BF16),
            pltpu.VMEM((2, 2, width // 2, inner), BF16),
            pltpu.VMEM((2, inner // 2, width // groups), BF16),
            pltpu.VMEM((2, 2, width, inner), BF16),
            pltpu.VMEM((2, inner, width // groups), BF16),
            pltpu.VMEM(dots.shape, F32),
            dma((12,)), dma((subs,)), dma((subs,)), dma((subs, 2)), dma((subs, 2)),
            dma((subs, 2)), dma((subs, 2)), dma((subs, 2)), dma((subs, 2)), dma((subs,)), dma((subs,)),
            dma((ranks,)), dma((ranks,)), dma((3, 2)), dma((3, 2)), dma((3, 2)), dma((3, 2)),
        ],
        compiler_params=pltpu.CompilerParams(
            collective_id=1, has_side_effects=True, vmem_limit_bytes=58000000
        ),
    )(ids_t, weight_t, table, dots, full, rows, hidden, delta, down)


def hand_over_kernel(*refs):
    ins, outs, sem = refs[0:5], refs[5:10], refs[10]
    copies = [pltpu.make_async_copy(ins[i], outs[i], sem.at[i]) for i in range(5)]
    for copy in copies:
        copy.start()
    for copy in copies:
        copy.wait()


def hand_over(*arrays):
    return pl.pallas_call(
        hand_over_kernel,
        out_shape=tuple(jax.ShapeDtypeStruct(a.shape, a.dtype) for a in arrays),
        in_specs=[pl.BlockSpec(memory_space=pltpu.VMEM)] * 5,
        out_specs=(pl.BlockSpec(memory_space=pl.ANY),) * 5,
        scratch_shapes=[pltpu.SemaphoreType.DMA((5,))],
        compiler_params=pltpu.CompilerParams(vmem_limit_bytes=8000000),
    )(*arrays)


def swap(block, axis, distance):
    ranks = lax.axis_size(axis)
    return lax.ppermute(block, axis, [(rank, rank ^ distance) for rank in range(ranks)])


def any_mesh(tokens, out_grad, expert_ids, route_weight, w_gate, w_up, w_down):
    tok_count = tokens.shape[0]
    route_count = expert_ids.shape[1]
    ranks = lax.axis_size("expert")
    groups = lax.axis_size("dp")
    me = lax.axis_index("expert")
    group = lax.axis_index("dp")
    capacity = 3 * tok_count * route_count // (2 * ranks)
    routes = tok_count * route_count
    total_slots = ranks * capacity
    full_gate = lax.all_gather(w_gate[0], "dp", axis=0, tiled=True)
    full_up = lax.all_gather(w_up[0], "dp", axis=0, tiled=True)
    full_down = lax.all_gather(w_down[0], "dp", axis=1, tiled=True)
    half = ranks // 2
    flat_ids = expert_ids.reshape(routes)
    one_hot = (flat_ids[:, None] == jnp.arange(ranks, dtype=jnp.int32)[None, :]).astype(jnp.int32)
    slot_order = jnp.sum((jnp.cumsum(one_hot, axis=0) - 1) * one_hot, axis=1)
    slot_order = slot_order.reshape(tok_count, route_count)
    routing = jnp.concatenate(
        [
            expert_ids.astype(jnp.float32),
            slot_order.astype(jnp.float32),
            route_weight.astype(jnp.float32),
        ],
        axis=1,
    )
    far_routing = swap(routing, "expert", half)
    far_ids = far_routing[:, :route_count].astype(jnp.int32)
    far_order = far_routing[:, route_count : 2 * route_count].astype(jnp.int32)
    far_weight = far_routing[:, 2 * route_count :].astype(jnp.bfloat16)
    far_tokens = swap(tokens, "expert", half)
    late_grad, slot_order = lax.optimization_barrier((out_grad, slot_order))
    far_grad = swap(late_grad, "expert", half)
    slots = jnp.arange(total_slots, dtype=jnp.int32)

    def selectors(destination, weight, count):
        picks = jnp.zeros((count, tok_count), jnp.bfloat16)
        weighted = jnp.zeros((count, tok_count), jnp.bfloat16)
        for k in range(route_count):
            hit = slots[:count, None] == destination[:, k][None, :]
            picks = jnp.where(hit, jnp.ones((), jnp.bfloat16), picks)
            weighted = jnp.where(hit, weight[:, k][None, :], weighted)
        return picks, weighted

    destination = (expert_ids ^ me) * capacity + slot_order
    far_destination = (far_ids ^ me) * capacity + far_order
    near_slots = half * capacity
    picks, _ = selectors(destination, route_weight, total_slots)
    near_picks, near_weighted = selectors(destination, route_weight, near_slots)
    far_picks, far_weighted = selectors(far_destination, far_weight, near_slots)

    def blocks(buffer, count=ranks):
        return [buffer[d * capacity : (d + 1) * capacity] for d in range(count)]

    def exchange(buffer, count=ranks):
        return [
            swap(block, "expert", d) if d else block for d, block in enumerate(blocks(buffer, count))
        ]

    rows_in = jnp.concatenate(
        exchange(dot(near_picks, tokens, 1, 0).astype(jnp.bfloat16), half)
        + exchange(dot(far_picks, far_tokens, 1, 0).astype(jnp.bfloat16), half)
    )
    gate_value = dot(rows_in, full_gate, 1, 0)
    up_value = dot(rows_in, full_up, 1, 0)
    sigmoid_gate = jax.nn.sigmoid(gate_value)
    activated = gate_value * sigmoid_gate
    hidden = (activated * up_value).astype(jnp.bfloat16)
    scaled_blocks = exchange(
        dot(near_weighted, late_grad, 1, 0).astype(jnp.bfloat16), half
    ) + exchange(dot(far_weighted, far_grad, 1, 0).astype(jnp.bfloat16), half)
    scaled_blocks, hidden = lax.optimization_barrier((scaled_blocks, hidden))
    scaled = jnp.concatenate(scaled_blocks)
    hidden_grad = dot(scaled, full_down, 1, 1)
    gate_delta = (
        hidden_grad * up_value * sigmoid_gate * (1.0 + gate_value * (1.0 - sigmoid_gate))
    ).astype(jnp.bfloat16)
    up_delta = (hidden_grad * activated).astype(jnp.bfloat16)
    input_grad = (
        dot(gate_delta, full_gate, 1, 1) + dot(up_delta, full_up, 1, 1)
    ).astype(jnp.bfloat16)
    back_blocks = []
    for d, block in enumerate(blocks(input_grad)):
        back_blocks.append(swap(block, "expert", d) if d else block)
    down_part = dot(hidden, scaled, 0, 0).astype(jnp.bfloat16)
    input_grad, rows_in, hidden = lax.optimization_barrier((input_grad, rows_in, hidden))
    expert_out = dot(hidden, full_down, 1, 0)
    weighted_dot = jnp.sum(expert_out * scaled.astype(jnp.float32), axis=1)
    gate_part = dot(rows_in, gate_delta, 0, 0).astype(jnp.bfloat16)
    up_part = dot(rows_in, up_delta, 0, 0).astype(jnp.bfloat16)
    down_grad = lax.psum_scatter(down_part, "dp", scatter_dimension=1, tiled=True)[None]
    gate_grad = lax.psum_scatter(gate_part, "dp", scatter_dimension=0, tiled=True)[None]
    depth = up_part.shape[0] // groups
    up_sum = jnp.zeros((depth, up_part.shape[1]), jnp.float32)
    for d in range(groups):
        piece = lax.dynamic_slice_in_dim(up_part, (group ^ d) * depth, depth, 0)
        up_sum = up_sum + (swap(piece, "dp", d) if d else piece).astype(jnp.float32)
    up_grad = up_sum.astype(jnp.bfloat16)[None]

    token_sum = jnp.zeros(tokens.shape, jnp.float32)
    for pick, block in zip(blocks(picks), back_blocks):
        token_sum = token_sum + dot(pick, block, 0, 0)
    token_grad = token_sum.astype(jnp.bfloat16)

    order = jnp.arange(ranks, dtype=jnp.int32)
    dots = weighted_dot.reshape(ranks, capacity)
    by_rank = jnp.sum(
        jnp.where(((order ^ me)[:, None] == order[None, :])[:, :, None], dots[None], 0.0), axis=1
    )
    back_dots = lax.all_to_all(by_rank, "expert", split_axis=0, concat_axis=0, tiled=True)
    arrival = expert_ids * capacity + slot_order
    hits = arrival.reshape(tok_count, route_count, 1) == slots[None, None, :]
    own_dots = jnp.sum(jnp.where(hits, back_dots.reshape(total_slots)[None, None, :], 0.0), axis=2)
    route_grad = (own_dots / route_weight.astype(jnp.float32)).astype(jnp.bfloat16)
    return (token_grad, route_grad, gate_grad, up_grad, down_grad)


def on_device(tokens, out_grad, expert_ids, route_weight, w_gate, w_up, w_down):
    count = tokens.shape[0]
    cap = 3 * count * expert_ids.shape[1] // (2 * lax.axis_size("expert"))
    ids_t, weight_t = expert_ids.T, route_weight.T
    full, rows, hidden, delta, down, dots, table = forward_call(
        ids_t, weight_t, tokens, out_grad, w_gate, w_up, w_down, cap
    )
    token_grad, route_grad, gate_grad, up_grad, down_grad = backward_call(
        ids_t, weight_t, table, dots, full, rows, hidden, delta, down, cap
    )
    token_grad, gate_grad, up_grad, down_grad, route_grad = hand_over(
        token_grad, gate_grad, up_grad, down_grad, route_grad
    )
    return token_grad, route_grad.T, gate_grad[None], up_grad[None], down_grad[None]


def solution(mesh):
    placed = (
        P(("dp", "expert"), None),
        P(("dp", "expert"), None),
        P(("dp", "expert"), None),
        P(("dp", "expert"), None),
        P("expert", "dp", None),
        P("expert", "dp", None),
        P("expert", None, "dp"),
    )
    chained = mesh.shape["expert"] == 8 and mesh.shape["dp"] == 4
    return jax.shard_map(
        on_device if chained else any_mesh, mesh=mesh, in_specs=placed,
        out_specs=(
            P(("dp", "expert"), None),
            P(("dp", "expert"), None),
            P("expert", "dp", None),
            P("expert", "dp", None),
            P("expert", None, "dp"),
        ),
        check_vma=False,
    )
```

```python
import functools
import jax
import jax.numpy as jnp
from jax import lax
from jax.experimental import pallas as pl
from jax.experimental.pallas import tpu as pltpu
from jax.sharding import PartitionSpec as P


MESH = pl.DeviceIdType.MESH
BF16 = jnp.bfloat16
F32 = jnp.float32


def dot(left, right, over_left=1, over_right=0):
    return lax.dot_general(
        left, right, (((over_left,), (over_right,)), ((), ())), preferred_element_type=F32
    )


class Chain:
    def __init__(self):
        self.g = lax.axis_index("dp")
        self.me = lax.axis_index("expert")
        self.c = self.me % 2
        self.z = self.me // 2
        self.half = self.z // 2
        self.far = 1 - self.half
        self.is_mid = (self.z + self.half) % 2 == 1
        self.is_end = (self.z + self.half) % 2 == 0
        self.z_mid = 1 + self.half
        self.z_end = 3 * self.half
        self.z_far_mid = 1 + self.far
        self.z_far_end = 3 * self.far
        self.z_near = self.z_mid + self.z_end - self.z

    def at(self, z, c):
        return (self.g, 2 * z + c)


def greet(chain, ranks, groups, meanwhile=None):
    barrier = pltpu.get_barrier_semaphore()
    for step in range(1, ranks):
        pl.semaphore_signal(
            barrier, inc=1, device_id=(chain.g, (chain.me + step) % ranks), device_id_type=MESH
        )
    for step in range(1, groups):
        pl.semaphore_signal(
            barrier, inc=1, device_id=((chain.g + step) % groups, chain.me), device_id_type=MESH
        )
    if meanwhile is not None:
        meanwhile()
    pl.semaphore_wait(barrier, ranks + groups - 2)


def neighbours(g):
    along_x = g + 1 - 2 * (g % 2)
    along_y = (g + 2) % 4
    return along_x, along_y


def send(src, dst, send_sem, recv_sem, device):
    return pltpu.make_async_remote_copy(
        src_ref=src, dst_ref=dst, send_sem=send_sem, recv_sem=recv_sem,
        device_id=device, device_id_type=MESH,
    )


def forward_kernel(
    cap,
    ids_ref, weight_ref, tokens_ref, grads_ref, wg_ref, wu_ref, wd_ref,
    full_out, rows_out, hidden_hbm, delta_hbm, down_hbm, dots_out, table_out,
    raw, rows, stage_d, stage_e, full_gate, full_up, full_down, gate_val, up_val, hg_val, select,
    down_part, down_relay, down_in, hidden_out, delta_out, down_out,
    load_sem, raw_ss, raw_rs, e_ss, e_rs, d_ss, d_rs, tab_ss, tab_rs,
    w_ls, wa_ss, wa_rs, wf_ss, wf_rs, out_sem, relay_ss, relay_rs, pair_ss, pair_rs,
):
    chain = Chain()
    g, me, c, z = chain.g, chain.me, chain.c, chain.z
    is_mid, is_end = chain.is_mid, chain.is_end
    groups = lax.axis_size("dp")
    ranks = lax.axis_size("expert")
    steps = 2 * groups
    width = raw.shape[-1]
    count = raw.shape[2]
    slot_rows = rows.shape[2]
    along_x, along_y = neighbours(g)
    fulls = (full_gate, full_up, full_down)
    shards = (wg_ref, wu_ref, wd_ref)

    sub = width // groups

    def load_x(k):
        return pltpu.make_async_copy(
            tokens_ref.at[:, pl.ds(k * width, width)], raw.at[0, k], load_sem.at[k]
        )

    def load_rest():
        for k in range(ahead, groups):
            load_x(k).start()
        for i in range(groups):
            for owner in range(groups):
                pltpu.make_async_copy(
                    grads_ref.at[:, pl.ds(owner * width + i * sub, sub)],
                    raw.at[0, groups + i, :, pl.ds(owner * sub, sub)], load_sem.at[groups + i],
                ).start()
        for w in range(3):
            pltpu.make_async_copy(shards[w].at[0], fulls[w].at[g], w_ls.at[w]).start()

    ahead = 3
    for k in range(ahead):
        load_x(k).start()

    def shard_to(w, way):
        device = (along_x, me) if way == 0 else (along_y, me)
        return send(shards[w].at[0], fulls[w].at[g], wa_ss.at[w, way], wa_rs.at[w, way], device)

    def forward_half(w, way):
        owner = along_y if way == 0 else along_x
        device = (along_x, me) if way == 0 else (along_y, me)
        half = fulls[w].shape[1] // 2
        piece = fulls[w].at[owner, pl.ds(way * half, half)]
        return send(piece, piece, wf_ss.at[w, way], wf_rs.at[w, way], device)

    def build_table():
        experts = lax.broadcasted_iota(jnp.int32, (ranks, count), 0)
        named = [experts == ids_ref[k : k + 1, :] for k in range(ids_ref.shape[0])]
        hits = functools.reduce(jnp.logical_or, named)
        before = lax.broadcasted_iota(jnp.int32, (count, count), 0) < lax.broadcasted_iota(
            jnp.int32, (count, count), 1
        )
        order = dot(hits.astype(F32).astype(BF16), before.astype(F32).astype(BF16))
        table_out[0, 0:ranks, :] = jnp.where(hits, order, -1.0)
        weight = jnp.zeros((ranks, count), F32)
        for k in range(ids_ref.shape[0]):
            weight = jnp.where(named[k], weight_ref[k : k + 1, :].astype(F32), weight)
        table_out[0, ranks : 2 * ranks, :] = weight

        rows[:, :, cap:, :] = jnp.zeros((steps, ranks, slot_rows - cap, width), BF16)

    def table_send(slot, sem, zz):
        return send(
            table_out.at[0], table_out.at[slot], tab_ss.at[sem], tab_rs.at[slot - 1], chain.at(zz, c)
        )

    targets = (me, me + 1 - 2 * c, 2 * chain.z_near, 2 * chain.z_near + 1)

    def selectors(j):
        slots = lax.broadcasted_iota(jnp.int32, (slot_rows, count), 0).astype(F32)
        for i, rank in enumerate(targets):
            hit = table_out[j, pl.ds(rank, 1), :] == slots
            block = pl.ds(i * slot_rows, slot_rows)
            select[0, j, block, :] = jnp.where(hit, 1.0, 0.0).astype(BF16)
            select[1, j, block, :] = jnp.where(
                hit, table_out[j, pl.ds(ranks + rank, 1), :], 0.0
            ).astype(BF16)

    def gather(j, k, z_from, blocks, e_slot):
        picked = dot(select[k // groups, j, 0 : blocks * slot_rows, :], raw[j, k]).astype(BF16)
        parts = [picked[i * slot_rows : (i + 1) * slot_rows] for i in range(blocks)]
        rows[k, 4 * c + z_from] = parts[0]
        stage_d[k, z_from] = parts[1]
        for i in range(2, blocks):
            stage_e[k, i - 2, e_slot] = parts[i]

    full = pl.ds(0, cap)
    far_places = ((chain.z_far_mid, 1), (chain.z_far_end, 2))

    def own_raw(k):
        return send(raw.at[0, k], raw.at[2, k], raw_ss.at[0, k], raw_rs.at[1, k], chain.at(chain.z_far_mid, c))

    def end_raw(k):
        return send(raw.at[0, k], raw.at[1, k], raw_ss.at[0, k], raw_rs.at[0, k], chain.at(chain.z_mid, c))

    def onward_raw(k):
        return send(raw.at[1, k], raw.at[3, k], raw_ss.at[1, k], raw_rs.at[2, k], chain.at(chain.z_far_mid, c))

    def own_to_end(k, i):
        return send(
            stage_e.at[k, i, 0, full], rows.at[k, 4 * c + z, full],
            e_ss.at[k, 0, i], e_rs.at[k, 0, c], chain.at(chain.z_end, i),
        )

    def far_to_end(k, i, which):
        z_from, slot = far_places[which]
        return send(
            stage_e.at[k, i, slot, full], rows.at[k, 4 * c + z_from, full],
            e_ss.at[k, 1 + which, i], e_rs.at[k, 1 + which, c], chain.at(chain.z_end, i),
        )

    def mid_to_partner(k):
        return send(
            stage_d.at[k, :, full], rows.at[k, pl.ds(4 * c, 4), full], d_ss.at[k], d_rs.at[k], chain.at(z, 1 - c)
        )

    def end_to_partner(k):
        return send(
            stage_d.at[k, z, full], rows.at[k, 4 * c + z, full], d_ss.at[k], d_rs.at[k], chain.at(z, 1 - c)
        )

    def own_block_from(k, core):
        return send(
            stage_e.at[k, 0, 0, full], rows.at[k, 4 * core + chain.z_mid, full],
            e_ss.at[k, 0, 0], e_rs.at[k, 0, core], chain.at(chain.z_mid, core),
        )

    def far_block_from(k, core, which):
        return send(
            stage_e.at[k, 0, 1, full], rows.at[k, 4 * core + far_places[which][0], full],
            e_ss.at[k, 1 + which, 0], e_rs.at[k, 1 + which, core], chain.at(chain.z_mid, core),
        )

    def landed_near(k):
        @pl.when(is_mid)
        def _():
            mid_to_partner(k).wait_recv()

        @pl.when(is_end)
        def _():
            end_to_partner(k).wait_recv()
            for core in range(2):
                own_block_from(k, core).wait_recv()

    def landed_far(k):
        @pl.when(is_end)
        def _():
            for core in range(2):
                for which in range(2):
                    far_block_from(k, core, which).wait_recv()

    def landed(k):
        landed_near(k)
        landed_far(k)

    def load_wait(k):
        pltpu.make_async_copy(
            tokens_ref.at[:, pl.ds(0, width)], raw.at[0, k], load_sem.at[k]
        ).wait()

    across = groups - 1 - g
    slots = ranks * slot_rows
    half_inner = hidden_out.shape[2] // 2

    def hidden_grad(q, carry):
        def tile(t, carry):
            four = pl.ds(4 * t, 4)
            value = functools.reduce(jnp.add, [
                dot(
                    rows[groups + q, four, :, owner * sub : (owner + 1) * sub].reshape(4 * slot_rows, sub),
                    full_down[owner, :, pl.ds(pl.multiple_of(q * sub, 128), sub)], 1, 1,
                )
                for owner in range(groups)
            ]).reshape(4, slot_rows, hg_val.shape[2])

            @pl.when(q == 0)
            def _():
                hg_val[four] = value

            @pl.when(q > 0)
            def _():
                hg_val[four] += value

            return carry

        return lax.fori_loop(0, ranks // 4, tile, carry)

    hidden_copy = pltpu.make_async_copy(hidden_out, hidden_hbm, out_sem.at[4])

    def block_of(tile):
        return pl.ds(tile * half_inner, half_inner)

    def of_owner(owner):
        return pl.ds(pl.multiple_of(owner * sub, 128), sub)

    def relay_to(i, way):
        device = (along_x, me) if way == 0 else (along_y, me)
        return send(
            down_part.at[i, block_of(way), of_owner(across)], down_relay.at[i, way],
            relay_ss.at[i, way], relay_rs.at[i, way], device,
        )

    def pair_to(i, way):
        owner = along_x if way == 0 else along_y
        return send(
            down_part.at[i, :, of_owner(owner)], down_in.at[i, way],
            pair_ss.at[i, way], pair_rs.at[i, way], (owner, me),
        )

    def down_make(i):
        for tile in range(2):
            left = hidden_out[:, :, tile * half_inner : (tile + 1) * half_inner].reshape(slots, half_inner)
            down_part[i, block_of(tile), :] = dot(
                left, rows[groups + i].reshape(slots, width), 0, 0
            ).astype(BF16)
        for way in range(2):
            relay_to(i, way).start()

    def down_pass(i):
        for way in range(2):
            owner = along_x if way == 0 else along_y
            relay_to(i, 1 - way).wait_recv()
            place = (i, block_of(1 - way), of_owner(owner))
            down_part[place] = (
                down_part[place].astype(F32) + down_relay[i, 1 - way].astype(F32)
            ).astype(BF16)
            pair_to(i, way).start()

    def down_own(i):
        for way in range(2):
            pair_to(i, way).wait_recv()
        total = down_part[i, :, of_owner(g)].astype(F32)
        for way in range(2):
            total = total + down_in[i, way].astype(F32)
        down_out[:, of_owner(i)] = total.astype(BF16)

    def prologue():
        build_table()
        selectors(0)
        for k in range(ahead):
            load_wait(k)

            @pl.when(is_mid)
            def _():
                gather(0, k, z, 4, 0)

    greet(chain, ranks, groups, prologue)
    for way in range(2):
        shard_to(0, way).start()

    @pl.when(is_mid)
    def _():
        own_raw(0).start()
        for k in range(ahead):
            own_to_end(k, 0).start()
            own_to_end(k, 1).start()

    @pl.when(is_end)
    def _():
        end_raw(0).start()
        table_send(1, 0, chain.z_mid).start()
        table_send(3, 1, chain.z_far_mid).start()

    @pl.when(is_mid)
    def _():
        table_send(2, 0, chain.z_far_mid).start()

    load_rest()
    for w in range(1, 3):
        for way in range(2):
            shard_to(w, way).start()
    for k in range(ahead, steps):
        load_wait(k)

    @pl.when(is_end)
    def _():
        for k in range(1, steps):
            end_raw(k).start()

    def step(k, carry):
        @pl.when(is_mid & (k < steps))
        def _():
            @pl.when(k > 0)
            def _():
                own_raw(k).start()

            @pl.when(k == 0)
            def _():
                table_send(1, 0, chain.z_mid).wait_recv()
                selectors(1)

            end_raw(k).wait_recv()
            onward_raw(k).start()

            @pl.when(k + ahead < steps)
            def _():
                gather(0, k + ahead, z, 4, 0)
                own_to_end(k + ahead, 0).start()
                own_to_end(k + ahead, 1).start()

            gather(1, k, chain.z_end, 2, 0)

        @pl.when(is_end & (k < steps))
        def _():
            gather(0, k, z, 2, 0)
            end_to_partner(k).start()

        for w in range(3):
            @pl.when(k == w + 2)
            def _():
                for way in range(2):
                    shard_to(w, 1 - way).wait_recv()
                    forward_half(w, way).start()

        @pl.when(k == groups + 1)
        def _():
            for kk in range(groups):
                landed(kk)
            for w in range(2):
                pltpu.make_async_copy(shards[w].at[0], fulls[w].at[g], w_ls.at[w]).wait()
                for way in range(2):
                    forward_half(w, way).wait_recv()

        @pl.when((k == groups + 1) | (k == groups + 2))
        def _():
            def forward(p, carry):
                pair = pl.ds(2 * p, 2)
                shape = (2, slot_rows, gate_val.shape[2])
                piece = [rows[kk, pair].reshape(2 * slot_rows, width) for kk in range(groups)]
                gate = functools.reduce(jnp.add, [dot(piece[kk], full_gate[kk]) for kk in range(groups)])
                up = functools.reduce(jnp.add, [dot(piece[kk], full_up[kk]) for kk in range(groups)])
                gate_val[pair] = gate.reshape(shape)
                up_val[pair] = up.reshape(shape)
                hidden_out[pair] = (gate * jax.nn.sigmoid(gate) * up).astype(BF16).reshape(shape)
                return carry

            start = (k - groups - 1) * (ranks // 4)
            lax.fori_loop(start, start + ranks // 4, forward, 0)

        @pl.when(k == groups + 2)
        def _():
            pltpu.make_async_copy(shards[2].at[0], fulls[2].at[g], w_ls.at[2]).wait()
            for way in range(2):
                forward_half(2, way).wait_recv()

        @pl.when(k >= groups + 2)
        def _():
            q = k - groups - 2

            @pl.when(q >= 1)
            def _():
                down_pass(q - 1)

            landed(groups + q)
            down_make(q)
            hidden_grad(q, 0)

            @pl.when(q == 0)
            def _():
                hidden_copy.start()

        @pl.when(is_mid & (k >= 1))
        def _():
            @pl.when(k == 1)
            def _():
                table_send(2, 0, chain.z_far_mid).wait_recv()
                table_send(3, 0, chain.z_far_mid).wait_recv()
                selectors(2)
                selectors(3)

            j = k - 1
            own_raw(j).wait_recv()
            gather(2, j, chain.z_far_mid, 4, 1)
            far_to_end(j, 0, 0).start()
            far_to_end(j, 1, 0).start()
            onward_raw(j).wait_recv()
            gather(3, j, chain.z_far_end, 4, 2)
            far_to_end(j, 0, 1).start()
            far_to_end(j, 1, 1).start()
            mid_to_partner(j).start()

        return carry

    lax.fori_loop(0, steps + 1, step, 0)

    outs = [
        pltpu.make_async_copy(full_gate, full_out.at[0], out_sem.at[0]),
        pltpu.make_async_copy(full_up, full_out.at[1], out_sem.at[1]),
    ]
    for copy in outs:
        copy.start()
    first = pltpu.make_async_copy(rows.at[pl.ds(0, groups)], rows_out.at[pl.ds(0, groups)], out_sem.at[2])
    first.start()

    down_pass(groups - 2)

    def deltas(t, carry):
        gate, up, grad = gate_val[t], up_val[t], hg_val[t]
        sig = jax.nn.sigmoid(gate)
        delta_out[0, t] = (grad * up * sig * (1.0 + gate * (1.0 - sig))).astype(BF16)
        delta_out[1, t] = (grad * (gate * sig)).astype(BF16)
        total = jnp.sum(hidden_out[t].astype(F32) * grad, axis=1, keepdims=True)
        dots_out[t] = jnp.broadcast_to(total, (total.shape[0], total.shape[0])).T[0:8, :]
        return carry

    late = pltpu.make_async_copy(rows.at[steps - 1], rows_out.at[groups], out_sem.at[3])

    def delta_copy(side, core, half):
        pair = pl.ds(4 * core + 2 * half, 2)
        return pltpu.make_async_copy(
            delta_out.at[:, pair], delta_hbm.at[:, pair], out_sem.at[6 + 2 * side + core]
        )

    for side, half in enumerate((chain.half, chain.far)):
        if side == 0:
            landed_near(steps - 1)
        else:
            landed_far(steps - 1)
            late.start()

        def last_rows(core, carry):
            pair = pl.ds(4 * core + 2 * half, 2)
            value = functools.reduce(jnp.add, [
                dot(
                    rows[steps - 1, pair, :, owner * sub : (owner + 1) * sub].reshape(2 * slot_rows, sub),
                    full_down[owner, :, (groups - 1) * sub : groups * sub], 1, 1,
                )
                for owner in range(groups)
            ])
            hg_val[pair] += value.reshape(2, slot_rows, hg_val.shape[2])
            for block in range(2):
                deltas(4 * core + 2 * half + block, 0)
            delta_copy(side, core, half).start()
            return carry

        lax.fori_loop(0, 2, last_rows, 0)

    for copy in outs:
        copy.wait()
    first.wait()
    late.wait()

    def finish_down(i, carry):
        down_own(i)
        for way in range(2):
            relay_to(i, way).wait_send()
            pair_to(i, way).wait_send()
        return carry

    lax.fori_loop(0, groups - 1, finish_down, 0)
    down_copy = pltpu.make_async_copy(down_out, down_hbm, out_sem.at[5])
    down_copy.start()
    for w in range(3):
        for way in range(2):
            shard_to(w, way).wait_send()
            forward_half(w, way).wait_send()

    def drain(k, carry):
        @pl.when(is_mid)
        def _():
            own_raw(k).wait_send()
            onward_raw(k).wait_send()
            for i in range(2):
                own_to_end(k, i).wait_send()
                for which in range(2):
                    far_to_end(k, i, which).wait_send()
            mid_to_partner(k).wait_send()

        @pl.when(is_end)
        def _():
            end_raw(k).wait_send()
            end_to_partner(k).wait_send()

        return carry

    lax.fori_loop(0, steps, drain, 0)

    @pl.when(is_mid)
    def _():
        table_send(2, 0, chain.z_far_mid).wait_send()

    @pl.when(is_end)
    def _():
        table_send(1, 0, chain.z_mid).wait_send()
        table_send(3, 1, chain.z_far_mid).wait_send()

    hidden_copy.wait()
    down_copy.wait()
    for side, half in enumerate((chain.half, chain.far)):
        for core in range(2):
            delta_copy(side, core, half).wait()


def forward_call(ids_t, weight_t, tokens, out_grad, w_gate, w_up, w_down, cap):
    count, depth = tokens.shape
    groups, ranks = lax.axis_size("dp"), lax.axis_size("expert")
    inner = w_gate.shape[2]
    width = depth // groups
    slot_rows = -(-cap // 16) * 16
    steps = 2 * groups
    hbm = pl.BlockSpec(memory_space=pl.ANY)
    vmem = pl.BlockSpec(memory_space=pltpu.VMEM)
    dma = pltpu.SemaphoreType.DMA
    return pl.pallas_call(
        functools.partial(forward_kernel, cap),
        out_shape=(
            jax.ShapeDtypeStruct((2, groups, width, inner), BF16),
            jax.ShapeDtypeStruct((groups + 1, ranks, slot_rows, width), BF16),
            jax.ShapeDtypeStruct((ranks, slot_rows, inner), BF16),
            jax.ShapeDtypeStruct((2, ranks, slot_rows, inner), BF16),
            jax.ShapeDtypeStruct((inner, width), BF16),
            jax.ShapeDtypeStruct((ranks, 8, slot_rows), F32),
            jax.ShapeDtypeStruct((4, 2 * ranks, count), F32),
        ),
        in_specs=[vmem, vmem, hbm, hbm, hbm, hbm, hbm],
        out_specs=(hbm,) * 5 + (vmem,) * 2,
        scratch_shapes=[
            pltpu.VMEM((4, steps, count, width), BF16),
            pltpu.VMEM((steps, ranks, slot_rows, width), BF16),
            pltpu.VMEM((steps, 4, slot_rows, width), BF16),
            pltpu.VMEM((steps, 2, 3, slot_rows, width), BF16),
            pltpu.VMEM((groups, width, inner), BF16),
            pltpu.VMEM((groups, width, inner), BF16),
            pltpu.VMEM((groups, inner, width), BF16),
            pltpu.VMEM((ranks, slot_rows, inner), F32),
            pltpu.VMEM((ranks, slot_rows, inner), F32),
            pltpu.VMEM((ranks, slot_rows, inner), F32),
            pltpu.VMEM((2, 4, 4 * slot_rows, count), BF16),
            pltpu.VMEM((groups - 1, inner, width), BF16),
            pltpu.VMEM((groups - 1, 2, inner // 2, width // groups), BF16),
            pltpu.VMEM((groups - 1, 2, inner, width // groups), BF16),
            pltpu.VMEM((ranks, slot_rows, inner), BF16),
            pltpu.VMEM((2, ranks, slot_rows, inner), BF16),
            pltpu.VMEM((inner, width), BF16),
            dma((steps,)), dma((2, steps)), dma((3, steps)), dma((steps, 3, 2)), dma((steps, 3, 2)),
            dma((steps,)), dma((steps,)), dma((2,)), dma((3,)),
            dma((3,)), dma((3, 2)), dma((3, 2)), dma((3, 2)), dma((3, 2)), dma((10,)),
            dma((groups - 1, 2)), dma((groups - 1, 2)), dma((groups - 1, 2)), dma((groups - 1, 2)),
        ],
        compiler_params=pltpu.CompilerParams(
            collective_id=0, has_side_effects=True, vmem_limit_bytes=67000000
        ),
    )(ids_t, weight_t, tokens, out_grad, w_gate, w_up, w_down)


def backward_kernel(
    cap,
    ids_ref, weight_ref, table_ref, dots_ref, full_ref, rows_ref, hidden_ref, delta_ref, down_ref,
    token_out, route_out, gate_out, up_out, down_out,
    full, rows, hidden, delta, grads, comb, gf_send, gf_in, end_send, select,
    diag_gu, pair_gu, pair_d, relay_gu, relay_d, in_gu, in_d, dots_in,
    load_sem, d_ss, d_rs, far_ss, far_rs, near_ss, near_rs, gf_ss, gf_rs, es_ss, es_rs,
    dots_ss, dots_rs, relay_ss, relay_rs, pair_ss, pair_rs,
):
    chain = Chain()
    g, me, c, z = chain.g, chain.me, chain.c, chain.z
    is_mid, is_end = chain.is_mid, chain.is_end
    groups = lax.axis_size("dp")
    ranks = lax.axis_size("expert")
    _, slot_rows, width = rows.shape[1:]
    count = table_ref.shape[2]
    inner = hidden.shape[2]
    along_x, along_y = neighbours(g)
    across = groups - 1 - g
    slots = ranks * slot_rows
    subs, narrow = grads.shape[0], grads.shape[3]

    loads = [
        pltpu.make_async_copy(delta_ref, delta, load_sem.at[0]),
        pltpu.make_async_copy(full_ref.at[:, 0], full.at[:, 0], load_sem.at[1]),
        pltpu.make_async_copy(rows_ref.at[across], rows.at[across], load_sem.at[2]),
        pltpu.make_async_copy(full_ref.at[:, pl.ds(1, subs - 1)], full.at[:, pl.ds(1, subs - 1)], load_sem.at[3]),
        pltpu.make_async_copy(rows_ref.at[groups], rows.at[groups], load_sem.at[4]),
        pltpu.make_async_copy(hidden_ref, hidden, load_sem.at[5]),
    ]
    for i, shard in enumerate((along_x, along_y, g)):
        loads.append(pltpu.make_async_copy(rows_ref.at[shard], rows.at[shard], load_sem.at[6 + i]))
    for copy in loads:
        copy.start()
    sub = width // groups
    half_inner = inner // 2
    down_ready = pltpu.make_async_copy(down_ref, down_out, load_sem.at[9])
    down_ready.start()

    def of_owner(owner):
        return pl.ds(pl.multiple_of(owner * sub, 128), sub)

    greet(chain, ranks, groups)

    real = pl.ds(0, cap)

    def dots_to(peer):
        return send(
            dots_ref.at[4 * (peer % 2) + peer // 2], dots_in.at[me],
            dots_ss.at[peer], dots_rs.at[me], (g, peer),
        )

    def dots_from(peer):
        return send(
            dots_ref.at[4 * c + z], dots_in.at[peer], dots_ss.at[peer], dots_rs.at[peer], (g, peer)
        )

    for step in range(1, ranks):
        dots_to((me + step) % ranks).start()

    comb[:, :, :, cap:, :] = jnp.zeros((subs, 4, 4, slot_rows - cap, narrow), BF16)
    targets = (me, me + 1 - 2 * c, 2 * chain.z_near, 2 * chain.z_near + 1)

    def selectors(j, z_from):
        slot = lax.broadcasted_iota(jnp.int32, (slot_rows, count), 0).astype(F32)
        for i, rank in enumerate(targets):
            hit = table_ref[j, pl.ds(rank, 1), :] == slot
            select[z_from, i * slot_rows : (i + 1) * slot_rows, :] = jnp.where(hit, 1.0, 0.0).astype(BF16)

    selectors(0, z)

    @pl.when(is_mid)
    def _():
        selectors(1, chain.z_end)
        selectors(2, chain.z_far_mid)
        selectors(3, chain.z_far_end)

    def to_partner(k):
        return send(
            grads.at[k, pl.ds(4 * (1 - c), 4), real], comb.at[k, :, 1, real],
            d_ss.at[k], d_rs.at[k], chain.at(z, 1 - c),
        )

    def end_to_partner(k):
        return send(
            grads.at[k, 4 * (1 - c) + z, real], comb.at[k, z, 1, real],
            d_ss.at[k], d_rs.at[k], chain.at(z, 1 - c),
        )

    homes = (chain.z_far_mid, chain.z_far_end)

    def far_home(k, core, home):
        return send(
            grads.at[k, 4 * core + homes[home], real], comb.at[k, homes[home], 2 + c, real],
            far_ss.at[k, core, home], far_rs.at[k, c, home], chain.at(chain.z_mid, core),
        )

    def far_from(k, core, home):
        return send(
            grads.at[k, 4 * core + homes[home], real], comb.at[k, homes[home], 2 + core, real],
            far_ss.at[k, core, home], far_rs.at[k, core, home], chain.at(chain.z_end, core),
        )

    def near_home(k, core):
        return send(
            grads.at[k, 4 * core + chain.z_mid, real], comb.at[k, chain.z_mid, 2 + c, real],
            near_ss.at[k, core], near_rs.at[k, c], chain.at(chain.z_mid, core),
        )

    def near_from(k, core):
        return send(
            grads.at[k, 4 * core + chain.z_mid, real], comb.at[k, chain.z_mid, 2 + core, real],
            near_ss.at[k, core], near_rs.at[k, core], chain.at(chain.z_end, core),
        )

    def sums_across(k, home):
        return send(
            gf_send.at[k, home], gf_in.at[k, home], gf_ss.at[k, home], gf_rs.at[k, home], chain.at(chain.z_far_mid, c)
        )

    def sums_to_end(k):
        return send(end_send.at[k], gf_in.at[k, 0], es_ss.at[k], es_rs.at[k], chain.at(chain.z_end, c))

    def device_on(way):
        return ((along_x if way == 0 else along_y), me)

    def relay_to(w, way):
        if w == 2:
            src, dst = pair_d.at[pl.ds(way * half_inner, half_inner), of_owner(across)], relay_d.at[way]
        else:
            half = width // 2
            src, dst = diag_gu.at[w, pl.ds(way * half, half)], relay_gu.at[w, way]
        return send(src, dst, relay_ss.at[w, way], relay_rs.at[w, way], device_on(way))

    def pair_to(w, way):
        if w == 2:
            src, dst = pair_d.at[:, of_owner(along_x if way == 0 else along_y)], in_d.at[way]
        else:
            src, dst = pair_gu.at[w, way], in_gu.at[w, way]
        return send(src, dst, pair_ss.at[w, way], pair_rs.at[w, way], device_on(way))

    def part(w, shard, tile):
        half = width // 2
        left = rows[shard, :, :, tile * half : (tile + 1) * half].reshape(slots, half)
        return dot(left, delta[w].reshape(slots, inner), 0, 0)

    def diagonal(w):
        if w == 2:
            for tile in range(2):
                left = hidden[:, :, tile * half_inner : (tile + 1) * half_inner].reshape(slots, half_inner)
                pair_d[pl.ds(tile * half_inner, half_inner), :] = dot(
                    left, rows[groups].reshape(slots, width), 0, 0
                ).astype(BF16)
        else:
            half = width // 2
            for tile in range(2):
                diag_gu[w, pl.ds(tile * half, half), :] = part(w, across, tile).astype(BF16)
        for way in range(2):
            relay_to(w, way).start()

    def pairs(w):
        for way in range(2):
            shard = along_x if way == 0 else along_y
            relay_to(w, 1 - way).wait_recv()
            if w == 2:
                place = (pl.ds((1 - way) * half_inner, half_inner), of_owner(shard))
                pair_d[place] = (pair_d[place].astype(F32) + relay_d[1 - way].astype(F32)).astype(BF16)
            else:
                half = width // 2
                for tile in range(2):
                    value = part(w, shard, tile).astype(BF16)
                    if tile == 1 - way:
                        value = (value.astype(F32) + relay_gu[w, 1 - way].astype(F32)).astype(BF16)
                    pair_gu[w, way, pl.ds(tile * half, half), :] = value
            pair_to(w, way).start()

    def finish(w):
        for way in range(2):
            pair_to(w, way).wait_recv()
        if w == 2:
            total = pair_d[:, of_owner(g)].astype(F32)
            for way in range(2):
                total = total + in_d[way].astype(F32)
            down_ready.wait()
            down_out[:, of_owner(groups - 1)] = total.astype(BF16)
        else:
            half = width // 2
            for tile in range(2):
                value = part(w, g, tile)
                block = pl.ds(tile * half, half)
                for way in range(2):
                    value = value + in_gu[w, way, block, :].astype(F32)
                (gate_out, up_out)[w][block, :] = value.astype(BF16)

    def input_grad(k):
        for hc in range(2):
            left = [delta[w, pl.ds(4 * hc, 4)].reshape(4 * slot_rows, inner) for w in range(2)]
            value = (dot(left[0], full[0, k], 1, 1) + dot(left[1], full[1, k], 1, 1)).astype(BF16)
            value = value.reshape(4, slot_rows, narrow)
            grads[k, pl.ds(4 * hc, 4)] = value

            @pl.when(is_end)
            def _():
                far_home(k, hc, 1).start()

            @pl.when(c == hc)
            def _():
                comb[k, :, 0] = value

    def summed(k, z_from, blocks):
        return dot(
            select[z_from, 0 : blocks * slot_rows, :],
            comb[k, z_from, 0:blocks].reshape(blocks * slot_rows, narrow), 0, 0,
        )

    for i in range(2):
        loads[i].wait()

    lag = 2

    def along(k, carry):
        @pl.when(k == 1)
        def _():
            loads[3].wait()

        @pl.when(k < subs)
        def _():
            input_grad(k)

            @pl.when(is_mid)
            def _():
                to_partner(k).start()

            @pl.when(is_end)
            def _():
                for core in range(2):
                    far_home(k, core, 0).start()
                end_to_partner(k).start()

        @pl.when(is_end & (k == subs - 1))
        def _():
            for j in range(subs):
                for core in range(2):
                    near_home(j, core).start()

        for w in range(2):
            @pl.when(k == w)
            def _():
                if w == 0:
                    loads[2].wait()
                diagonal(w)

        @pl.when(k == 2)
        def _():
            loads[4].wait()
            loads[5].wait()

            diagonal(2)

        @pl.when(is_mid & (k >= 1) & (k <= subs))
        def _():
            j = k - 1
            to_partner(j).wait_recv()
            for core in range(2):
                far_from(j, core, 1).wait_recv()
            gf_send[j, 1] = summed(j, chain.z_far_end, 4).astype(BF16)
            sums_across(j, 1).start()
            for core in range(2):
                far_from(j, core, 0).wait_recv()
            gf_send[j, 0] = summed(j, chain.z_far_mid, 4).astype(BF16)
            sums_across(j, 0).start()

        @pl.when(k == 3)
        def _():
            for copy in loads[6:]:
                copy.wait()

        for at, w in ((3, 0), (4, 2), (5, 1)):
            @pl.when(k == at)
            def _():
                pairs(w)

        @pl.when(is_mid & (k > lag))
        def _():
            j = k - 1 - lag
            sums_across(j, 1).wait_recv()
            end_send[j] = (summed(j, chain.z_end, 2) + gf_in[j, 1].astype(F32)).astype(BF16)
            sums_to_end(j).start()

        return carry

    lax.fori_loop(0, subs + 1 + lag, along, 0)

    for step in range(1, ranks):
        dots_from((me + step) % ranks).wait_recv()
    dots_in[me] = dots_ref[4 * c + z]
    found = jnp.zeros(ids_ref.shape, F32)
    slot = lax.broadcasted_iota(jnp.int32, (slot_rows, count), 0).astype(F32)
    for rank in range(ranks):
        hit = jnp.where(table_ref[0, rank : rank + 1, :] == slot, 1.0, 0.0)
        value = lax.dot_general(
            dots_in[rank], hit, (((1,), (0,)), ((), ())),
            precision=lax.Precision.HIGHEST, preferred_element_type=F32,
        )[0:1, :]
        found = jnp.where(ids_ref[...] == rank, value, found)
    route_out[...] = (found / weight_ref[...].astype(F32)).astype(BF16)

    def third(k, carry):
        columns = pl.ds(pl.multiple_of(k * narrow, 128), narrow)

        @pl.when(k == 0)
        def _():
            finish(0)

        @pl.when(k == 3)
        def _():
            finish(2)

        @pl.when(k == subs - 1)
        def _():
            finish(1)

        @pl.when(is_mid)
        def _():
            sums_across(k, 0).wait_recv()
            for core in range(2):
                near_from(k, core).wait_recv()
            token_out[:, columns] = (summed(k, z, 4) + gf_in[k, 0].astype(F32)).astype(BF16)

        @pl.when(is_end)
        def _():
            end_to_partner(k).wait_recv()
            sums_to_end(k).wait_recv()
            token_out[:, columns] = (summed(k, z, 2) + gf_in[k, 0].astype(F32)).astype(BF16)

        return carry

    lax.fori_loop(0, subs, third, 0)

    for w in range(3):
        for way in range(2):
            relay_to(w, way).wait_send()
            pair_to(w, way).wait_send()
    for step in range(1, ranks):
        dots_to((me + step) % ranks).wait_send()

    def drain(k, carry):
        @pl.when(is_mid)
        def _():
            to_partner(k).wait_send()
            for home in range(2):
                sums_across(k, home).wait_send()
            sums_to_end(k).wait_send()

        @pl.when(is_end)
        def _():
            for core in range(2):
                for home in range(2):
                    far_home(k, core, home).wait_send()
                near_home(k, core).wait_send()
            end_to_partner(k).wait_send()

        return carry

    lax.fori_loop(0, subs, drain, 0)


def backward_call(ids_t, weight_t, table, dots, full, rows, hidden, delta, down, cap):
    groups, ranks = lax.axis_size("dp"), lax.axis_size("expert")
    _, _, slot_rows, width = rows.shape
    count = table.shape[2]
    inner = hidden.shape[2]
    subs, narrow = 2 * groups, width // 2
    full = full.reshape(2, subs, narrow, inner)
    hbm = pl.BlockSpec(memory_space=pl.ANY)
    vmem = pl.BlockSpec(memory_space=pltpu.VMEM)
    dma = pltpu.SemaphoreType.DMA
    return pl.pallas_call(
        functools.partial(backward_kernel, cap),
        out_shape=(
            pltpu.VMEM((count, groups * width), BF16),
            pltpu.VMEM(ids_t.shape, BF16),
            pltpu.VMEM((width, inner), BF16),
            pltpu.VMEM((width, inner), BF16),
            pltpu.VMEM((inner, width), BF16),
        ),
        in_specs=[vmem, vmem, vmem, vmem, hbm, hbm, hbm, hbm, hbm],
        out_specs=(vmem,) * 5,
        scratch_shapes=[
            pltpu.VMEM(full.shape, BF16),
            pltpu.VMEM(rows.shape, BF16),
            pltpu.VMEM(hidden.shape, BF16),
            pltpu.VMEM(delta.shape, BF16),
            pltpu.VMEM((subs, ranks, slot_rows, narrow), BF16),
            pltpu.VMEM((subs, 4, 4, slot_rows, narrow), BF16),
            pltpu.VMEM((subs, 2, count, narrow), BF16),
            pltpu.VMEM((subs, 2, count, narrow), BF16),
            pltpu.VMEM((subs, count, narrow), BF16),
            pltpu.VMEM((4, 4 * slot_rows, count), BF16),
            pltpu.VMEM((2, width, inner), BF16),
            pltpu.VMEM((2, 2, width, inner), BF16),
            pltpu.VMEM((inner, width), BF16),
            pltpu.VMEM((2, 2, width // 2, inner), BF16),
            pltpu.VMEM((2, inner // 2, width // groups), BF16),
            pltpu.VMEM((2, 2, width, inner), BF16),
            pltpu.VMEM((2, inner, width // groups), BF16),
            pltpu.VMEM(dots.shape, F32),
            dma((12,)), dma((subs,)), dma((subs,)), dma((subs, 2, 2)), dma((subs, 2, 2)),
            dma((subs, 2)), dma((subs, 2)), dma((subs, 2)), dma((subs, 2)), dma((subs,)), dma((subs,)),
            dma((ranks,)), dma((ranks,)), dma((3, 2)), dma((3, 2)), dma((3, 2)), dma((3, 2)),
        ],
        compiler_params=pltpu.CompilerParams(
            collective_id=1, has_side_effects=True, vmem_limit_bytes=58000000
        ),
    )(ids_t, weight_t, table, dots, full, rows, hidden, delta, down)


def hand_over_kernel(*refs):
    ins, outs, sem = refs[0:5], refs[5:10], refs[10]
    copies = [pltpu.make_async_copy(ins[i], outs[i], sem.at[i]) for i in range(5)]
    for copy in copies:
        copy.start()
    for copy in copies:
        copy.wait()


def hand_over(*arrays):
    return pl.pallas_call(
        hand_over_kernel,
        out_shape=tuple(jax.ShapeDtypeStruct(a.shape, a.dtype) for a in arrays),
        in_specs=[pl.BlockSpec(memory_space=pltpu.VMEM)] * 5,
        out_specs=(pl.BlockSpec(memory_space=pl.ANY),) * 5,
        scratch_shapes=[pltpu.SemaphoreType.DMA((5,))],
        compiler_params=pltpu.CompilerParams(vmem_limit_bytes=8000000),
    )(*arrays)


def swap(block, axis, distance):
    ranks = lax.axis_size(axis)
    return lax.ppermute(block, axis, [(rank, rank ^ distance) for rank in range(ranks)])


def any_mesh(tokens, out_grad, expert_ids, route_weight, w_gate, w_up, w_down):
    tok_count = tokens.shape[0]
    route_count = expert_ids.shape[1]
    ranks = lax.axis_size("expert")
    groups = lax.axis_size("dp")
    me = lax.axis_index("expert")
    group = lax.axis_index("dp")
    capacity = 3 * tok_count * route_count // (2 * ranks)
    routes = tok_count * route_count
    total_slots = ranks * capacity
    full_gate = lax.all_gather(w_gate[0], "dp", axis=0, tiled=True)
    full_up = lax.all_gather(w_up[0], "dp", axis=0, tiled=True)
    full_down = lax.all_gather(w_down[0], "dp", axis=1, tiled=True)
    half = ranks // 2
    flat_ids = expert_ids.reshape(routes)
    one_hot = (flat_ids[:, None] == jnp.arange(ranks, dtype=jnp.int32)[None, :]).astype(jnp.int32)
    slot_order = jnp.sum((jnp.cumsum(one_hot, axis=0) - 1) * one_hot, axis=1)
    slot_order = slot_order.reshape(tok_count, route_count)
    routing = jnp.concatenate(
        [
            expert_ids.astype(jnp.float32),
            slot_order.astype(jnp.float32),
            route_weight.astype(jnp.float32),
        ],
        axis=1,
    )
    far_routing = swap(routing, "expert", half)
    far_ids = far_routing[:, :route_count].astype(jnp.int32)
    far_order = far_routing[:, route_count : 2 * route_count].astype(jnp.int32)
    far_weight = far_routing[:, 2 * route_count :].astype(jnp.bfloat16)
    far_tokens = swap(tokens, "expert", half)
    late_grad, slot_order = lax.optimization_barrier((out_grad, slot_order))
    far_grad = swap(late_grad, "expert", half)
    slots = jnp.arange(total_slots, dtype=jnp.int32)

    def selectors(destination, weight, count):
        picks = jnp.zeros((count, tok_count), jnp.bfloat16)
        weighted = jnp.zeros((count, tok_count), jnp.bfloat16)
        for k in range(route_count):
            hit = slots[:count, None] == destination[:, k][None, :]
            picks = jnp.where(hit, jnp.ones((), jnp.bfloat16), picks)
            weighted = jnp.where(hit, weight[:, k][None, :], weighted)
        return picks, weighted

    destination = (expert_ids ^ me) * capacity + slot_order
    far_destination = (far_ids ^ me) * capacity + far_order
    near_slots = half * capacity
    picks, _ = selectors(destination, route_weight, total_slots)
    near_picks, near_weighted = selectors(destination, route_weight, near_slots)
    far_picks, far_weighted = selectors(far_destination, far_weight, near_slots)

    def blocks(buffer, count=ranks):
        return [buffer[d * capacity : (d + 1) * capacity] for d in range(count)]

    def exchange(buffer, count=ranks):
        return [
            swap(block, "expert", d) if d else block for d, block in enumerate(blocks(buffer, count))
        ]

    rows_in = jnp.concatenate(
        exchange(dot(near_picks, tokens, 1, 0).astype(jnp.bfloat16), half)
        + exchange(dot(far_picks, far_tokens, 1, 0).astype(jnp.bfloat16), half)
    )
    gate_value = dot(rows_in, full_gate, 1, 0)
    up_value = dot(rows_in, full_up, 1, 0)
    sigmoid_gate = jax.nn.sigmoid(gate_value)
    activated = gate_value * sigmoid_gate
    hidden = (activated * up_value).astype(jnp.bfloat16)
    scaled_blocks = exchange(
        dot(near_weighted, late_grad, 1, 0).astype(jnp.bfloat16), half
    ) + exchange(dot(far_weighted, far_grad, 1, 0).astype(jnp.bfloat16), half)
    scaled_blocks, hidden = lax.optimization_barrier((scaled_blocks, hidden))
    scaled = jnp.concatenate(scaled_blocks)
    hidden_grad = dot(scaled, full_down, 1, 1)
    gate_delta = (
        hidden_grad * up_value * sigmoid_gate * (1.0 + gate_value * (1.0 - sigmoid_gate))
    ).astype(jnp.bfloat16)
    up_delta = (hidden_grad * activated).astype(jnp.bfloat16)
    input_grad = (
        dot(gate_delta, full_gate, 1, 1) + dot(up_delta, full_up, 1, 1)
    ).astype(jnp.bfloat16)
    back_blocks = []
    for d, block in enumerate(blocks(input_grad)):
        back_blocks.append(swap(block, "expert", d) if d else block)
    down_part = dot(hidden, scaled, 0, 0).astype(jnp.bfloat16)
    input_grad, rows_in, hidden = lax.optimization_barrier((input_grad, rows_in, hidden))
    expert_out = dot(hidden, full_down, 1, 0)
    weighted_dot = jnp.sum(expert_out * scaled.astype(jnp.float32), axis=1)
    gate_part = dot(rows_in, gate_delta, 0, 0).astype(jnp.bfloat16)
    up_part = dot(rows_in, up_delta, 0, 0).astype(jnp.bfloat16)
    down_grad = lax.psum_scatter(down_part, "dp", scatter_dimension=1, tiled=True)[None]
    gate_grad = lax.psum_scatter(gate_part, "dp", scatter_dimension=0, tiled=True)[None]
    depth = up_part.shape[0] // groups
    up_sum = jnp.zeros((depth, up_part.shape[1]), jnp.float32)
    for d in range(groups):
        piece = lax.dynamic_slice_in_dim(up_part, (group ^ d) * depth, depth, 0)
        up_sum = up_sum + (swap(piece, "dp", d) if d else piece).astype(jnp.float32)
    up_grad = up_sum.astype(jnp.bfloat16)[None]

    token_sum = jnp.zeros(tokens.shape, jnp.float32)
    for pick, block in zip(blocks(picks), back_blocks):
        token_sum = token_sum + dot(pick, block, 0, 0)
    token_grad = token_sum.astype(jnp.bfloat16)

    order = jnp.arange(ranks, dtype=jnp.int32)
    dots = weighted_dot.reshape(ranks, capacity)
    by_rank = jnp.sum(
        jnp.where(((order ^ me)[:, None] == order[None, :])[:, :, None], dots[None], 0.0), axis=1
    )
    back_dots = lax.all_to_all(by_rank, "expert", split_axis=0, concat_axis=0, tiled=True)
    arrival = expert_ids * capacity + slot_order
    hits = arrival.reshape(tok_count, route_count, 1) == slots[None, None, :]
    own_dots = jnp.sum(jnp.where(hits, back_dots.reshape(total_slots)[None, None, :], 0.0), axis=2)
    route_grad = (own_dots / route_weight.astype(jnp.float32)).astype(jnp.bfloat16)
    return (token_grad, route_grad, gate_grad, up_grad, down_grad)


def on_device(tokens, out_grad, expert_ids, route_weight, w_gate, w_up, w_down):
    count = tokens.shape[0]
    cap = 3 * count * expert_ids.shape[1] // (2 * lax.axis_size("expert"))
    ids_t, weight_t = expert_ids.T, route_weight.T
    full, rows, hidden, delta, down, dots, table = forward_call(
        ids_t, weight_t, tokens, out_grad, w_gate, w_up, w_down, cap
    )
    token_grad, route_grad, gate_grad, up_grad, down_grad = backward_call(
        ids_t, weight_t, table, dots, full, rows, hidden, delta, down, cap
    )
    token_grad, gate_grad, up_grad, down_grad, route_grad = hand_over(
        token_grad, gate_grad, up_grad, down_grad, route_grad
    )
    return token_grad, route_grad.T, gate_grad[None], up_grad[None], down_grad[None]


def solution(mesh):
    placed = (
        P(("dp", "expert"), None),
        P(("dp", "expert"), None),
        P(("dp", "expert"), None),
        P(("dp", "expert"), None),
        P("expert", "dp", None),
        P("expert", "dp", None),
        P("expert", None, "dp"),
    )
    chained = mesh.shape["expert"] == 8 and mesh.shape["dp"] == 4
    return jax.shard_map(
        on_device if chained else any_mesh, mesh=mesh, in_specs=placed,
        out_specs=(
            P(("dp", "expert"), None),
            P(("dp", "expert"), None),
            P("expert", "dp", None),
            P("expert", "dp", None),
            P("expert", None, "dp"),
        ),
        check_vma=False,
    )
```
